512 devices in a mesh: seq: 64 (over z, x, core), mp: 8 (over y).
Axes of the slice: x: 4, y: 8, z: 8, core: 2. Of those that a mesh axis runs over, the one named last changes fastest.
Arguments:
- x_inner: bfloat16 [2, 16384, 5120], P(None, 'seq', 'mp'), may hold values from -6 to 6
- z_gate: bfloat16 [2, 16384, 5120], P(None, 'seq', 'mp'), may hold values from -6 to 6
- b_input: bfloat16 [2, 16384, 128], P(None, 'seq'), may hold values from -6 to 6
- c_input: bfloat16 [2, 16384, 128], P(None, 'seq'), may hold values from -6 to 6
- dt_raw: float32 [2, 16384, 80], P(None, 'seq', 'mp'), may hold values from -3 to 3
- doc_ids: int32 [2, 16384], P(None, 'seq'), may hold values from 0 to 2, never falling along the last dimension, each value on 1 to 8192 neighbouring positions
- conv_x: bfloat16 [4, 5120], P(None, 'mp'), may hold values from -3 to 3
- conv_b: bfloat16 [4, 128], replicated, may hold values from -3 to 3
- conv_c: bfloat16 [4, 128], replicated, may hold values from -3 to 3
- dt_bias: float32 [80], P('mp'), as said below
- decay_rate: float32 [80], P('mp'), may hold values from 0.0625 to 0.25
- norm_gain: float32 [5120], P('mp'), may hold values from 0.25 to 1.75
- w_out: bfloat16 [5120, 2560], P('mp'), may hold values from -0.078125 to 0.078125
Outputs:
- layer_out: bfloat16 [2, 16384, 2560], P(None, 'seq', 'mp')
The draws below stay inside these ranges and needn't reach their ends.
Inputs may be any that keep to these rules, and one draw needn't show every extreme that they name: `doc_ids`: in each sequence the document numbers start at 0, never fall and rise by one at each new document; there are three documents, the longest exactly 8192 positions. `dt_bias`: softplus of each entry lies between 8/16384 and 1.
All inputs are finite; a program needn't handle non-finite values.
Results may differ from the reference program's by a relative error of at most 0.02.
Values may be sent and summed in bfloat16 or wider, within the bound.
A program may use at most 128 MiB of HBM per device.

```python
import math
import jax
import jax.numpy as jnp
import numpy as np
from jax import lax

D = 2560
HEADS = 80
HEADDIM = 64
DSTATE = 128
CONV = 4
BLOCK = 256
BATCH = 2
SEQLEN = 16384
INNER = 5120
N_MP = 8


def draw_dt_bias(key, part):
    level = jax.random.uniform(key, (HEADS,), jnp.float32)
    lowest = jnp.log(8.0 / SEQLEN)
    target = jnp.exp(lowest * level)
    return jnp.log(jnp.expm1(target)).astype(jnp.float32)


def levels(stream_key, shape, pieces, low, largest):
    def one(axis_at, parts):
        draws = jax.random.uniform(jax.random.fold_in(jax.random.fold_in(stream_key, 6), axis_at), (parts,), jnp.float32, low / len(pieces), largest / len(pieces))
        return jnp.repeat(jnp.exp(draws), shape[axis_at] // parts).reshape((-1,) + (1,) * (len(shape) - axis_at - 1))

    loudness = one(*pieces[0])
    for cut in pieces[1:]:
        loudness = loudness * one(*cut)
    return loudness


def split_up(amount, total, limit, slope):
    weights = [(1 << 20) // math.isqrt(rank ** slope) + 1 for rank in range(2, amount + 1)]
    surplus, holding = total - limit - (amount - 1), [1] * (amount - 1)
    while surplus > 0:
        movable = [i for i in range(amount - 1) if holding[i] < limit]
        whole, remaining = sum([weights[i] for i in movable]), surplus
        for i in movable:
            more = min(limit - holding[i], max(1, remaining * weights[i] // whole), surplus)
            holding[i] = holding[i] + more
            surplus = surplus - more
    return np.array([limit] + holding)


def ragged_sizes(rng, number_of, total, reach, skew):
    if number_of == 2:
        one = jax.random.randint(rng, (), max(1, total - reach), min(reach, total - 1) + 1)
        return jnp.stack([one, total - one])
    tallies = jnp.asarray(split_up(number_of, total, reach, skew), jnp.int32)
    twos = (number_of - 1) // 2
    source_of, sink = tallies[1:1 + 2 * twos:2], tallies[2:2 + 2 * twos:2]
    slack = jnp.minimum(source_of - 1, reach - sink)
    passed = jax.random.randint(jax.random.fold_in(rng, 1), (twos,), 0, 1 << 20) % (slack + 1)
    tallies = tallies.at[1:1 + 2 * twos:2].set(source_of - passed).at[2:2 + 2 * twos:2].set(sink + passed)
    return tallies[jax.random.permutation(jax.random.fold_in(rng, 2), number_of)]


def scatter_about(stream_key, extent, deviation, bound, shards=(), held_as=jnp.bfloat16):
    gain = levels(stream_key, extent, shards, -0.22, 0.18) if shards else 1.0
    values = jax.random.normal(stream_key, extent, jnp.float32) * deviation * gain
    return jnp.minimum(jnp.maximum(values, -bound), bound).astype(held_as)


def setup_inputs(seed: int = 0) -> dict:
    streams_of = jax.random.split(jax.random.key(seed), 14)
    x_inner = scatter_about(streams_of[0], (BATCH, SEQLEN, INNER), 1.0, 6.0, ((1, 64), (2, 8)))
    z_gate = scatter_about(streams_of[1], (BATCH, SEQLEN, INNER), 1.0, 6.0, ((1, 64), (2, 8)))
    b_input = scatter_about(streams_of[2], (BATCH, SEQLEN, DSTATE), 1.0, 6.0, ((1, 64),))
    c_input = scatter_about(streams_of[3], (BATCH, SEQLEN, DSTATE), 1.0, 6.0, ((1, 64),))
    dt_raw = scatter_about(streams_of[4], (BATCH, SEQLEN, HEADS), 0.5, 3.0, ((1, 64), (2, 8)), jnp.float32)
    doc_ids = jax.vmap(lambda own: jnp.searchsorted(jnp.cumsum(ragged_sizes(own, 3, SEQLEN, SEQLEN // 2, 0)), jnp.arange(SEQLEN), side="right"))(jax.random.split(streams_of[5], BATCH)).reshape((BATCH, SEQLEN)).astype(jnp.int32)
    conv_x = scatter_about(streams_of[6], (CONV, INNER), CONV ** -0.5, 3.0, ((1, 8),))
    conv_b = scatter_about(streams_of[7], (CONV, DSTATE), CONV ** -0.5, 3.0)
    conv_c = scatter_about(streams_of[8], (CONV, DSTATE), CONV ** -0.5, 3.0)
    dt_bias = draw_dt_bias(jax.random.fold_in(streams_of[13], 71), 0)
    decay_rate = jnp.clip(jnp.exp(math.log(0.25) - 1.3862944 * jax.random.uniform(streams_of[10], (HEADS,), jnp.float32) ** levels(streams_of[10], (HEADS,), ((0, 8),), -0.2, 0.2)), 0.0625, 0.25)
    norm_gain = jnp.clip(1.0 + 0.15 * jax.random.normal(streams_of[11], (INNER,), jnp.float32), 0.25, 1.75)
    w_out = scatter_about(streams_of[12], (INNER, D), INNER ** -0.5, 0.078125, ((0, 8),))
    return {"x_inner": x_inner, "z_gate": z_gate, "b_input": b_input, "c_input": c_input, "dt_raw": dt_raw, "doc_ids": doc_ids, "conv_x": conv_x, "conv_b": conv_b, "conv_c": conv_c, "dt_bias": dt_bias, "decay_rate": decay_rate, "norm_gain": norm_gain, "w_out": w_out}


EPSILON = 1e-05

def causal_conv(values, docs, weight):
    taps = weight.shape[0]
    length = values.shape[0]
    window = jnp.concatenate([jnp.zeros((taps - 1, values.shape[1]), jnp.bfloat16), values], axis=0)
    marks = jnp.concatenate([jnp.full((taps - 1,), -1, jnp.int32), docs.astype(jnp.int32)], axis=0)
    total = jnp.zeros(values.shape, jnp.float32)
    for offset in range(taps):
        same = (marks[offset:offset + length] == docs)[:, None]
        term = window[offset:offset + length].astype(jnp.float32) * weight[offset].astype(jnp.float32)
        total = total + jnp.where(same, term, 0.0)
    return jax.nn.silu(total).astype(jnp.bfloat16)

def sequence_mix(xs, bs, cs, steps, docs, rates):
    blocks = SEQLEN // BLOCK
    xs_b = xs.reshape(blocks, BLOCK, HEADS, HEADDIM)
    bs_b = bs.reshape(blocks, BLOCK, DSTATE)
    cs_b = cs.reshape(blocks, BLOCK, DSTATE)
    steps_b = steps.reshape(blocks, BLOCK, HEADS)
    docs_b = docs.reshape(blocks, BLOCK)
    order = jnp.arange(BLOCK)
    causal = order[:, None] >= order[None, :]

    def step_block(carry, block):
        state, before = carry
        xs_c, bs_c, cs_c, steps_c, docs_c = block
        logs = jnp.cumsum(-(steps_c * rates), axis=0)
        masked = causal & (docs_c[:, None] == docs_c[None, :])
        scores = jnp.dot(cs_c, bs_c.T, preferred_element_type=jnp.float32)
        spread = jnp.where(masked[:, :, None], logs[:, None, :] - logs[None, :, :], 0.0)
        mixing = jnp.where(masked[:, :, None], scores[:, :, None] * jnp.exp(spread) * steps_c[None, :, :], 0.0).astype(jnp.bfloat16)
        inner = jnp.einsum('tsh,shp->thp', mixing.astype(jnp.float32), xs_c.astype(jnp.float32))
        keeps = (docs_c == docs_c[-1])[:, None]
        weights = jnp.where(keeps, jnp.exp(logs[-1:] - logs) * steps_c, 0.0)
        loaded = (weights[:, :, None] * bs_c[:, None, :].astype(jnp.float32)).astype(jnp.bfloat16)
        fresh = jnp.einsum('shp,shn->hpn', xs_c.astype(jnp.float32), loaded.astype(jnp.float32))
        carried = docs_c == before
        entry = jnp.where(carried[:, None], jnp.exp(logs), 0.0)
        entering = state.astype(jnp.bfloat16)
        outer = jnp.einsum('tn,hpn->thp', cs_c.astype(jnp.float32), entering.astype(jnp.float32))
        mixed = inner + entry[:, :, None] * outer
        new_state = entry[-1][:, None, None] * state + fresh
        return ((new_state, docs_c[-1]), mixed)
    start = (jnp.zeros((HEADS, HEADDIM, DSTATE), jnp.float32), jnp.array(-1, dtype=jnp.int32))
    final, mixed_all = lax.scan(step_block, start, (xs_b, bs_b, cs_b, steps_b, docs_b))
    return mixed_all.reshape(SEQLEN, INNER)

def reference(x_inner, z_gate, b_input, c_input, dt_raw, doc_ids, conv_x, conv_b, conv_c, dt_bias, decay_rate, norm_gain, w_out):
    group = INNER // N_MP
    results = []
    for member in range(BATCH):
        docs = doc_ids[member].astype(jnp.int32)
        xs = causal_conv(x_inner[member], docs, conv_x)
        bs = causal_conv(b_input[member], docs, conv_b)
        cs = causal_conv(c_input[member], docs, conv_c)
        steps = jax.nn.softplus(dt_raw[member] + dt_bias)
        mixed = sequence_mix(xs.reshape(SEQLEN, HEADS, HEADDIM), bs, cs, steps, docs, decay_rate)
        gated = mixed * jax.nn.silu(z_gate[member].astype(jnp.float32))
        scale = lax.rsqrt(lax.optimization_barrier(jnp.sum(gated * gated, axis=1)) / INNER + EPSILON)
        normed = (gated * scale[:, None] * norm_gain).astype(jnp.bfloat16)
        total = jnp.zeros((SEQLEN, D), jnp.float32)
        for member_group in range(N_MP):
            lower = member_group * group
            partial_value = jnp.dot(normed[:, lower:lower + group], w_out[lower:lower + group], preferred_element_type=jnp.float32).astype(jnp.bfloat16)
            total = total + lax.optimization_barrier(partial_value).astype(jnp.float32)
        results.append(total.astype(jnp.bfloat16))
    return jnp.stack(results, axis=0)
```

```python
import functools

import jax
import jax.numpy as jnp
from jax import lax
from jax.experimental import pallas as pl
from jax.experimental.pallas import tpu as pltpu
from jax.sharding import Mesh
from jax.sharding import PartitionSpec as P

SPLIT = (8, 4, 2)
SEQ = ("sz", "sx", "sc")
INNER = 5120
EPSILON = 1e-05
BATCH = 2
LENGTH = 256
HALF = 128
HALO = 8
TAPS = 4
HEADDIM = 64
DSTATE = 128
REACH = 8192 // LENGTH
F32 = jnp.float32
BF16 = jnp.bfloat16
LANES = (((1,), (1,)), ((), ()))
ROWS = (((0,), (0,)), ((), ()))


def dot(a, b, dims):
    return lax.dot_general(a, b, dims, preferred_element_type=F32)


def split_two(value):
    high = value.astype(BF16)
    return high, (value - high.astype(F32)).astype(BF16)


def silu(value):
    return value / (1.0 + jnp.exp(-value))


class Plan:
    def __init__(self, split, members, channels, width):
        self.planes, self.xs, self.cores = split
        self.ring = self.xs * self.cores
        self.members = members
        self.channels = channels
        self.heads = channels // HEADDIM
        self.pairs = self.heads // 2
        self.conv = channels + 2 * DSTATE
        self.shard = channels // self.ring
        self.groups = self.shard // 16
        self.gate_rows = 8 if self.groups <= 8 else 16
        self.packet = self.shard + 2 * self.gate_rows
        self.reach = min(-(-REACH // self.ring), self.planes - 1)
        self.width = width
        self.out = width // members
        self.far = members // 2


def spread(rows, plan):
    return jnp.concatenate(
        [jnp.broadcast_to(rows[q : q + 1], (16, DSTATE)) for q in range(plan.groups)], axis=0
    )


def pair_columns(cols, first, lane):
    a = jnp.broadcast_to(cols[:, first : first + 1], (cols.shape[0], 128))
    b = jnp.broadcast_to(cols[:, first + 1 : first + 2], (cols.shape[0], 128))
    return jnp.where(lane < HEADDIM, a, b)


def layer_kernel(
    plan,
    x_hbm,
    z_hbm,
    b_hbm,
    c_hbm,
    dt_hbm,
    doc_hbm,
    cx_hbm,
    cb_hbm,
    cc_hbm,
    bias_ref,
    rate_ref,
    gain_ref,
    w_hbm,
    out_ref,
    xbc,
    halo,
    docs_ref,
    doc_halo,
    dt_ref,
    taps,
    z_ref,
    w_ref,
    wt,
    conv,
    masks,
    xw,
    y,
    scores,
    zg,
    gated,
    fsend,
    arecv,
    pref,
    qpref,
    tsend,
    brecv,
    hsend,
    hstate,
    part,
    up_recv,
    dn_recv,
    ssend,
    srecv,
    load_sem,
    halo_send,
    halo_recv,
    a_send,
    a_recv,
    b_send,
    b_recv,
    c_send,
    c_recv,
    s_send,
    s_recv,
    up_send,
    up_got,
    dn_send,
    dn_got,
):
    ch, nh, ring, members = plan.channels, plan.heads, plan.ring, plan.members
    iz, ix, ic = lax.axis_index("sz"), lax.axis_index("sx"), lax.axis_index("sc")
    me = lax.axis_index("mp")
    rank = ix * plan.cores + ic
    place = iz * ring + rank
    blocks = plan.planes * ring

    def in_plane(r):
        return {"sx": r // plan.cores, "sc": r % plan.cores}

    def in_line(j):
        return {"sz": j // ring, "sx": (j % ring) // plan.cores, "sc": j % plan.cores}

    after = in_line(lax.rem(place + 1, blocks))
    prior = in_line(lax.rem(place + blocks - 1, blocks))
    up = {"mp": lax.rem(me + 1, members)}
    down = {"mp": lax.rem(me + members - 1, members)}

    barrier = pltpu.get_barrier_semaphore()
    count = 0
    greet = [after, prior]
    greet += [in_plane(lax.rem(rank + k, ring)) for k in range(1, ring)]
    for k in range(1, plan.reach + 1):
        greet.append({"sz": lax.rem(iz + k, plan.planes)})
        greet.append({"sz": lax.rem(iz + plan.planes - k, plan.planes)})
    greet += [{"mp": lax.rem(me + k, members)} for k in range(1, members)]
    for peer in greet:
        pl.semaphore_signal(barrier, inc=1, device_id=peer, device_id_type=pl.DeviceIdType.MESH)
        count += 1

    loads = []

    def load(src, dst):
        copy = pltpu.make_async_copy(src, dst, load_sem.at[len(loads)])
        copy.start()
        loads.append(copy)
        return copy

    got_dt = load(dt_hbm, dt_ref)
    got_docs = load(doc_hbm, docs_ref)
    got_taps = [
        load(cx_hbm, taps.at[:, pl.ds(0, ch)]),
        load(cb_hbm, taps.at[:, pl.ds(ch, DSTATE)]),
        load(cc_hbm, taps.at[:, pl.ds(ch + DSTATE, DSTATE)]),
    ]
    got_rows = []
    for m in range(BATCH):
        got_rows.append(
            [
                load(x_hbm.at[m], xbc.at[m, :, pl.ds(0, ch)]),
                load(b_hbm.at[m], xbc.at[m, :, pl.ds(ch, DSTATE)]),
                load(c_hbm.at[m], xbc.at[m, :, pl.ds(ch + DSTATE, DSTATE)]),
            ]
        )
    got_z = load(z_hbm, z_ref)
    got_w = load(w_hbm, w_ref)

    lane = lax.broadcasted_iota(jnp.int32, (LENGTH, 128), 1)

    got_docs.wait()
    got_dt.wait()
    docs = docs_ref[...].astype(F32)
    head_row = lax.broadcasted_iota(jnp.int32, (16, LENGTH), 0)
    bias = jnp.zeros((16, LENGTH), F32)
    rate = jnp.zeros((16, LENGTH), F32)
    for h in range(nh):
        bias = jnp.where(head_row == h, bias_ref[h], bias)
        rate = jnp.where(head_row == h, rate_ref[h], rate)
    step_rows, log_parts = [], []
    for m in range(BATCH):
        raw = dt_ref[:, m, :]
        if nh < 16:
            raw = jnp.concatenate([raw, jnp.zeros((16 - nh, LENGTH), F32)], axis=0)
        shifted = raw + bias
        step = jnp.maximum(shifted, 0.0) + jnp.log1p(jnp.exp(-jnp.abs(shifted)))
        step_rows.append(step)
        log_parts.append(-(step * rate))
    log_step = jnp.concatenate(log_parts, axis=0)
    hi = log_step.astype(BF16)
    rest = log_step - hi.astype(F32)
    mid = rest.astype(BF16)
    low = (rest - mid.astype(F32)).astype(BF16)
    before = lax.broadcasted_iota(jnp.int32, (LENGTH, LENGTH), 0) <= lax.broadcasted_iota(
        jnp.int32, (LENGTH, LENGTH), 1
    )
    upper = jnp.where(before, 1.0, 0.0).astype(BF16)
    sums = dot(jnp.concatenate([low, mid, hi], axis=0), upper, (((1,), (0,)), ((), ())))
    span = BATCH * 16
    log_cum = sums[0:span] + sums[span : 2 * span] + sums[2 * span : 3 * span]
    log_rows = [log_cum[m * 16 : (m + 1) * 16] for m in range(BATCH)]
    row_mats = list(log_rows)
    ends = []
    for m in range(BATCH):
        end = log_rows[m][:, LENGTH - 1 : LENGTH]
        ends.append(end)
        keep = jnp.where(docs[m : m + 1] == docs[m : m + 1, LENGTH - 1 : LENGTH], 1.0, 0.0)
        row_mats.append(jnp.exp(jnp.minimum(end - log_rows[m], 0.0)) * step_rows[m] * keep)
    for m in range(BATCH):
        row_mats.append(jnp.exp(log_rows[m]))
    marks = []
    for m in range(BATCH):
        own = docs[m : m + 1]
        marks.append(own)
        for k in range(1, TAPS):
            marks.append(jnp.where(pltpu.roll(own, k, 1) == own, 1.0, 0.0))
    row_mats.append(jnp.concatenate(marks + [jnp.zeros((32 - len(marks), LENGTH), F32)], axis=0))
    cols = jnp.concatenate(row_mats, axis=0).T
    log_col, weight_col, entry_col, mark_col = 0, span, 2 * span, 3 * span

    for copy in got_taps:
        copy.wait()
    tap = taps[...].astype(F32)
    tiles = plan.conv // 128
    for m in range(BATCH):
        for k in range(1, TAPS):
            at = mark_col + m * TAPS + k
            masks[m, k - 1] = jnp.broadcast_to(cols[:, at : at + 1], (LENGTH, 128))
    for m in range(BATCH):
        for copy in got_rows[m]:
            copy.wait()
        for j in range(tiles):
            at = slice(j * 128, (j + 1) * 128)
            rows = xbc[m, :, at].astype(F32)
            total = rows * tap[TAPS - 1 : TAPS, at]
            for k in range(1, TAPS):
                weight = tap[TAPS - 1 - k : TAPS - k, at]
                total = total + (pltpu.roll(rows, k, 0) * weight) * masks[m, k - 1]
            total = silu(total)
            conv[m, :, at] = total.astype(BF16)
            if j < plan.pairs:
                scale = pair_columns(cols, weight_col + m * 16 + 2 * j, lane)
                xw[m, :, at] = (total.astype(BF16).astype(F32) * scale).astype(BF16)

    pl.semaphore_wait(barrier, count)

    halos = []
    for m in range(BATCH):
        halos.append(
            pltpu.make_async_remote_copy(
                src_ref=xbc.at[m, pl.ds(LENGTH - HALO, HALO)],
                dst_ref=halo.at[m],
                send_sem=halo_send.at[m],
                recv_sem=halo_recv.at[m],
                device_id=after,
                device_id_type=pl.DeviceIdType.MESH,
            )
        )
    halos.append(
        pltpu.make_async_remote_copy(
            src_ref=docs_ref.at[:, pl.ds(LENGTH - 128, 128)],
            dst_ref=doc_halo,
            send_sem=halo_send.at[BATCH],
            recv_sem=halo_recv.at[BATCH],
            device_id=after,
            device_id_type=pl.DeviceIdType.MESH,
        )
    )
    for copy in (halos[BATCH], *halos[:BATCH]):
        copy.start()

    got_w.wait()
    for j in range(plan.width // 128):
        wt[j * 128 : (j + 1) * 128, :] = w_ref[:, j * 128 : (j + 1) * 128].T
    got_z.wait()
    for m in range(BATCH):
        for j in range(plan.pairs):
            at = slice(j * 128, (j + 1) * 128)
            zg[m, :, at] = silu(z_ref[m, :, at].astype(F32))

    halos[BATCH].wait()
    doc_before = jnp.where(place == 0, -1.0, doc_halo[...].astype(F32))
    edge_marks = []
    joined = jnp.concatenate([doc_before, docs[:, 0:128]], axis=1)
    for k in range(1, TAPS):
        edge_marks.append(jnp.where(pltpu.roll(joined, k, 1) == joined, 1.0, 0.0))
    edge_rows = jnp.concatenate(
        edge_marks + [jnp.zeros((16 - BATCH * (TAPS - 1), LENGTH), F32)], axis=0
    )[:, 128:256]
    edge_rows = jnp.concatenate([edge_rows, jnp.zeros((112, 128), F32)], axis=0)
    edge_cols = edge_rows.T[0:HALO]

    def exchange(m, source, target, peers_send, peers_recv):
        copies = []
        for k in range(1, ring):
            to = lax.rem(rank + k, ring)
            copies.append(
                pltpu.make_async_remote_copy(
                    src_ref=source.at[m, to],
                    dst_ref=target(to),
                    send_sem=peers_send.at[m, k],
                    recv_sem=peers_recv.at[m, k],
                    device_id=in_plane(to),
                    device_id_type=pl.DeviceIdType.MESH,
                )
            )
        return copies

    group_row = lax.broadcasted_iota(jnp.int32, (ring * plan.gate_rows, 16), 0)
    group_head = lax.broadcasted_iota(jnp.int32, (ring * plan.gate_rows, 16), 1)
    bits = plan.gate_rows.bit_length() - 1
    shard_of, group_of = group_row >> bits, group_row & (plan.gate_rows - 1)
    picks = (((shard_of * plan.groups + group_of) >> 2) == group_head) & (group_of < plan.groups)
    pick = jnp.where(picks, 1.0, 0.0).astype(BF16)
    a_copies = []
    for m in range(BATCH):
        halos[m].wait()
        for j in range(tiles):
            at = slice(j * 128, (j + 1) * 128)
            lead = halo[m, :, at].astype(F32)
            own = xbc[m, 0:HALO, at].astype(F32)
            both = jnp.concatenate([lead, own], axis=0)
            total = own * tap[TAPS - 1 : TAPS, at]
            for k in range(1, TAPS):
                weight = tap[TAPS - 1 - k : TAPS - k, at]
                same = edge_cols[:, (k - 1) * BATCH + m : (k - 1) * BATCH + m + 1]
                total = total + (pltpu.roll(both, k, 0)[HALO : 2 * HALO] * weight) * same
            total = silu(total)
            conv[m, 0:HALO, at] = total.astype(BF16)
            if j < plan.pairs:
                scale = pair_columns(cols[0:HALO], weight_col + m * 16 + 2 * j, lane[0:HALO])
                xw[m, 0:HALO, at] = (total.astype(BF16).astype(F32) * scale).astype(BF16)
        state = dot(xw[m], conv[m, :, ch : ch + DSTATE], ROWS).astype(BF16)
        carried_end = docs[m : m + 1, LENGTH - 1 : LENGTH] == doc_before[m : m + 1, 127:128]
        gate = jnp.broadcast_to(jnp.exp(ends[m]) * jnp.where(carried_end, 1.0, 0.0), (16, DSTATE))
        gate_hi, gate_lo = split_two(gate)
        plain = (((1,), (0,)), ((), ()))
        hi_rows = dot(pick, gate_hi, plain).astype(BF16)
        lo_rows = dot(pick, gate_lo, plain).astype(BF16)
        for r in range(ring):
            fsend[m, r, 0 : plan.shard] = state[r * plan.shard : (r + 1) * plan.shard]
            at = slice(r * plan.gate_rows, (r + 1) * plan.gate_rows)
            fsend[m, r, plan.shard : plan.packet] = jnp.concatenate(
                [hi_rows[at], lo_rows[at]], axis=0
            )
        copies = exchange(m, fsend, lambda to, m=m: arecv.at[m, rank], a_send, a_recv)
        for copy in copies:
            copy.start()
        a_copies.append(copies)
        arecv[m, pl.ds(rank, 1)] = fsend[m, pl.ds(rank, 1)]

    def scores_of(m):
        t_pos = lax.broadcasted_iota(jnp.int32, (LENGTH, LENGTH), 0)
        s_pos = lax.broadcasted_iota(jnp.int32, (LENGTH, LENGTH), 1)
        doc_t = cols[:, mark_col + m * TAPS : mark_col + m * TAPS + 1]
        keep = (s_pos <= t_pos) & (doc_t == docs[m : m + 1])
        full = dot(conv[m, :, ch + DSTATE : ch + 2 * DSTATE], conv[m, :, ch : ch + DSTATE], LANES)
        scores[m] = jnp.where(keep, full, 0.0)

    def inner_of(m):
        low_lane = lane < HEADDIM
        for j in range(plan.pairs):
            at = slice(j * 128, (j + 1) * 128)
            xs = conv[m, :, at]
            xs_a = jnp.where(low_lane, xs, jnp.zeros_like(xs))
            xs_b = jnp.where(low_lane, jnp.zeros_like(xs), xs)
            for half in range(2):
                t0, s1 = half * HALF, (half + 1) * HALF
                base = scores[m, t0 : t0 + HALF, 0:s1]
                mixes = []
                for h in (2 * j, 2 * j + 1):
                    t_log = cols[t0 : t0 + HALF, log_col + m * 16 + h : log_col + m * 16 + h + 1]
                    s_log = log_rows[m][h : h + 1, 0:s1]
                    decay = jnp.exp(jnp.minimum(t_log - s_log, 0.0))
                    mixes.append((base * step_rows[m][h : h + 1, 0:s1] * decay).astype(BF16))
                y[m, t0 : t0 + HALF, at] = dot(
                    jnp.concatenate(mixes, axis=1),
                    jnp.concatenate([xs_a[0:s1], xs_b[0:s1]], axis=0),
                    (((1,), (0,)), ((), ())),
                )

    b_copies = []
    for m in range(BATCH):
        scores_of(m)
    for m in range(BATCH):
        for copy in a_copies[m]:
            copy.wait_recv()
        total = jnp.zeros((plan.shard, DSTATE), F32)
        product = jnp.ones((plan.gate_rows, DSTATE), F32)
        for d in range(ring):
            pref[m, d] = total
            qpref[m, d] = product
            packet = arecv[m, d].astype(F32)
            gates = (
                packet[plan.shard : plan.shard + plan.gate_rows]
                + packet[plan.shard + plan.gate_rows :]
            )
            total = spread(gates, plan) * total + packet[0 : plan.shard]
            product = product * gates
        tsend[m, 0 : plan.shard] = total.astype(BF16)
        hi_rows, lo_rows = split_two(product)
        tsend[m, plan.shard : plan.packet] = jnp.concatenate([hi_rows, lo_rows], axis=0)
        copies = []
        for k in range(1, plan.reach + 1):
            copy = pltpu.make_async_remote_copy(
                src_ref=tsend.at[m],
                dst_ref=brecv.at[m, k - 1],
                send_sem=b_send.at[m, k - 1],
                recv_sem=b_recv.at[m, k - 1],
                device_id={"sz": lax.rem(iz + k, plan.planes)},
                device_id_type=pl.DeviceIdType.MESH,
            )
            copy.start()
            copies.append(copy)
        b_copies.append(copies)
        if m == 0:
            inner_of(0)

    c_copies = []
    for m in range(BATCH):
        for copy in b_copies[m]:
            copy.wait_recv()
        incoming = jnp.zeros((plan.shard, DSTATE), F32)
        for k in range(plan.reach, 0, -1):
            packet = brecv[m, k - 1].astype(F32)
            gates = (
                packet[plan.shard : plan.shard + plan.gate_rows]
                + packet[plan.shard + plan.gate_rows :]
            )
            fresh = jnp.where(iz >= k, packet[0 : plan.shard], 0.0)
            incoming = spread(gates, plan) * incoming + fresh
            incoming = jnp.where(iz >= k, incoming, 0.0)
        for d in range(ring):
            entering = pref[m, d] + spread(qpref[m, d], plan) * incoming
            hsend[m, d] = entering.astype(BF16)
        home = pl.ds(pl.multiple_of(rank * plan.shard, 16), plan.shard)
        copies = exchange(m, hsend, lambda to, m=m: hstate.at[m, home], c_send, c_recv)
        for copy in copies:
            copy.start()
        c_copies.append(copies)
        hstate[m, home] = hsend[m, rank]
        if m == 0:
            inner_of(1)

    def arrow(chunk, step, upward):
        if upward:
            owner = lax.rem(me + plan.far - step, members)
            first, buffer, send, got, to = 0, up_recv, up_send, up_got, up
        else:
            owner = lax.rem(me + members - plan.far + step, members)
            first, buffer, send, got, to = plan.out // 2, dn_recv, dn_send, dn_got, down
        rows = pl.ds(first, plan.out // 2) if step == 0 else pl.ds(0, plan.out)
        return pltpu.make_async_remote_copy(
            src_ref=part.at[chunk, owner, rows],
            dst_ref=buffer.at[chunk, step, rows],
            send_sem=send.at[chunk, step],
            recv_sem=got.at[chunk, step],
            device_id=to,
            device_id_type=pl.DeviceIdType.MESH,
        )

    arrows = {}
    s_copies = []
    gain = gain_ref[...]
    for m in range(BATCH):
        for copy in c_copies[m]:
            copy.wait_recv()
        carried = cols[:, mark_col + m * TAPS : mark_col + m * TAPS + 1] == doc_before[m : m + 1, 127:128]
        squares = jnp.zeros((LENGTH, 128), F32)
        outer = dot(conv[m, :, ch + DSTATE : ch + 2 * DSTATE], hstate[m], LANES)
        for j in range(plan.pairs):
            at = slice(j * 128, (j + 1) * 128)
            entry = pair_columns(cols, entry_col + m * 16 + 2 * j, lane)
            entry = jnp.where(carried, entry, 0.0)
            mixed = (y[m, :, at] + entry * outer[:, at]) * zg[m, :, at]
            squares = squares + mixed * mixed
            gated[m, :, at] = (mixed * gain[:, at]).astype(BF16)
        square_hi, square_lo = split_two(squares)
        ones = jnp.ones((8, 128), BF16)
        square_rows = dot(ones, square_hi, LANES) + dot(ones, square_lo, LANES)
        ssend[m] = square_rows[0:1]

        def project(owner, m=m):
            rows = pl.ds(pl.multiple_of(owner * plan.out, 16), plan.out)
            tile = dot(wt[rows, :], gated[m], LANES).astype(BF16)
            part[2 * m, owner] = tile[:, 0:HALF]
            part[2 * m + 1, owner] = tile[:, HALF:LENGTH]

        project(lax.rem(me + plan.far, members))
        for chunk in (2 * m, 2 * m + 1):
            for upward in (True, False):
                arrows[chunk, 0, upward] = arrow(chunk, 0, upward)
                arrows[chunk, 0, upward].start()
        for k in range(1, members):
            copy = pltpu.make_async_remote_copy(
                src_ref=ssend.at[m],
                dst_ref=srecv.at[m, k],
                send_sem=s_send.at[m, k],
                recv_sem=s_recv.at[m, k],
                device_id={"mp": lax.rem(me + k, members)},
                device_id_type=pl.DeviceIdType.MESH,
            )
            copy.start()
            s_copies.append(copy)
        for step in range(1, plan.far):
            project(lax.rem(me + plan.far - step, members))
            project(lax.rem(me + members - plan.far + step, members))
        project(me)

    half = plan.out // 2
    chunks = range(2 * BATCH)
    for step in range(1, plan.far):
        for chunk in chunks:
            for upward in (True, False):
                arrows[chunk, step - 1, upward].wait_recv()
                buffer = up_recv if upward else dn_recv
                if upward:
                    owner = lax.rem(me + plan.far - step, members)
                else:
                    owner = lax.rem(me + members - plan.far + step, members)
                if step == 1:
                    rows = slice(0, half) if upward else slice(half, plan.out)
                else:
                    rows = slice(0, plan.out)
                total = part[chunk, owner, rows].astype(F32) + buffer[chunk, step - 1, rows].astype(F32)
                part[chunk, owner, rows] = total.astype(BF16)
                arrows[chunk, step, upward] = arrow(chunk, step, upward)
                arrows[chunk, step, upward].start()

    for copy in s_copies:
        copy.wait_recv()
    last = plan.far - 1
    for m in range(BATCH):
        square = ssend[m]
        for k in range(1, members):
            square = square + srecv[m, k]
        scale = lax.rsqrt(square / INNER + EPSILON)
        for side in range(2):
            chunk = 2 * m + side
            total = part[chunk, me].astype(F32)
            if last == 0:
                arrows[chunk, last, True].wait_recv()
                arrows[chunk, last, False].wait_recv()
                total = total + jnp.concatenate(
                    [up_recv[chunk, 0, 0:half], dn_recv[chunk, 0, half : plan.out]], axis=0
                ).astype(F32)
            else:
                for upward in (True, False):
                    arrows[chunk, last, upward].wait_recv()
                    buffer = up_recv if upward else dn_recv
                    total = total + buffer[chunk, last].astype(F32)
            at = slice(side * HALF, (side + 1) * HALF)
            out_ref[m, :, at] = (total * scale[:, at]).astype(BF16)

    for copy in halos:
        pass
    for group in (*a_copies, *b_copies, *c_copies, s_copies, list(arrows.values())):
        for copy in group:
            copy.wait_send()


def shards(
    plan,
    x_inner,
    z_gate,
    b_input,
    c_input,
    dt_raw,
    doc_ids,
    conv_x,
    conv_b,
    conv_c,
    dt_bias,
    decay_rate,
    norm_gain,
    w_out,
):
    hbm = pl.BlockSpec(memory_space=pltpu.HBM)
    smem = pl.BlockSpec(memory_space=pltpu.SMEM)
    vmem = pl.BlockSpec(memory_space=pltpu.VMEM)
    ch, ring, members = plan.channels, plan.ring, plan.members
    chunks = 2 * BATCH
    dma = pltpu.SemaphoreType.DMA
    reach = max(plan.reach, 1)
    scratch = [
        pltpu.VMEM((BATCH, LENGTH, plan.conv), BF16),
        pltpu.VMEM((BATCH, HALO, plan.conv), BF16),
        pltpu.VMEM((BATCH, LENGTH), jnp.int32),
        pltpu.VMEM((BATCH, 128), jnp.int32),
        pltpu.VMEM((plan.heads, BATCH, LENGTH), F32),
        pltpu.VMEM((TAPS, plan.conv), BF16),
        pltpu.VMEM((BATCH, LENGTH, ch), BF16),
        pltpu.VMEM((ch, plan.width), BF16),
        pltpu.VMEM((plan.width, ch), BF16),
        pltpu.VMEM((BATCH, LENGTH, plan.conv), BF16),
        pltpu.VMEM((BATCH, TAPS - 1, LENGTH, 128), F32),
        pltpu.VMEM((BATCH, LENGTH, ch), BF16),
        pltpu.VMEM((BATCH, LENGTH, ch), F32),
        pltpu.VMEM((BATCH, LENGTH, LENGTH), F32),
        pltpu.VMEM((BATCH, LENGTH, ch), F32),
        pltpu.VMEM((BATCH, LENGTH, ch), BF16),
        pltpu.VMEM((BATCH, ring, plan.packet, DSTATE), BF16),
        pltpu.VMEM((BATCH, ring, plan.packet, DSTATE), BF16),
        pltpu.VMEM((BATCH, ring, plan.shard, DSTATE), F32),
        pltpu.VMEM((BATCH, ring, plan.gate_rows, DSTATE), F32),
        pltpu.VMEM((BATCH, plan.packet, DSTATE), BF16),
        pltpu.VMEM((BATCH, reach, plan.packet, DSTATE), BF16),
        pltpu.VMEM((BATCH, ring, plan.shard, DSTATE), BF16),
        pltpu.VMEM((BATCH, ch, DSTATE), BF16),
        pltpu.VMEM((chunks, members, plan.out, HALF), BF16),
        pltpu.VMEM((chunks, plan.far, plan.out, HALF), BF16),
        pltpu.VMEM((chunks, plan.far, plan.out, HALF), BF16),
        pltpu.VMEM((BATCH, 1, LENGTH), F32),
        pltpu.VMEM((BATCH, members, 1, LENGTH), F32),
        dma((13,)),
        dma((BATCH + 1,)),
        dma((BATCH + 1,)),
        dma((BATCH, ring)),
        dma((BATCH, ring)),
        dma((BATCH, reach)),
        dma((BATCH, reach)),
        dma((BATCH, ring)),
        dma((BATCH, ring)),
        dma((BATCH, members)),
        dma((BATCH, members)),
        dma((chunks, plan.far)),
        dma((chunks, plan.far)),
        dma((chunks, plan.far)),
        dma((chunks, plan.far)),
    ]
    out = pl.pallas_call(
        functools.partial(layer_kernel, plan),
        name="mixer_layer",
        out_shape=jax.ShapeDtypeStruct((BATCH, plan.out, LENGTH), BF16),
        in_specs=[hbm] * 9 + [smem, smem, vmem, hbm],
        out_specs=vmem,
        scratch_shapes=scratch,
        compiler_params=pltpu.CompilerParams(
            collective_id=0, has_side_effects=True, vmem_limit_bytes=60 * 1024 * 1024
        ),
    )(
        x_inner,
        z_gate,
        b_input,
        c_input,
        jnp.transpose(dt_raw, (2, 0, 1)),
        doc_ids,
        conv_x,
        conv_b,
        conv_c,
        dt_bias,
        decay_rate,
        norm_gain.reshape(1, ch),
        w_out,
    )
    return jnp.transpose(out, (0, 2, 1))


def solution(mesh):
    members = mesh.shape["mp"]
    line = Mesh(mesh.devices.reshape(*SPLIT, members), (*SEQ, "mp"))

    def layer(*arrays):
        channels = arrays[0].shape[2] // members
        plan = Plan(SPLIT, members, channels, arrays[12].shape[1])
        placed = (
            P(None, SEQ, "mp"),
            P(None, SEQ, "mp"),
            P(None, SEQ, None),
            P(None, SEQ, None),
            P(None, SEQ, "mp"),
            P(None, SEQ),
            P(None, "mp"),
            P(),
            P(),
            P("mp"),
            P("mp"),
            P("mp"),
            P("mp", None),
        )
        return jax.shard_map(
            functools.partial(shards, plan),
            mesh=line,
            in_specs=placed,
            out_specs=P(None, SEQ, "mp"),
            check_vma=False,
        )(*arrays)

    return layer
```

```python
import functools

import jax
import jax.numpy as jnp
from jax import lax
from jax.experimental import pallas as pl
from jax.experimental.pallas import tpu as pltpu
from jax.sharding import Mesh
from jax.sharding import PartitionSpec as P

SPLIT = (8, 4, 2)
SEQ = ("sz", "sx", "sc")
INNER = 5120
EPSILON = 1e-05
BATCH = 2
LENGTH = 256
HALF = 128
HALO = 8
TAPS = 4
HEADDIM = 64
DSTATE = 128
REACH = 8192 // LENGTH
F32 = jnp.float32
BF16 = jnp.bfloat16
LANES = (((1,), (1,)), ((), ()))
ROWS = (((0,), (0,)), ((), ()))


def dot(a, b, dims):
    return lax.dot_general(a, b, dims, preferred_element_type=F32)


def split_two(value):
    high = value.astype(BF16)
    return high, (value - high.astype(F32)).astype(BF16)


def silu(value):
    return value / (1.0 + jnp.exp(-value))


class Plan:
    def __init__(self, split, members, channels, width):
        self.planes, self.xs, self.cores = split
        self.ring = self.xs * self.cores
        self.members = members
        self.channels = channels
        self.heads = channels // HEADDIM
        self.pairs = self.heads // 2
        self.conv = channels + 2 * DSTATE
        self.shard = channels // self.ring
        self.groups = self.shard // 16
        self.gate_rows = 8 if self.groups <= 8 else 16
        self.packet = self.shard + 2 * self.gate_rows
        self.reach = min(-(-REACH // self.ring), self.planes - 1)
        self.width = width
        self.out = width // members
        self.far = members // 2


def spread(rows, plan):
    return jnp.concatenate(
        [jnp.broadcast_to(rows[q : q + 1], (16, DSTATE)) for q in range(plan.groups)], axis=0
    )


def pair_columns(cols, first, lane):
    a = jnp.broadcast_to(cols[:, first : first + 1], (cols.shape[0], 128))
    b = jnp.broadcast_to(cols[:, first + 1 : first + 2], (cols.shape[0], 128))
    return jnp.where(lane < HEADDIM, a, b)


def layer_kernel(
    plan,
    x_hbm,
    z_hbm,
    b_hbm,
    c_hbm,
    dt_hbm,
    doc_hbm,
    cx_hbm,
    cb_hbm,
    cc_hbm,
    bias_ref,
    rate_ref,
    gain_ref,
    w_hbm,
    out_ref,
    xbc,
    halo,
    docs_ref,
    doc_halo,
    dt_ref,
    taps,
    z_ref,
    w_ref,
    wt,
    conv,
    masks,
    xw,
    y,
    scores,
    zg,
    gated,
    fsend,
    arecv,
    pref,
    qpref,
    tsend,
    brecv,
    hsend,
    hstate,
    part,
    up_recv,
    dn_recv,
    ssend,
    srecv,
    load_sem,
    halo_send,
    halo_recv,
    a_send,
    a_recv,
    b_send,
    b_recv,
    c_send,
    c_recv,
    s_send,
    s_recv,
    up_send,
    up_got,
    dn_send,
    dn_got,
):
    ch, nh, ring, members = plan.channels, plan.heads, plan.ring, plan.members
    iz, ix, ic = lax.axis_index("sz"), lax.axis_index("sx"), lax.axis_index("sc")
    me = lax.axis_index("mp")
    rank = ix * plan.cores + ic
    place = iz * ring + rank
    blocks = plan.planes * ring

    def in_plane(r):
        return {"sx": r // plan.cores, "sc": r % plan.cores}

    def in_line(j):
        return {"sz": j // ring, "sx": (j % ring) // plan.cores, "sc": j % plan.cores}

    after, prior = in_line(place + 1), in_line(place - 1)
    up = {"mp": lax.rem(me + 1, members)}
    down = {"mp": lax.rem(me + members - 1, members)}

    has_next, has_prior = place + 1 < blocks, place > 0

    def one(flag):
        return jnp.where(flag, 1, 0)

    barrier = pltpu.get_barrier_semaphore()

    def greet(peer):
        pl.semaphore_signal(barrier, inc=1, device_id=peer, device_id_type=pl.DeviceIdType.MESH)

    for k in range(1, ring):
        greet(in_plane(lax.rem(rank + k, ring)))
    for k in range(1, members):
        greet({"mp": lax.rem(me + k, members)})
    pl.when(has_prior)(lambda: greet(prior))
    count = ring - 1 + members - 1 + one(has_next)
    for k in range(1, plan.reach + 1):
        pl.when(iz >= k)(lambda k=k: greet({"sz": iz - k}))
        count = count + one(iz + k < plan.planes)

    loads = []

    def load(src, dst):
        copy = pltpu.make_async_copy(src, dst, load_sem.at[len(loads)])
        copy.start()
        loads.append(copy)
        return copy

    done = []

    def need(copy):
        if not any(copy is other for other in done):
            copy.wait()
            done.append(copy)

    def got_waits():
        for copy in loads:
            need(copy)

    got_dt = load(dt_hbm, dt_ref)
    got_docs = load(doc_hbm, docs_ref)
    got_taps = [
        load(cx_hbm, taps.at[:, pl.ds(0, ch)]),
        load(cb_hbm, taps.at[:, pl.ds(ch, DSTATE)]),
        load(cc_hbm, taps.at[:, pl.ds(ch + DSTATE, DSTATE)]),
    ]
    got_rows = []
    for m in range(BATCH):
        got_rows.append(
            [
                load(x_hbm.at[m], xbc.at[m, :, pl.ds(0, ch)]),
                load(b_hbm.at[m], xbc.at[m, :, pl.ds(ch, DSTATE)]),
                load(c_hbm.at[m], xbc.at[m, :, pl.ds(ch + DSTATE, DSTATE)]),
            ]
        )
    got_z = load(z_hbm, z_ref)
    got_w = load(w_hbm, w_ref)

    lane = lax.broadcasted_iota(jnp.int32, (LENGTH, 128), 1)

    need(got_docs)
    need(got_dt)
    docs = docs_ref[...].astype(F32)
    head_row = lax.broadcasted_iota(jnp.int32, (16, LENGTH), 0)
    bias = jnp.zeros((16, LENGTH), F32)
    rate = jnp.zeros((16, LENGTH), F32)
    for h in range(nh):
        bias = jnp.where(head_row == h, bias_ref[h], bias)
        rate = jnp.where(head_row == h, rate_ref[h], rate)
    step_rows, log_parts = [], []
    for m in range(BATCH):
        raw = dt_ref[:, m, :]
        if nh < 16:
            raw = jnp.concatenate([raw, jnp.zeros((16 - nh, LENGTH), F32)], axis=0)
        shifted = raw + bias
        step = jnp.maximum(shifted, 0.0) + jnp.log1p(jnp.exp(-jnp.abs(shifted)))
        step_rows.append(step)
        log_parts.append(-(step * rate))
    log_step = jnp.concatenate(log_parts, axis=0)
    hi = log_step.astype(BF16)
    rest = log_step - hi.astype(F32)
    mid = rest.astype(BF16)
    low = (rest - mid.astype(F32)).astype(BF16)
    before = lax.broadcasted_iota(jnp.int32, (LENGTH, LENGTH), 0) <= lax.broadcasted_iota(
        jnp.int32, (LENGTH, LENGTH), 1
    )
    upper = jnp.where(before, 1.0, 0.0).astype(BF16)
    sums = dot(jnp.concatenate([low, mid, hi], axis=0), upper, (((1,), (0,)), ((), ())))
    span = BATCH * 16
    log_cum = sums[0:span] + sums[span : 2 * span] + sums[2 * span : 3 * span]
    log_rows = [log_cum[m * 16 : (m + 1) * 16] for m in range(BATCH)]
    row_mats = list(log_rows)
    ends = []
    for m in range(BATCH):
        end = log_rows[m][:, LENGTH - 1 : LENGTH]
        ends.append(end)
        keep = jnp.where(docs[m : m + 1] == docs[m : m + 1, LENGTH - 1 : LENGTH], 1.0, 0.0)
        row_mats.append(jnp.exp(jnp.minimum(end - log_rows[m], 0.0)) * step_rows[m] * keep)
    for m in range(BATCH):
        row_mats.append(jnp.exp(log_rows[m]))
    marks = []
    for m in range(BATCH):
        own = docs[m : m + 1]
        marks.append(own)
        for k in range(1, TAPS):
            marks.append(jnp.where(pltpu.roll(own, k, 1) == own, 1.0, 0.0))
    row_mats.append(jnp.concatenate(marks + [jnp.zeros((32 - len(marks), LENGTH), F32)], axis=0))
    cols = jnp.concatenate(row_mats, axis=0).T
    log_col, weight_col, entry_col, mark_col = 0, span, 2 * span, 3 * span

    for copy in got_taps:
        need(copy)
    tap = taps[...].astype(F32)
    tiles = plan.conv // 128
    for m in range(BATCH):
        for k in range(1, TAPS):
            at = mark_col + m * TAPS + k
            masks[m, k - 1] = jnp.broadcast_to(cols[:, at : at + 1], (LENGTH, 128))
    def convolve(m):
        for copy in got_rows[m]:
            need(copy)
        for j in range(tiles):
            at = slice(j * 128, (j + 1) * 128)
            rows = xbc[m, :, at].astype(F32)
            total = rows * tap[TAPS - 1 : TAPS, at]
            for k in range(1, TAPS):
                weight = tap[TAPS - 1 - k : TAPS - k, at]
                total = total + (pltpu.roll(rows, k, 0) * weight) * masks[m, k - 1]
            total = silu(total)
            conv[m, :, at] = total.astype(BF16)
            if j < plan.pairs:
                scale = pair_columns(cols, weight_col + m * 16 + 2 * j, lane)
                xw[m, :, at] = (total.astype(BF16).astype(F32) * scale).astype(BF16)

    convolve(0)
    for copy in got_rows[1]:
        need(copy)
    pl.semaphore_wait(barrier, count)

    halos = []
    for m in range(BATCH):
        halos.append(
            pltpu.make_async_remote_copy(
                src_ref=xbc.at[m, pl.ds(LENGTH - HALO, HALO)],
                dst_ref=halo.at[m],
                send_sem=halo_send.at[m],
                recv_sem=halo_recv.at[m],
                device_id=after,
                device_id_type=pl.DeviceIdType.MESH,
            )
        )
    halos.append(
        pltpu.make_async_remote_copy(
            src_ref=docs_ref.at[:, pl.ds(LENGTH - 128, 128)],
            dst_ref=doc_halo,
            send_sem=halo_send.at[BATCH],
            recv_sem=halo_recv.at[BATCH],
            device_id=after,
            device_id_type=pl.DeviceIdType.MESH,
        )
    )
    def send_halo():
        for copy in (halos[BATCH], *halos[:BATCH]):
            copy.start()

    pl.when(has_next)(send_halo)
    convolve(1)

    def turn_weights():
        need(got_w)
        for j in range(plan.width // 128):
            wt[j * 128 : (j + 1) * 128, :] = w_ref[:, j * 128 : (j + 1) * 128].T

    def gate_inputs(m):
        need(got_z)
        for j in range(plan.pairs):
            at = slice(j * 128, (j + 1) * 128)
            zg[m, :, at] = silu(z_ref[m, :, at].astype(F32))

    pl.when(has_prior)(halos[BATCH].wait_recv)
    doc_before = jnp.where(has_prior, doc_halo[...].astype(F32), -1.0)
    edge_marks = []
    joined = jnp.concatenate([doc_before, docs[:, 0:128]], axis=1)
    for k in range(1, TAPS):
        edge_marks.append(jnp.where(pltpu.roll(joined, k, 1) == joined, 1.0, 0.0))
    edge_rows = jnp.concatenate(
        edge_marks + [jnp.zeros((16 - BATCH * (TAPS - 1), LENGTH), F32)], axis=0
    )[:, 128:256]
    edge_rows = jnp.concatenate([edge_rows, jnp.zeros((112, 128), F32)], axis=0)
    edge_cols = edge_rows.T[0:HALO]

    def exchange(m, source, target, peers_send, peers_recv):
        copies = []
        for k in range(1, ring):
            to = lax.rem(rank + k, ring)
            copies.append(
                pltpu.make_async_remote_copy(
                    src_ref=source.at[m, to],
                    dst_ref=target(to),
                    send_sem=peers_send.at[m, k],
                    recv_sem=peers_recv.at[m, k],
                    device_id=in_plane(to),
                    device_id_type=pl.DeviceIdType.MESH,
                )
            )
        return copies

    group_row = lax.broadcasted_iota(jnp.int32, (ring * plan.gate_rows, 16), 0)
    group_head = lax.broadcasted_iota(jnp.int32, (ring * plan.gate_rows, 16), 1)
    bits = plan.gate_rows.bit_length() - 1
    shard_of, group_of = group_row >> bits, group_row & (plan.gate_rows - 1)
    picks = (((shard_of * plan.groups + group_of) >> 2) == group_head) & (group_of < plan.groups)
    pick = jnp.where(picks, 1.0, 0.0).astype(BF16)
    a_copies = []
    for m in range(BATCH):
        pl.when(has_prior)(halos[m].wait_recv)
        for j in range(tiles):
            at = slice(j * 128, (j + 1) * 128)
            lead = jnp.where(has_prior, halo[m, :, at].astype(F32), 0.0)
            own = xbc[m, 0:HALO, at].astype(F32)
            both = jnp.concatenate([lead, own], axis=0)
            total = own * tap[TAPS - 1 : TAPS, at]
            for k in range(1, TAPS):
                weight = tap[TAPS - 1 - k : TAPS - k, at]
                same = edge_cols[:, (k - 1) * BATCH + m : (k - 1) * BATCH + m + 1]
                total = total + (pltpu.roll(both, k, 0)[HALO : 2 * HALO] * weight) * same
            total = silu(total)
            conv[m, 0:HALO, at] = total.astype(BF16)
            if j < plan.pairs:
                scale = pair_columns(cols[0:HALO], weight_col + m * 16 + 2 * j, lane[0:HALO])
                xw[m, 0:HALO, at] = (total.astype(BF16).astype(F32) * scale).astype(BF16)
        state = dot(xw[m], conv[m, :, ch : ch + DSTATE], ROWS).astype(BF16)
        carried_end = docs[m : m + 1, LENGTH - 1 : LENGTH] == doc_before[m : m + 1, 127:128]
        gate = jnp.broadcast_to(jnp.exp(ends[m]) * jnp.where(carried_end, 1.0, 0.0), (16, DSTATE))
        gate_hi, gate_lo = split_two(gate)
        plain = (((1,), (0,)), ((), ()))
        hi_rows = dot(pick, gate_hi, plain).astype(BF16)
        lo_rows = dot(pick, gate_lo, plain).astype(BF16)
        for r in range(ring):
            fsend[m, r, 0 : plan.shard] = state[r * plan.shard : (r + 1) * plan.shard]
            at = slice(r * plan.gate_rows, (r + 1) * plan.gate_rows)
            fsend[m, r, plan.shard : plan.packet] = jnp.concatenate(
                [hi_rows[at], lo_rows[at]], axis=0
            )
        copies = exchange(m, fsend, lambda to, m=m: arecv.at[m, rank], a_send, a_recv)
        for copy in copies:
            copy.start()
        a_copies.append(copies)
        arecv[m, pl.ds(rank, 1)] = fsend[m, pl.ds(rank, 1)]

    def scores_of(m):
        t_pos = lax.broadcasted_iota(jnp.int32, (LENGTH, LENGTH), 0)
        s_pos = lax.broadcasted_iota(jnp.int32, (LENGTH, LENGTH), 1)
        doc_t = cols[:, mark_col + m * TAPS : mark_col + m * TAPS + 1]
        keep = (s_pos <= t_pos) & (doc_t == docs[m : m + 1])
        full = dot(conv[m, :, ch + DSTATE : ch + 2 * DSTATE], conv[m, :, ch : ch + DSTATE], LANES)
        scores[m] = jnp.where(keep, full, 0.0)

    def inner_of(m):
        low_lane = lane < HEADDIM
        for j in range(plan.pairs):
            at = slice(j * 128, (j + 1) * 128)
            xs = conv[m, :, at]
            xs_a = jnp.where(low_lane, xs, jnp.zeros_like(xs))
            xs_b = jnp.where(low_lane, jnp.zeros_like(xs), xs)
            for half in range(2):
                t0, s1 = half * HALF, (half + 1) * HALF
                base = scores[m, t0 : t0 + HALF, 0:s1]
                mixes = []
                for h in (2 * j, 2 * j + 1):
                    t_log = cols[t0 : t0 + HALF, log_col + m * 16 + h : log_col + m * 16 + h + 1]
                    s_log = log_rows[m][h : h + 1, 0:s1]
                    decay = jnp.exp(jnp.minimum(t_log - s_log, 0.0))
                    mixes.append((base * step_rows[m][h : h + 1, 0:s1] * decay).astype(BF16))
                y[m, t0 : t0 + HALF, at] = dot(
                    jnp.concatenate(mixes, axis=1),
                    jnp.concatenate([xs_a[0:s1], xs_b[0:s1]], axis=0),
                    (((1,), (0,)), ((), ())),
                )

    gate_inputs(0)
    gate_inputs(1)
    scores_of(0)
    scores_of(1)
    b_copies = []
    for m in range(BATCH):
        for copy in a_copies[m]:
            copy.wait_recv()
        total = jnp.zeros((plan.shard, DSTATE), F32)
        product = jnp.ones((plan.gate_rows, DSTATE), F32)
        for d in range(ring):
            pref[m, d] = total
            qpref[m, d] = product
            packet = arecv[m, d].astype(F32)
            gates = (
                packet[plan.shard : plan.shard + plan.gate_rows]
                + packet[plan.shard + plan.gate_rows :]
            )
            total = spread(gates, plan) * total + packet[0 : plan.shard]
            product = product * gates
        tsend[m, 0 : plan.shard] = total.astype(BF16)
        hi_rows, lo_rows = split_two(product)
        tsend[m, plan.shard : plan.packet] = jnp.concatenate([hi_rows, lo_rows], axis=0)
        copies = []
        for k in range(1, plan.reach + 1):
            copy = pltpu.make_async_remote_copy(
                src_ref=tsend.at[m],
                dst_ref=brecv.at[m, k - 1],
                send_sem=b_send.at[m, k - 1],
                recv_sem=b_recv.at[m, k - 1],
                device_id={"sz": iz + k},
                device_id_type=pl.DeviceIdType.MESH,
            )
            pl.when(iz + k < plan.planes)(copy.start)
            copies.append(copy)
        b_copies.append(copies)

    turn_weights()
    inner_of(0)
    inner_of(1)
    c_copies = []
    for m in range(BATCH):
        for k in range(plan.reach, 0, -1):
            pl.when(iz >= k)(b_copies[m][k - 1].wait_recv)
        incoming = jnp.zeros((plan.shard, DSTATE), F32)
        for k in range(plan.reach, 0, -1):
            packet = brecv[m, k - 1].astype(F32)
            gates = (
                packet[plan.shard : plan.shard + plan.gate_rows]
                + packet[plan.shard + plan.gate_rows :]
            )
            fresh = jnp.where(iz >= k, packet[0 : plan.shard], 0.0)
            incoming = spread(gates, plan) * incoming + fresh
            incoming = jnp.where(iz >= k, incoming, 0.0)
        for d in range(ring):
            entering = pref[m, d] + spread(qpref[m, d], plan) * incoming
            hsend[m, d] = entering.astype(BF16)
        home = pl.ds(pl.multiple_of(rank * plan.shard, 16), plan.shard)
        copies = exchange(m, hsend, lambda to, m=m: hstate.at[m, home], c_send, c_recv)
        for copy in copies:
            copy.start()
        c_copies.append(copies)
        hstate[m, home] = hsend[m, rank]

    def arrow(chunk, step, upward):
        if upward:
            owner = lax.rem(me + plan.far - step, members)
            first, buffer, send, got, to = 0, up_recv, up_send, up_got, up
        else:
            owner = lax.rem(me + members - plan.far + step, members)
            first, buffer, send, got, to = plan.out // 2, dn_recv, dn_send, dn_got, down
        rows = pl.ds(first, plan.out // 2) if step == 0 else pl.ds(0, plan.out)
        return pltpu.make_async_remote_copy(
            src_ref=part.at[chunk, owner, rows],
            dst_ref=buffer.at[chunk, step, rows],
            send_sem=send.at[chunk, step],
            recv_sem=got.at[chunk, step],
            device_id=to,
            device_id_type=pl.DeviceIdType.MESH,
        )

    arrows = {}
    s_copies = []
    gain = gain_ref[...].reshape(1, ch)
    for m in range(BATCH):
        for copy in c_copies[m]:
            copy.wait_recv()
        carried = cols[:, mark_col + m * TAPS : mark_col + m * TAPS + 1] == doc_before[m : m + 1, 127:128]
        squares = jnp.zeros((LENGTH, 128), F32)
        outer = dot(conv[m, :, ch + DSTATE : ch + 2 * DSTATE], hstate[m], LANES)
        for j in range(plan.pairs):
            at = slice(j * 128, (j + 1) * 128)
            entry = pair_columns(cols, entry_col + m * 16 + 2 * j, lane)
            entry = jnp.where(carried, entry, 0.0)
            mixed = (y[m, :, at] + entry * outer[:, at]) * zg[m, :, at]
            squares = squares + mixed * mixed
            gated[m, :, at] = (mixed * gain[:, at]).astype(BF16)
        square_hi, square_lo = split_two(squares)
        ones = jnp.ones((8, 128), BF16)
        square_rows = dot(ones, square_hi, LANES) + dot(ones, square_lo, LANES)
        ssend[m] = square_rows[0:1]

        def project(owner, m=m):
            rows = pl.ds(pl.multiple_of(owner * plan.out, 16), plan.out)
            tile = dot(wt[rows, :], gated[m], LANES).astype(BF16)
            part[2 * m, owner] = tile[:, 0:HALF]
            part[2 * m + 1, owner] = tile[:, HALF:LENGTH]

        project(lax.rem(me + plan.far, members))
        for chunk in (2 * m, 2 * m + 1):
            for upward in (True, False):
                arrows[chunk, 0, upward] = arrow(chunk, 0, upward)
                arrows[chunk, 0, upward].start()
        for k in range(1, members):
            copy = pltpu.make_async_remote_copy(
                src_ref=ssend.at[m],
                dst_ref=srecv.at[m, k],
                send_sem=s_send.at[m, k],
                recv_sem=s_recv.at[m, k],
                device_id={"mp": lax.rem(me + k, members)},
                device_id_type=pl.DeviceIdType.MESH,
            )
            copy.start()
            s_copies.append(copy)
        for step in range(1, plan.far):
            project(lax.rem(me + plan.far - step, members))
            project(lax.rem(me + members - plan.far + step, members))
        project(me)

    half = plan.out // 2
    chunks = range(2 * BATCH)
    for step in range(1, plan.far):
        for chunk in chunks:
            for upward in (True, False):
                arrows[chunk, step - 1, upward].wait_recv()
                buffer = up_recv if upward else dn_recv
                if upward:
                    owner = lax.rem(me + plan.far - step, members)
                else:
                    owner = lax.rem(me + members - plan.far + step, members)
                if step == 1:
                    rows = slice(0, half) if upward else slice(half, plan.out)
                else:
                    rows = slice(0, plan.out)
                total = part[chunk, owner, rows].astype(F32) + buffer[chunk, step - 1, rows].astype(F32)
                part[chunk, owner, rows] = total.astype(BF16)
                arrows[chunk, step, upward] = arrow(chunk, step, upward)
                arrows[chunk, step, upward].start()

    for copy in s_copies:
        copy.wait_recv()
    last = plan.far - 1
    for m in range(BATCH):
        square = ssend[m]
        for k in range(1, members):
            square = square + srecv[m, k]
        scale = lax.rsqrt(square / INNER + EPSILON)
        for side in range(2):
            chunk = 2 * m + side
            total = part[chunk, me].astype(F32)
            if last == 0:
                arrows[chunk, last, True].wait_recv()
                arrows[chunk, last, False].wait_recv()
                total = total + jnp.concatenate(
                    [up_recv[chunk, 0, 0:half], dn_recv[chunk, 0, half : plan.out]], axis=0
                ).astype(F32)
            else:
                for upward in (True, False):
                    arrows[chunk, last, upward].wait_recv()
                    buffer = up_recv if upward else dn_recv
                    total = total + buffer[chunk, last].astype(F32)
            at = slice(side * HALF, (side + 1) * HALF)
            out_ref[m, :, at] = (total * scale[:, at]).astype(BF16)

    def sent():
        for copy in halos:
            copy.wait_send()

    pl.when(has_next)(sent)
    for group in (*a_copies, *c_copies, s_copies, list(arrows.values())):
        for copy in group:
            copy.wait_send()
    for m in range(BATCH):
        for k in range(1, plan.reach + 1):
            pl.when(iz + k < plan.planes)(b_copies[m][k - 1].wait_send)


def shards(
    plan,
    x_inner,
    z_gate,
    b_input,
    c_input,
    dt_raw,
    doc_ids,
    conv_x,
    conv_b,
    conv_c,
    dt_bias,
    decay_rate,
    norm_gain,
    w_out,
):
    hbm = pl.BlockSpec(memory_space=pltpu.HBM)
    smem = pl.BlockSpec(memory_space=pltpu.SMEM)
    vmem = pl.BlockSpec(memory_space=pltpu.VMEM)
    ch, ring, members = plan.channels, plan.ring, plan.members
    chunks = 2 * BATCH
    dma = pltpu.SemaphoreType.DMA
    reach = max(plan.reach, 1)
    scratch = [
        pltpu.VMEM((BATCH, LENGTH, plan.conv), BF16),
        pltpu.VMEM((BATCH, HALO, plan.conv), BF16),
        pltpu.VMEM((BATCH, LENGTH), jnp.int32),
        pltpu.VMEM((BATCH, 128), jnp.int32),
        pltpu.VMEM((plan.heads, BATCH, LENGTH), F32),
        pltpu.VMEM((TAPS, plan.conv), BF16),
        pltpu.VMEM((BATCH, LENGTH, ch), BF16),
        pltpu.VMEM((ch, plan.width), BF16),
        pltpu.VMEM((plan.width, ch), BF16),
        pltpu.VMEM((BATCH, LENGTH, plan.conv), BF16),
        pltpu.VMEM((BATCH, TAPS - 1, LENGTH, 128), F32),
        pltpu.VMEM((BATCH, LENGTH, ch), BF16),
        pltpu.VMEM((BATCH, LENGTH, ch), F32),
        pltpu.VMEM((BATCH, LENGTH, LENGTH), F32),
        pltpu.VMEM((BATCH, LENGTH, ch), F32),
        pltpu.VMEM((BATCH, LENGTH, ch), BF16),
        pltpu.VMEM((BATCH, ring, plan.packet, DSTATE), BF16),
        pltpu.VMEM((BATCH, ring, plan.packet, DSTATE), BF16),
        pltpu.VMEM((BATCH, ring, plan.shard, DSTATE), F32),
        pltpu.VMEM((BATCH, ring, plan.gate_rows, DSTATE), F32),
        pltpu.VMEM((BATCH, plan.packet, DSTATE), BF16),
        pltpu.VMEM((BATCH, reach, plan.packet, DSTATE), BF16),
        pltpu.VMEM((BATCH, ring, plan.shard, DSTATE), BF16),
        pltpu.VMEM((BATCH, ch, DSTATE), BF16),
        pltpu.VMEM((chunks, members, plan.out, HALF), BF16),
        pltpu.VMEM((chunks, plan.far, plan.out, HALF), BF16),
        pltpu.VMEM((chunks, plan.far, plan.out, HALF), BF16),
        pltpu.VMEM((BATCH, 1, LENGTH), F32),
        pltpu.VMEM((BATCH, members, 1, LENGTH), F32),
        dma((13,)),
        dma((BATCH + 1,)),
        dma((BATCH + 1,)),
        dma((BATCH, ring)),
        dma((BATCH, ring)),
        dma((BATCH, reach)),
        dma((BATCH, reach)),
        dma((BATCH, ring)),
        dma((BATCH, ring)),
        dma((BATCH, members)),
        dma((BATCH, members)),
        dma((chunks, plan.far)),
        dma((chunks, plan.far)),
        dma((chunks, plan.far)),
        dma((chunks, plan.far)),
    ]
    out = pl.pallas_call(
        functools.partial(layer_kernel, plan),
        name="mixer_layer",
        out_shape=jax.ShapeDtypeStruct((BATCH, plan.out, LENGTH), BF16),
        in_specs=[hbm] * 9 + [smem, smem, vmem, hbm],
        out_specs=vmem,
        scratch_shapes=scratch,
        compiler_params=pltpu.CompilerParams(
            collective_id=0, has_side_effects=True, vmem_limit_bytes=60 * 1024 * 1024
        ),
    )(
        x_inner,
        z_gate,
        b_input,
        c_input,
        jnp.transpose(dt_raw, (2, 0, 1)),
        doc_ids,
        conv_x,
        conv_b,
        conv_c,
        dt_bias,
        decay_rate,
        norm_gain,
        w_out,
    )
    return jnp.transpose(out, (0, 2, 1))


def solution(mesh):
    members = mesh.shape["mp"]
    line = Mesh(mesh.devices.reshape(*SPLIT, members), (*SEQ, "mp"))

    def layer(*arrays):
        channels = arrays[0].shape[2] // members
        plan = Plan(SPLIT, members, channels, arrays[12].shape[1])
        placed = (
            P(None, SEQ, "mp"),
            P(None, SEQ, "mp"),
            P(None, SEQ, None),
            P(None, SEQ, None),
            P(None, SEQ, "mp"),
            P(None, SEQ),
            P(None, "mp"),
            P(),
            P(),
            P("mp"),
            P("mp"),
            P("mp"),
            P("mp", None),
        )
        return jax.shard_map(
            functools.partial(shards, plan),
            mesh=line,
            in_specs=placed,
            out_specs=P(None, SEQ, "mp"),
            check_vma=False,
        )(*arrays)

    return layer
```

```python
import functools

import jax
import jax.numpy as jnp
from jax import lax
from jax.experimental import pallas as pl
from jax.experimental.pallas import tpu as pltpu
from jax.sharding import Mesh
from jax.sharding import PartitionSpec as P

SPLIT = (8, 4, 2)
SEQ = ("sz", "sx", "sc")
INNER = 5120
EPSILON = 1e-05
BATCH = 2
LENGTH = 256
HALF = 128
HALO = 8
TAPS = 4
HEADDIM = 64
DSTATE = 128
REACH = 8192 // LENGTH
F32 = jnp.float32
BF16 = jnp.bfloat16
LANES = (((1,), (1,)), ((), ()))
ROWS = (((0,), (0,)), ((), ()))


def dot(a, b, dims):
    return lax.dot_general(a, b, dims, preferred_element_type=F32)


def split_two(value):
    high = value.astype(BF16)
    return high, (value - high.astype(F32)).astype(BF16)


def silu(value):
    return value / (1.0 + jnp.exp(-value))


class Plan:
    def __init__(self, split, members, channels, width):
        self.planes, self.xs, self.cores = split
        self.ring = self.xs * self.cores
        self.members = members
        self.channels = channels
        self.heads = channels // HEADDIM
        self.pairs = self.heads // 2
        self.conv = channels + 2 * DSTATE
        self.shard = channels // self.ring
        self.groups = self.shard // 16
        self.gate_rows = 8 if self.groups <= 8 else 16
        self.packet = self.shard + 2 * self.gate_rows
        self.reach = min(-(-REACH // self.ring), self.planes - 1)
        assert self.reach <= 4
        self.width = width
        self.out = width // members
        self.far = members // 2


def spread(rows, plan):
    return jnp.concatenate(
        [jnp.broadcast_to(rows[q : q + 1], (16, DSTATE)) for q in range(plan.groups)], axis=0
    )


def pair_columns(cols, first, lane):
    a = jnp.broadcast_to(cols[:, first : first + 1], (cols.shape[0], 128))
    b = jnp.broadcast_to(cols[:, first + 1 : first + 2], (cols.shape[0], 128))
    return jnp.where(lane < HEADDIM, a, b)


def layer_kernel(
    plan,
    x_hbm,
    z_hbm,
    b_hbm,
    c_hbm,
    dt_hbm,
    doc_hbm,
    cx_hbm,
    cb_hbm,
    cc_hbm,
    bias_ref,
    rate_ref,
    gain_ref,
    w_hbm,
    out_ref,
    xbc,
    halo,
    docs_ref,
    doc_halo,
    dt_ref,
    taps,
    z_ref,
    w_ref,
    wt,
    conv,
    masks,
    xw,
    y,
    scores,
    zg,
    gated,
    fsend,
    arecv,
    pref,
    qpref,
    tsend,
    brecv,
    hsend,
    hstate,
    part,
    up_recv,
    dn_recv,
    ssend,
    srecv,
    load_sem,
    halo_send,
    halo_recv,
    a_send,
    a_recv,
    b_send,
    b_recv,
    c_send,
    c_recv,
    s_send,
    s_recv,
    up_send,
    up_got,
    dn_send,
    dn_got,
    word,
):
    ch, nh, ring, members = plan.channels, plan.heads, plan.ring, plan.members
    iz, ix, ic = lax.axis_index("sz"), lax.axis_index("sx"), lax.axis_index("sc")
    me = lax.axis_index("mp")
    rank = ix * plan.cores + ic
    place = iz * ring + rank
    blocks = plan.planes * ring

    def in_plane(r):
        return {"sx": r // plan.cores, "sc": r % plan.cores}

    def in_line(j):
        return {"sz": j // ring, "sx": (j % ring) // plan.cores, "sc": j % plan.cores}

    after, prior = in_line(place + 1), in_line(place - 1)
    up = {"mp": lax.rem(me + 1, members)}
    down = {"mp": lax.rem(me + members - 1, members)}

    has_next, has_prior = place + 1 < blocks, place > 0

    def one(flag):
        return jnp.where(flag, 1, 0)

    barrier = pltpu.get_barrier_semaphore()

    def greet(peer):
        pl.semaphore_signal(barrier, inc=1, device_id=peer, device_id_type=pl.DeviceIdType.MESH)

    for k in range(1, ring):
        greet(in_plane(lax.rem(rank + k, ring)))
    for k in range(1, members):
        greet({"mp": lax.rem(me + k, members)})
    pl.when(has_prior)(lambda: greet(prior))
    count = ring - 1 + members - 1 + one(has_next)
    above, below = {"sz": iz + 1}, {"sz": iz - 1}
    has_above, has_below = iz + 1 < plan.planes, iz > 0
    pl.when(has_below)(lambda: greet(below))
    pl.when(has_above)(lambda: greet(above))
    count = count + one(has_above) + one(has_below)

    def pass_word(k):
        pl.when(has_below & (iz + k - 1 < plan.planes))(
            lambda: pl.semaphore_signal(
                word.at[k], inc=1, device_id=below, device_id_type=pl.DeviceIdType.MESH
            )
        )

    def hear_word(k):
        pl.when(iz + k < plan.planes)(lambda: pl.semaphore_wait(word.at[k], 1))

    loads = []

    def load(src, dst):
        copy = pltpu.make_async_copy(src, dst, load_sem.at[len(loads)])
        copy.start()
        loads.append(copy)
        return copy

    done = []

    def need(copy):
        if not any(copy is other for other in done):
            copy.wait()
            done.append(copy)

    def got_waits():
        for copy in loads:
            need(copy)

    got_dt = load(dt_hbm, dt_ref)
    got_docs = load(doc_hbm, docs_ref)
    got_taps = [
        load(cx_hbm, taps.at[:, pl.ds(0, ch)]),
        load(cb_hbm, taps.at[:, pl.ds(ch, DSTATE)]),
        load(cc_hbm, taps.at[:, pl.ds(ch + DSTATE, DSTATE)]),
    ]
    got_rows = []
    for m in range(BATCH):
        got_rows.append(
            [
                load(x_hbm.at[m], xbc.at[m, :, pl.ds(0, ch)]),
                load(b_hbm.at[m], xbc.at[m, :, pl.ds(ch, DSTATE)]),
                load(c_hbm.at[m], xbc.at[m, :, pl.ds(ch + DSTATE, DSTATE)]),
            ]
        )
    got_z = load(z_hbm, z_ref)
    got_w = load(w_hbm, w_ref)

    lane = lax.broadcasted_iota(jnp.int32, (LENGTH, 128), 1)

    need(got_docs)
    need(got_dt)
    docs = docs_ref[...].astype(F32)
    head_row = lax.broadcasted_iota(jnp.int32, (16, LENGTH), 0)
    bias = jnp.zeros((16, LENGTH), F32)
    rate = jnp.zeros((16, LENGTH), F32)
    for h in range(nh):
        bias = jnp.where(head_row == h, bias_ref[h], bias)
        rate = jnp.where(head_row == h, rate_ref[h], rate)
    step_rows, log_parts = [], []
    for m in range(BATCH):
        raw = dt_ref[:, m, :]
        if nh < 16:
            raw = jnp.concatenate([raw, jnp.zeros((16 - nh, LENGTH), F32)], axis=0)
        shifted = raw + bias
        step = jnp.maximum(shifted, 0.0) + jnp.log1p(jnp.exp(-jnp.abs(shifted)))
        step_rows.append(step)
        log_parts.append(-(step * rate))
    log_step = jnp.concatenate(log_parts, axis=0)
    hi = log_step.astype(BF16)
    rest = log_step - hi.astype(F32)
    mid = rest.astype(BF16)
    low = (rest - mid.astype(F32)).astype(BF16)
    before = lax.broadcasted_iota(jnp.int32, (LENGTH, LENGTH), 0) <= lax.broadcasted_iota(
        jnp.int32, (LENGTH, LENGTH), 1
    )
    upper = jnp.where(before, 1.0, 0.0).astype(BF16)
    sums = dot(jnp.concatenate([low, mid, hi], axis=0), upper, (((1,), (0,)), ((), ())))
    span = BATCH * 16
    log_cum = sums[0:span] + sums[span : 2 * span] + sums[2 * span : 3 * span]
    log_rows = [log_cum[m * 16 : (m + 1) * 16] for m in range(BATCH)]
    row_mats = list(log_rows)
    ends = []
    for m in range(BATCH):
        end = log_rows[m][:, LENGTH - 1 : LENGTH]
        ends.append(end)
        keep = jnp.where(docs[m : m + 1] == docs[m : m + 1, LENGTH - 1 : LENGTH], 1.0, 0.0)
        row_mats.append(jnp.exp(jnp.minimum(end - log_rows[m], 0.0)) * step_rows[m] * keep)
    for m in range(BATCH):
        row_mats.append(jnp.exp(log_rows[m]))
    marks = []
    for m in range(BATCH):
        own = docs[m : m + 1]
        marks.append(own)
        for k in range(1, TAPS):
            marks.append(jnp.where(pltpu.roll(own, k, 1) == own, 1.0, 0.0))
    row_mats.append(jnp.concatenate(marks + [jnp.zeros((32 - len(marks), LENGTH), F32)], axis=0))
    cols = jnp.concatenate(row_mats, axis=0).T
    log_col, weight_col, entry_col, mark_col = 0, span, 2 * span, 3 * span

    for copy in got_taps:
        need(copy)
    tap = taps[...].astype(F32)
    tiles = plan.conv // 128
    for m in range(BATCH):
        for k in range(1, TAPS):
            at = mark_col + m * TAPS + k
            masks[m, k - 1] = jnp.broadcast_to(cols[:, at : at + 1], (LENGTH, 128))
    def convolve(m):
        for copy in got_rows[m]:
            need(copy)
        for j in range(tiles):
            at = slice(j * 128, (j + 1) * 128)
            rows = xbc[m, :, at].astype(F32)
            total = rows * tap[TAPS - 1 : TAPS, at]
            for k in range(1, TAPS):
                weight = tap[TAPS - 1 - k : TAPS - k, at]
                total = total + (pltpu.roll(rows, k, 0) * weight) * masks[m, k - 1]
            total = silu(total)
            conv[m, :, at] = total.astype(BF16)
            if j < plan.pairs:
                scale = pair_columns(cols, weight_col + m * 16 + 2 * j, lane)
                xw[m, :, at] = (total.astype(BF16).astype(F32) * scale).astype(BF16)

    convolve(0)
    for copy in got_rows[1]:
        need(copy)
    pl.semaphore_wait(barrier, count)
    if plan.reach >= 2:
        pass_word(2)

    halos = []
    for m in range(BATCH):
        halos.append(
            pltpu.make_async_remote_copy(
                src_ref=xbc.at[m, pl.ds(LENGTH - HALO, HALO)],
                dst_ref=halo.at[m],
                send_sem=halo_send.at[m],
                recv_sem=halo_recv.at[m],
                device_id=after,
                device_id_type=pl.DeviceIdType.MESH,
            )
        )
    halos.append(
        pltpu.make_async_remote_copy(
            src_ref=docs_ref.at[:, pl.ds(LENGTH - 128, 128)],
            dst_ref=doc_halo,
            send_sem=halo_send.at[BATCH],
            recv_sem=halo_recv.at[BATCH],
            device_id=after,
            device_id_type=pl.DeviceIdType.MESH,
        )
    )
    def send_halo():
        for copy in (halos[BATCH], *halos[:BATCH]):
            copy.start()

    pl.when(has_next)(send_halo)
    convolve(1)

    def turn_weights():
        need(got_w)
        for j in range(plan.width // 128):
            wt[j * 128 : (j + 1) * 128, :] = w_ref[:, j * 128 : (j + 1) * 128].T

    def gate_inputs(m):
        need(got_z)
        for j in range(plan.pairs):
            at = slice(j * 128, (j + 1) * 128)
            zg[m, :, at] = silu(z_ref[m, :, at].astype(F32))

    pl.when(has_prior)(halos[BATCH].wait_recv)
    doc_before = jnp.where(has_prior, doc_halo[...].astype(F32), -1.0)
    edge_marks = []
    joined = jnp.concatenate([doc_before, docs[:, 0:128]], axis=1)
    for k in range(1, TAPS):
        edge_marks.append(jnp.where(pltpu.roll(joined, k, 1) == joined, 1.0, 0.0))
    edge_rows = jnp.concatenate(
        edge_marks + [jnp.zeros((16 - BATCH * (TAPS - 1), LENGTH), F32)], axis=0
    )[:, 128:256]
    edge_rows = jnp.concatenate([edge_rows, jnp.zeros((112, 128), F32)], axis=0)
    edge_cols = edge_rows.T[0:HALO]

    def exchange(m, source, target, peers_send, peers_recv):
        copies = []
        for k in range(1, ring):
            to = lax.rem(rank + k, ring)
            copies.append(
                pltpu.make_async_remote_copy(
                    src_ref=source.at[m, to],
                    dst_ref=target(to),
                    send_sem=peers_send.at[m, k],
                    recv_sem=peers_recv.at[m, k],
                    device_id=in_plane(to),
                    device_id_type=pl.DeviceIdType.MESH,
                )
            )
        return copies

    group_row = lax.broadcasted_iota(jnp.int32, (ring * plan.gate_rows, 16), 0)
    group_head = lax.broadcasted_iota(jnp.int32, (ring * plan.gate_rows, 16), 1)
    bits = plan.gate_rows.bit_length() - 1
    shard_of, group_of = group_row >> bits, group_row & (plan.gate_rows - 1)
    picks = (((shard_of * plan.groups + group_of) >> 2) == group_head) & (group_of < plan.groups)
    pick = jnp.where(picks, 1.0, 0.0).astype(BF16)
    a_copies = []
    for m in range(BATCH):
        pl.when(has_prior)(halos[m].wait_recv)
        for j in range(tiles):
            at = slice(j * 128, (j + 1) * 128)
            lead = jnp.where(has_prior, halo[m, :, at].astype(F32), 0.0)
            own = xbc[m, 0:HALO, at].astype(F32)
            both = jnp.concatenate([lead, own], axis=0)
            total = own * tap[TAPS - 1 : TAPS, at]
            for k in range(1, TAPS):
                weight = tap[TAPS - 1 - k : TAPS - k, at]
                same = edge_cols[:, (k - 1) * BATCH + m : (k - 1) * BATCH + m + 1]
                total = total + (pltpu.roll(both, k, 0)[HALO : 2 * HALO] * weight) * same
            total = silu(total)
            conv[m, 0:HALO, at] = total.astype(BF16)
            if j < plan.pairs:
                scale = pair_columns(cols[0:HALO], weight_col + m * 16 + 2 * j, lane[0:HALO])
                xw[m, 0:HALO, at] = (total.astype(BF16).astype(F32) * scale).astype(BF16)
        state = dot(xw[m], conv[m, :, ch : ch + DSTATE], ROWS).astype(BF16)
        carried_end = docs[m : m + 1, LENGTH - 1 : LENGTH] == doc_before[m : m + 1, 127:128]
        gate = jnp.broadcast_to(jnp.exp(ends[m]) * jnp.where(carried_end, 1.0, 0.0), (16, DSTATE))
        gate_hi, gate_lo = split_two(gate)
        plain = (((1,), (0,)), ((), ()))
        hi_rows = dot(pick, gate_hi, plain).astype(BF16)
        lo_rows = dot(pick, gate_lo, plain).astype(BF16)
        for r in range(ring):
            fsend[m, r, 0 : plan.shard] = state[r * plan.shard : (r + 1) * plan.shard]
            at = slice(r * plan.gate_rows, (r + 1) * plan.gate_rows)
            fsend[m, r, plan.shard : plan.packet] = jnp.concatenate(
                [hi_rows[at], lo_rows[at]], axis=0
            )
        copies = exchange(m, fsend, lambda to, m=m: arecv.at[m, rank], a_send, a_recv)
        for copy in copies:
            copy.start()
        a_copies.append(copies)
        arecv[m, pl.ds(rank, 1)] = fsend[m, pl.ds(rank, 1)]

    def scores_of(m):
        t_pos = lax.broadcasted_iota(jnp.int32, (LENGTH, LENGTH), 0)
        s_pos = lax.broadcasted_iota(jnp.int32, (LENGTH, LENGTH), 1)
        doc_t = cols[:, mark_col + m * TAPS : mark_col + m * TAPS + 1]
        keep = (s_pos <= t_pos) & (doc_t == docs[m : m + 1])
        full = dot(conv[m, :, ch + DSTATE : ch + 2 * DSTATE], conv[m, :, ch : ch + DSTATE], LANES)
        scores[m] = jnp.where(keep, full, 0.0)

    def inner_of(m):
        low_lane = lane < HEADDIM
        for j in range(plan.pairs):
            at = slice(j * 128, (j + 1) * 128)
            xs = conv[m, :, at]
            xs_a = jnp.where(low_lane, xs, jnp.zeros_like(xs))
            xs_b = jnp.where(low_lane, jnp.zeros_like(xs), xs)
            for half in range(2):
                t0, s1 = half * HALF, (half + 1) * HALF
                base = scores[m, t0 : t0 + HALF, 0:s1]
                mixes = []
                for h in (2 * j, 2 * j + 1):
                    t_log = cols[t0 : t0 + HALF, log_col + m * 16 + h : log_col + m * 16 + h + 1]
                    s_log = log_rows[m][h : h + 1, 0:s1]
                    decay = jnp.exp(jnp.minimum(t_log - s_log, 0.0))
                    mixes.append((base * step_rows[m][h : h + 1, 0:s1] * decay).astype(BF16))
                y[m, t0 : t0 + HALF, at] = dot(
                    jnp.concatenate(mixes, axis=1),
                    jnp.concatenate([xs_a[0:s1], xs_b[0:s1]], axis=0),
                    (((1,), (0,)), ((), ())),
                )

    gate_inputs(0)
    gate_inputs(1)
    if plan.reach >= 2:
        hear_word(2)
    if plan.reach >= 3:
        pass_word(3)
    scores_of(0)
    if plan.reach >= 3:
        hear_word(3)
    if plan.reach >= 4:
        pass_word(4)
    scores_of(1)
    b_copies = []
    for m in range(BATCH):
        for copy in a_copies[m]:
            copy.wait_recv()
        total = jnp.zeros((plan.shard, DSTATE), F32)
        product = jnp.ones((plan.gate_rows, DSTATE), F32)
        for d in range(ring):
            pref[m, d] = total
            qpref[m, d] = product
            packet = arecv[m, d].astype(F32)
            gates = (
                packet[plan.shard : plan.shard + plan.gate_rows]
                + packet[plan.shard + plan.gate_rows :]
            )
            total = spread(gates, plan) * total + packet[0 : plan.shard]
            product = product * gates
        tsend[m, 0 : plan.shard] = total.astype(BF16)
        hi_rows, lo_rows = split_two(product)
        tsend[m, plan.shard : plan.packet] = jnp.concatenate([hi_rows, lo_rows], axis=0)
        copies = []
        if m == 0 and plan.reach >= 4:
            hear_word(4)
        for k in range(1, plan.reach + 1):
            copy = pltpu.make_async_remote_copy(
                src_ref=tsend.at[m],
                dst_ref=brecv.at[m, k - 1],
                send_sem=b_send.at[m, k - 1],
                recv_sem=b_recv.at[m, k - 1],
                device_id={"sz": iz + k},
                device_id_type=pl.DeviceIdType.MESH,
            )
            pl.when(iz + k < plan.planes)(copy.start)
            copies.append(copy)
        b_copies.append(copies)

    turn_weights()
    inner_of(0)
    inner_of(1)
    c_copies = []
    for m in range(BATCH):
        for k in range(plan.reach, 0, -1):
            pl.when(iz >= k)(b_copies[m][k - 1].wait_recv)
        incoming = jnp.zeros((plan.shard, DSTATE), F32)
        for k in range(plan.reach, 0, -1):
            packet = brecv[m, k - 1].astype(F32)
            gates = (
                packet[plan.shard : plan.shard + plan.gate_rows]
                + packet[plan.shard + plan.gate_rows :]
            )
            fresh = jnp.where(iz >= k, packet[0 : plan.shard], 0.0)
            incoming = spread(gates, plan) * incoming + fresh
            incoming = jnp.where(iz >= k, incoming, 0.0)
        for d in range(ring):
            entering = pref[m, d] + spread(qpref[m, d], plan) * incoming
            hsend[m, d] = entering.astype(BF16)
        home = pl.ds(pl.multiple_of(rank * plan.shard, 16), plan.shard)
        copies = exchange(m, hsend, lambda to, m=m: hstate.at[m, home], c_send, c_recv)
        for copy in copies:
            copy.start()
        c_copies.append(copies)
        hstate[m, home] = hsend[m, rank]

    def arrow(chunk, step, upward):
        if upward:
            owner = lax.rem(me + plan.far - step, members)
            first, buffer, send, got, to = 0, up_recv, up_send, up_got, up
        else:
            owner = lax.rem(me + members - plan.far + step, members)
            first, buffer, send, got, to = plan.out // 2, dn_recv, dn_send, dn_got, down
        rows = pl.ds(first, plan.out // 2) if step == 0 else pl.ds(0, plan.out)
        return pltpu.make_async_remote_copy(
            src_ref=part.at[chunk, owner, rows],
            dst_ref=buffer.at[chunk, step, rows],
            send_sem=send.at[chunk, step],
            recv_sem=got.at[chunk, step],
            device_id=to,
            device_id_type=pl.DeviceIdType.MESH,
        )

    arrows = {}
    s_copies = []
    gain = gain_ref[...].reshape(1, ch)
    for m in range(BATCH):
        for copy in c_copies[m]:
            copy.wait_recv()
        carried = cols[:, mark_col + m * TAPS : mark_col + m * TAPS + 1] == doc_before[m : m + 1, 127:128]
        squares = jnp.zeros((LENGTH, 128), F32)
        outer = dot(conv[m, :, ch + DSTATE : ch + 2 * DSTATE], hstate[m], LANES)
        for j in range(plan.pairs):
            at = slice(j * 128, (j + 1) * 128)
            entry = pair_columns(cols, entry_col + m * 16 + 2 * j, lane)
            entry = jnp.where(carried, entry, 0.0)
            mixed = (y[m, :, at] + entry * outer[:, at]) * zg[m, :, at]
            squares = squares + mixed * mixed
            gated[m, :, at] = (mixed * gain[:, at]).astype(BF16)
        square_hi, square_lo = split_two(squares)
        ones = jnp.ones((8, 128), BF16)
        square_rows = dot(ones, square_hi, LANES) + dot(ones, square_lo, LANES)
        ssend[m] = square_rows[0:1]

        def project(owner, m=m):
            rows = pl.ds(pl.multiple_of(owner * plan.out, 16), plan.out)
            tile = dot(wt[rows, :], gated[m], LANES).astype(BF16)
            part[2 * m, owner] = tile[:, 0:HALF]
            part[2 * m + 1, owner] = tile[:, HALF:LENGTH]

        project(lax.rem(me + plan.far, members))
        for chunk in (2 * m, 2 * m + 1):
            for upward in (True, False):
                arrows[chunk, 0, upward] = arrow(chunk, 0, upward)
                arrows[chunk, 0, upward].start()
        for k in range(1, members):
            copy = pltpu.make_async_remote_copy(
                src_ref=ssend.at[m],
                dst_ref=srecv.at[m, k],
                send_sem=s_send.at[m, k],
                recv_sem=s_recv.at[m, k],
                device_id={"mp": lax.rem(me + k, members)},
                device_id_type=pl.DeviceIdType.MESH,
            )
            copy.start()
            s_copies.append(copy)
        for step in range(1, plan.far):
            project(lax.rem(me + plan.far - step, members))
            project(lax.rem(me + members - plan.far + step, members))
        project(me)

    half = plan.out // 2
    chunks = range(2 * BATCH)
    for step in range(1, plan.far):
        for chunk in chunks:
            for upward in (True, False):
                arrows[chunk, step - 1, upward].wait_recv()
                buffer = up_recv if upward else dn_recv
                if upward:
                    owner = lax.rem(me + plan.far - step, members)
                else:
                    owner = lax.rem(me + members - plan.far + step, members)
                if step == 1:
                    rows = slice(0, half) if upward else slice(half, plan.out)
                else:
                    rows = slice(0, plan.out)
                total = part[chunk, owner, rows].astype(F32) + buffer[chunk, step - 1, rows].astype(F32)
                part[chunk, owner, rows] = total.astype(BF16)
                arrows[chunk, step, upward] = arrow(chunk, step, upward)
                arrows[chunk, step, upward].start()

    for copy in s_copies:
        copy.wait_recv()
    last = plan.far - 1
    for m in range(BATCH):
        square = ssend[m]
        for k in range(1, members):
            square = square + srecv[m, k]
        scale = lax.rsqrt(square / INNER + EPSILON)
        for side in range(2):
            chunk = 2 * m + side
            total = part[chunk, me].astype(F32)
            if last == 0:
                arrows[chunk, last, True].wait_recv()
                arrows[chunk, last, False].wait_recv()
                total = total + jnp.concatenate(
                    [up_recv[chunk, 0, 0:half], dn_recv[chunk, 0, half : plan.out]], axis=0
                ).astype(F32)
            else:
                for upward in (True, False):
                    arrows[chunk, last, upward].wait_recv()
                    buffer = up_recv if upward else dn_recv
                    total = total + buffer[chunk, last].astype(F32)
            at = slice(side * HALF, (side + 1) * HALF)
            out_ref[m, :, at] = (total * scale[:, at]).astype(BF16)

    def sent():
        for copy in halos:
            copy.wait_send()

    pl.when(has_next)(sent)
    for group in (*a_copies, *c_copies, s_copies, list(arrows.values())):
        for copy in group:
            copy.wait_send()
    for m in range(BATCH):
        for k in range(1, plan.reach + 1):
            pl.when(iz + k < plan.planes)(b_copies[m][k - 1].wait_send)


def shards(
    plan,
    x_inner,
    z_gate,
    b_input,
    c_input,
    dt_raw,
    doc_ids,
    conv_x,
    conv_b,
    conv_c,
    dt_bias,
    decay_rate,
    norm_gain,
    w_out,
):
    hbm = pl.BlockSpec(memory_space=pltpu.HBM)
    smem = pl.BlockSpec(memory_space=pltpu.SMEM)
    vmem = pl.BlockSpec(memory_space=pltpu.VMEM)
    ch, ring, members = plan.channels, plan.ring, plan.members
    chunks = 2 * BATCH
    dma = pltpu.SemaphoreType.DMA
    reach = max(plan.reach, 1)
    scratch = [
        pltpu.VMEM((BATCH, LENGTH, plan.conv), BF16),
        pltpu.VMEM((BATCH, HALO, plan.conv), BF16),
        pltpu.VMEM((BATCH, LENGTH), jnp.int32),
        pltpu.VMEM((BATCH, 128), jnp.int32),
        pltpu.VMEM((plan.heads, BATCH, LENGTH), F32),
        pltpu.VMEM((TAPS, plan.conv), BF16),
        pltpu.VMEM((BATCH, LENGTH, ch), BF16),
        pltpu.VMEM((ch, plan.width), BF16),
        pltpu.VMEM((plan.width, ch), BF16),
        pltpu.VMEM((BATCH, LENGTH, plan.conv), BF16),
        pltpu.VMEM((BATCH, TAPS - 1, LENGTH, 128), F32),
        pltpu.VMEM((BATCH, LENGTH, ch), BF16),
        pltpu.VMEM((BATCH, LENGTH, ch), F32),
        pltpu.VMEM((BATCH, LENGTH, LENGTH), F32),
        pltpu.VMEM((BATCH, LENGTH, ch), F32),
        pltpu.VMEM((BATCH, LENGTH, ch), BF16),
        pltpu.VMEM((BATCH, ring, plan.packet, DSTATE), BF16),
        pltpu.VMEM((BATCH, ring, plan.packet, DSTATE), BF16),
        pltpu.VMEM((BATCH, ring, plan.shard, DSTATE), F32),
        pltpu.VMEM((BATCH, ring, plan.gate_rows, DSTATE), F32),
        pltpu.VMEM((BATCH, plan.packet, DSTATE), BF16),
        pltpu.VMEM((BATCH, reach, plan.packet, DSTATE), BF16),
        pltpu.VMEM((BATCH, ring, plan.shard, DSTATE), BF16),
        pltpu.VMEM((BATCH, ch, DSTATE), BF16),
        pltpu.VMEM((chunks, members, plan.out, HALF), BF16),
        pltpu.VMEM((chunks, plan.far, plan.out, HALF), BF16),
        pltpu.VMEM((chunks, plan.far, plan.out, HALF), BF16),
        pltpu.VMEM((BATCH, 1, LENGTH), F32),
        pltpu.VMEM((BATCH, members, 1, LENGTH), F32),
        dma((13,)),
        dma((BATCH + 1,)),
        dma((BATCH + 1,)),
        dma((BATCH, ring)),
        dma((BATCH, ring)),
        dma((BATCH, reach)),
        dma((BATCH, reach)),
        dma((BATCH, ring)),
        dma((BATCH, ring)),
        dma((BATCH, members)),
        dma((BATCH, members)),
        dma((chunks, plan.far)),
        dma((chunks, plan.far)),
        dma((chunks, plan.far)),
        dma((chunks, plan.far)),
        pltpu.SemaphoreType.REGULAR((5,)),
    ]
    out = pl.pallas_call(
        functools.partial(layer_kernel, plan),
        name="mixer_layer",
        out_shape=pltpu.VMEM((BATCH, plan.out, LENGTH), BF16),
        in_specs=[hbm] * 9 + [smem, smem, vmem, hbm],
        out_specs=vmem,
        scratch_shapes=scratch,
        compiler_params=pltpu.CompilerParams(
            collective_id=0, has_side_effects=True, vmem_limit_bytes=60 * 1024 * 1024
        ),
    )(
        x_inner,
        z_gate,
        b_input,
        c_input,
        jnp.transpose(dt_raw, (2, 0, 1)),
        doc_ids,
        conv_x,
        conv_b,
        conv_c,
        dt_bias,
        decay_rate,
        norm_gain,
        w_out,
    )
    return jnp.transpose(out, (0, 2, 1))


def solution(mesh):
    members = mesh.shape["mp"]
    line = Mesh(mesh.devices.reshape(*SPLIT, members), (*SEQ, "mp"))

    def layer(*arrays):
        channels = arrays[0].shape[2] // members
        plan = Plan(SPLIT, members, channels, arrays[12].shape[1])
        placed = (
            P(None, SEQ, "mp"),
            P(None, SEQ, "mp"),
            P(None, SEQ, None),
            P(None, SEQ, None),
            P(None, SEQ, "mp"),
            P(None, SEQ),
            P(None, "mp"),
            P(),
            P(),
            P("mp"),
            P("mp"),
            P("mp"),
            P("mp", None),
        )
        return jax.shard_map(
            functools.partial(shards, plan),
            mesh=line,
            in_specs=placed,
            out_specs=P(None, SEQ, "mp"),
            check_vma=False,
        )(*arrays)

    return layer
```

```python
import functools

import jax
import jax.numpy as jnp
from jax import lax
from jax.experimental import pallas as pl
from jax.experimental.pallas import tpu as pltpu
from jax.sharding import Mesh
from jax.sharding import PartitionSpec as P

SPLIT = (8, 4, 2)
SEQ = ("sz", "sx", "sc")
INNER = 5120
EPSILON = 1e-05
BATCH = 2
LENGTH = 256
HALF = 128
HALO = 8
TAPS = 4
HEADDIM = 64
DSTATE = 128
REACH = 8192 // LENGTH
F32 = jnp.float32
BF16 = jnp.bfloat16
LANES = (((1,), (1,)), ((), ()))
ROWS = (((0,), (0,)), ((), ()))


def dot(a, b, dims):
    return lax.dot_general(a, b, dims, preferred_element_type=F32)


def split_two(value):
    high = value.astype(BF16)
    return high, (value - high.astype(F32)).astype(BF16)


def silu(value):
    return value / (1.0 + jnp.exp(-value))


class Plan:
    def __init__(self, split, members, channels, width):
        self.planes, self.xs, self.cores = split
        self.ring = self.xs * self.cores
        self.members = members
        self.channels = channels
        self.heads = channels // HEADDIM
        self.pairs = self.heads // 2
        self.conv = channels + 2 * DSTATE
        self.shard = channels // self.ring
        self.groups = self.shard // 16
        self.gate_rows = 8 if self.groups <= 8 else 16
        self.packet = self.shard + 2 * self.gate_rows
        self.reach = min(-(-REACH // self.ring), self.planes - 1)
        assert self.reach <= 4
        self.width = width
        self.out = width // members
        self.far = members // 2


def spread(rows, plan):
    return jnp.concatenate(
        [jnp.broadcast_to(rows[q : q + 1], (16, DSTATE)) for q in range(plan.groups)], axis=0
    )


def pair_columns(cols, first, lane):
    a = jnp.broadcast_to(cols[:, first : first + 1], (cols.shape[0], 128))
    b = jnp.broadcast_to(cols[:, first + 1 : first + 2], (cols.shape[0], 128))
    return jnp.where(lane < HEADDIM, a, b)


def layer_kernel(
    plan,
    x_hbm,
    z_hbm,
    b_hbm,
    c_hbm,
    dt_hbm,
    doc_hbm,
    cx_hbm,
    cb_hbm,
    cc_hbm,
    bias_ref,
    rate_ref,
    gain_ref,
    w_hbm,
    out_ref,
    xbc,
    halo,
    docs_ref,
    doc_halo,
    dt_ref,
    taps,
    z_ref,
    w_ref,
    wt,
    conv,
    masks,
    xw,
    y,
    scores,
    zg,
    gated,
    fsend,
    arecv,
    pref,
    qpref,
    tsend,
    brecv,
    hsend,
    hstate,
    part,
    up_recv,
    dn_recv,
    ssend,
    srecv,
    load_sem,
    halo_send,
    halo_recv,
    a_send,
    a_recv,
    b_send,
    b_recv,
    c_send,
    c_recv,
    s_send,
    s_recv,
    up_send,
    up_got,
    dn_send,
    dn_got,
    word,
):
    ch, nh, ring, members = plan.channels, plan.heads, plan.ring, plan.members
    iz, ix, ic = lax.axis_index("sz"), lax.axis_index("sx"), lax.axis_index("sc")
    me = lax.axis_index("mp")
    rank = ix * plan.cores + ic
    place = iz * ring + rank
    blocks = plan.planes * ring

    def in_plane(r):
        return {"sx": r // plan.cores, "sc": r % plan.cores}

    def in_line(j):
        return {"sz": j // ring, "sx": (j % ring) // plan.cores, "sc": j % plan.cores}

    after, prior = in_line(place + 1), in_line(place - 1)
    up = {"mp": lax.rem(me + 1, members)}
    down = {"mp": lax.rem(me + members - 1, members)}

    has_next, has_prior = place + 1 < blocks, place > 0

    def one(flag):
        return jnp.where(flag, 1, 0)

    barrier = pltpu.get_barrier_semaphore()

    def greet(peer):
        pl.semaphore_signal(barrier, inc=1, device_id=peer, device_id_type=pl.DeviceIdType.MESH)

    for k in range(1, ring):
        greet(in_plane(lax.rem(rank + k, ring)))
    for k in range(1, members):
        greet({"mp": lax.rem(me + k, members)})
    pl.when(has_prior)(lambda: greet(prior))
    count = ring - 1 + members - 1 + one(has_next)
    above, below = {"sz": iz + 1}, {"sz": iz - 1}
    has_above, has_below = iz + 1 < plan.planes, iz > 0
    pl.when(has_below)(lambda: greet(below))
    pl.when(has_above)(lambda: greet(above))
    count = count + one(has_above) + one(has_below)

    def pass_word(k):
        pl.when(has_below & (iz + k - 1 < plan.planes))(
            lambda: pl.semaphore_signal(
                word.at[k], inc=1, device_id=below, device_id_type=pl.DeviceIdType.MESH
            )
        )

    def hear_word(k):
        pl.when(iz + k < plan.planes)(lambda: pl.semaphore_wait(word.at[k], 1))

    loads = []

    def load(src, dst):
        copy = pltpu.make_async_copy(src, dst, load_sem.at[len(loads)])
        copy.start()
        loads.append(copy)
        return copy

    done = []

    def need(copy):
        if not any(copy is other for other in done):
            copy.wait()
            done.append(copy)

    def got_waits():
        for copy in loads:
            need(copy)

    got_dt = load(dt_hbm, dt_ref)
    got_docs = load(doc_hbm, docs_ref)
    got_taps = [
        load(cx_hbm, taps.at[:, pl.ds(0, ch)]),
        load(cb_hbm, taps.at[:, pl.ds(ch, DSTATE)]),
        load(cc_hbm, taps.at[:, pl.ds(ch + DSTATE, DSTATE)]),
    ]
    got_rows = []
    for m in range(BATCH):
        got_rows.append(
            [
                load(x_hbm.at[m], xbc.at[m, :, pl.ds(0, ch)]),
                load(b_hbm.at[m], xbc.at[m, :, pl.ds(ch, DSTATE)]),
                load(c_hbm.at[m], xbc.at[m, :, pl.ds(ch + DSTATE, DSTATE)]),
            ]
        )
    got_z = load(z_hbm, z_ref)
    got_w = load(w_hbm, w_ref)

    lane = lax.broadcasted_iota(jnp.int32, (LENGTH, 128), 1)

    need(got_docs)
    need(got_dt)
    docs = docs_ref[...].astype(F32)
    head_row = lax.broadcasted_iota(jnp.int32, (16, LENGTH), 0)
    bias = jnp.zeros((16, LENGTH), F32)
    rate = jnp.zeros((16, LENGTH), F32)
    for h in range(nh):
        bias = jnp.where(head_row == h, bias_ref[h], bias)
        rate = jnp.where(head_row == h, rate_ref[h], rate)
    step_rows, log_parts = [], []
    for m in range(BATCH):
        raw = dt_ref[:, m, :]
        if nh < 16:
            raw = jnp.concatenate([raw, jnp.zeros((16 - nh, LENGTH), F32)], axis=0)
        shifted = raw + bias
        step = jnp.maximum(shifted, 0.0) + jnp.log1p(jnp.exp(-jnp.abs(shifted)))
        step_rows.append(step)
        log_parts.append(-(step * rate))
    log_step = jnp.concatenate(log_parts, axis=0)
    hi = log_step.astype(BF16)
    rest = log_step - hi.astype(F32)
    mid = rest.astype(BF16)
    low = (rest - mid.astype(F32)).astype(BF16)
    before = lax.broadcasted_iota(jnp.int32, (LENGTH, LENGTH), 0) <= lax.broadcasted_iota(
        jnp.int32, (LENGTH, LENGTH), 1
    )
    upper = jnp.where(before, 1.0, 0.0).astype(BF16)
    sums = dot(jnp.concatenate([low, mid, hi], axis=0), upper, (((1,), (0,)), ((), ())))
    span = BATCH * 16
    log_cum = sums[0:span] + sums[span : 2 * span] + sums[2 * span : 3 * span]
    log_rows = [log_cum[m * 16 : (m + 1) * 16] for m in range(BATCH)]
    row_mats = list(log_rows)
    ends = []
    for m in range(BATCH):
        end = log_rows[m][:, LENGTH - 1 : LENGTH]
        ends.append(end)
        keep = jnp.where(docs[m : m + 1] == docs[m : m + 1, LENGTH - 1 : LENGTH], 1.0, 0.0)
        row_mats.append(jnp.exp(jnp.minimum(end - log_rows[m], 0.0)) * step_rows[m] * keep)
    for m in range(BATCH):
        row_mats.append(jnp.exp(log_rows[m]))
    marks = []
    for m in range(BATCH):
        own = docs[m : m + 1]
        marks.append(own)
        for k in range(1, TAPS):
            marks.append(jnp.where(pltpu.roll(own, k, 1) == own, 1.0, 0.0))
    row_mats.append(jnp.concatenate(marks + [jnp.zeros((32 - len(marks), LENGTH), F32)], axis=0))
    cols = jnp.concatenate(row_mats, axis=0).T
    log_col, weight_col, entry_col, mark_col = 0, span, 2 * span, 3 * span

    for copy in got_taps:
        need(copy)
    tap = taps[...].astype(F32)
    tiles = plan.conv // 128
    for m in range(BATCH):
        for k in range(1, TAPS):
            at = mark_col + m * TAPS + k
            masks[m, k - 1] = jnp.broadcast_to(cols[:, at : at + 1], (LENGTH, 128))
    def convolve(m):
        for copy in got_rows[m]:
            need(copy)
        for j in range(tiles):
            at = slice(j * 128, (j + 1) * 128)
            rows = xbc[m, :, at].astype(F32)
            total = rows * tap[TAPS - 1 : TAPS, at]
            for k in range(1, TAPS):
                weight = tap[TAPS - 1 - k : TAPS - k, at]
                total = total + (pltpu.roll(rows, k, 0) * weight) * masks[m, k - 1]
            total = silu(total)
            conv[m, :, at] = total.astype(BF16)
            if j < plan.pairs:
                scale = pair_columns(cols, weight_col + m * 16 + 2 * j, lane)
                xw[m, :, at] = (total.astype(BF16).astype(F32) * scale).astype(BF16)

    convolve(0)
    for copy in got_rows[1]:
        need(copy)
    pl.semaphore_wait(barrier, count)
    if plan.reach >= 2:
        pass_word(2)

    halos = []
    for m in range(BATCH):
        halos.append(
            pltpu.make_async_remote_copy(
                src_ref=xbc.at[m, pl.ds(LENGTH - HALO, HALO)],
                dst_ref=halo.at[m],
                send_sem=halo_send.at[m],
                recv_sem=halo_recv.at[m],
                device_id=after,
                device_id_type=pl.DeviceIdType.MESH,
            )
        )
    halos.append(
        pltpu.make_async_remote_copy(
            src_ref=docs_ref.at[:, pl.ds(LENGTH - 128, 128)],
            dst_ref=doc_halo,
            send_sem=halo_send.at[BATCH],
            recv_sem=halo_recv.at[BATCH],
            device_id=after,
            device_id_type=pl.DeviceIdType.MESH,
        )
    )
    def send_halo():
        for copy in (halos[BATCH], *halos[:BATCH]):
            copy.start()

    pl.when(has_next)(send_halo)
    convolve(1)

    def turn_weights():
        need(got_w)
        for j in range(plan.width // 128):
            wt[j * 128 : (j + 1) * 128, :] = w_ref[:, j * 128 : (j + 1) * 128].T

    def gate_inputs(m):
        need(got_z)
        for j in range(plan.pairs):
            at = slice(j * 128, (j + 1) * 128)
            zg[m, :, at] = silu(z_ref[m, :, at].astype(F32))

    pl.when(has_prior)(halos[BATCH].wait_recv)
    doc_before = jnp.where(has_prior, doc_halo[...].astype(F32), -1.0)
    edge_marks = []
    joined = jnp.concatenate([doc_before, docs[:, 0:128]], axis=1)
    for k in range(1, TAPS):
        edge_marks.append(jnp.where(pltpu.roll(joined, k, 1) == joined, 1.0, 0.0))
    edge_rows = jnp.concatenate(
        edge_marks + [jnp.zeros((16 - BATCH * (TAPS - 1), LENGTH), F32)], axis=0
    )[:, 128:256]
    edge_rows = jnp.concatenate([edge_rows, jnp.zeros((112, 128), F32)], axis=0)
    edge_cols = edge_rows.T[0:HALO]

    def exchange(m, source, target, peers_send, peers_recv):
        copies = []
        for k in range(1, ring):
            to = lax.rem(rank + k, ring)
            copies.append(
                pltpu.make_async_remote_copy(
                    src_ref=source.at[m, to],
                    dst_ref=target(to),
                    send_sem=peers_send.at[m, k],
                    recv_sem=peers_recv.at[m, k],
                    device_id=in_plane(to),
                    device_id_type=pl.DeviceIdType.MESH,
                )
            )
        return copies

    group_row = lax.broadcasted_iota(jnp.int32, (ring * plan.gate_rows, 16), 0)
    group_head = lax.broadcasted_iota(jnp.int32, (ring * plan.gate_rows, 16), 1)
    bits = plan.gate_rows.bit_length() - 1
    shard_of, group_of = group_row >> bits, group_row & (plan.gate_rows - 1)
    picks = (((shard_of * plan.groups + group_of) >> 2) == group_head) & (group_of < plan.groups)
    pick = jnp.where(picks, 1.0, 0.0).astype(BF16)
    a_copies = []
    for m in range(BATCH):
        pl.when(has_prior)(halos[m].wait_recv)
        for j in range(tiles):
            at = slice(j * 128, (j + 1) * 128)
            lead = jnp.where(has_prior, halo[m, :, at].astype(F32), 0.0)
            own = xbc[m, 0:HALO, at].astype(F32)
            both = jnp.concatenate([lead, own], axis=0)
            total = own * tap[TAPS - 1 : TAPS, at]
            for k in range(1, TAPS):
                weight = tap[TAPS - 1 - k : TAPS - k, at]
                same = edge_cols[:, (k - 1) * BATCH + m : (k - 1) * BATCH + m + 1]
                total = total + (pltpu.roll(both, k, 0)[HALO : 2 * HALO] * weight) * same
            total = silu(total)
            conv[m, 0:HALO, at] = total.astype(BF16)
            if j < plan.pairs:
                scale = pair_columns(cols[0:HALO], weight_col + m * 16 + 2 * j, lane[0:HALO])
                xw[m, 0:HALO, at] = (total.astype(BF16).astype(F32) * scale).astype(BF16)
        state = dot(xw[m], conv[m, :, ch : ch + DSTATE], ROWS).astype(BF16)
        carried_end = docs[m : m + 1, LENGTH - 1 : LENGTH] == doc_before[m : m + 1, 127:128]
        gate = jnp.broadcast_to(jnp.exp(ends[m]) * jnp.where(carried_end, 1.0, 0.0), (16, DSTATE))
        gate_hi, gate_lo = split_two(gate)
        plain = (((1,), (0,)), ((), ()))
        hi_rows = dot(pick, gate_hi, plain).astype(BF16)
        lo_rows = dot(pick, gate_lo, plain).astype(BF16)
        for r in range(ring):
            fsend[m, r, 0 : plan.shard] = state[r * plan.shard : (r + 1) * plan.shard]
            at = slice(r * plan.gate_rows, (r + 1) * plan.gate_rows)
            fsend[m, r, plan.shard : plan.packet] = jnp.concatenate(
                [hi_rows[at], lo_rows[at]], axis=0
            )
        copies = exchange(m, fsend, lambda to, m=m: arecv.at[m, rank], a_send, a_recv)
        for copy in copies:
            copy.start()
        a_copies.append(copies)
        arecv[m, pl.ds(rank, 1)] = fsend[m, pl.ds(rank, 1)]

    def scores_of(m):
        t_pos = lax.broadcasted_iota(jnp.int32, (LENGTH, LENGTH), 0)
        s_pos = lax.broadcasted_iota(jnp.int32, (LENGTH, LENGTH), 1)
        doc_t = cols[:, mark_col + m * TAPS : mark_col + m * TAPS + 1]
        keep = (s_pos <= t_pos) & (doc_t == docs[m : m + 1])
        full = dot(conv[m, :, ch + DSTATE : ch + 2 * DSTATE], conv[m, :, ch : ch + DSTATE], LANES)
        scores[m] = jnp.where(keep, full, 0.0)

    def inner_of(m):
        low_lane = lane < HEADDIM
        for j in range(plan.pairs):
            at = slice(j * 128, (j + 1) * 128)
            xs = conv[m, :, at]
            xs_a = jnp.where(low_lane, xs, jnp.zeros_like(xs))
            xs_b = jnp.where(low_lane, jnp.zeros_like(xs), xs)
            for half in range(2):
                t0, s1 = half * HALF, (half + 1) * HALF
                base = scores[m, t0 : t0 + HALF, 0:s1]
                mixes = []
                for h in (2 * j, 2 * j + 1):
                    t_log = cols[t0 : t0 + HALF, log_col + m * 16 + h : log_col + m * 16 + h + 1]
                    s_log = log_rows[m][h : h + 1, 0:s1]
                    decay = jnp.exp(jnp.minimum(t_log - s_log, 0.0))
                    mixes.append((base * step_rows[m][h : h + 1, 0:s1] * decay).astype(BF16))
                y[m, t0 : t0 + HALF, at] = dot(
                    jnp.concatenate(mixes, axis=1),
                    jnp.concatenate([xs_a[0:s1], xs_b[0:s1]], axis=0),
                    (((1,), (0,)), ((), ())),
                )

    def gate_both(m):
        carried = cols[:, mark_col + m * TAPS : mark_col + m * TAPS + 1] == doc_before[m : m + 1, 127:128]
        for j in range(plan.pairs):
            at = slice(j * 128, (j + 1) * 128)
            opened = zg[m, :, at]
            y[m, :, at] = y[m, :, at] * opened
            entry = pair_columns(cols, entry_col + m * 16 + 2 * j, lane)
            zg[m, :, at] = jnp.where(carried, entry, 0.0) * opened

    gate_inputs(0)
    gate_inputs(1)
    if plan.reach >= 2:
        hear_word(2)
    if plan.reach >= 3:
        pass_word(3)
    scores_of(0)
    if plan.reach >= 3:
        hear_word(3)
    if plan.reach >= 4:
        pass_word(4)
    scores_of(1)
    b_copies = []
    for m in range(BATCH):
        for copy in a_copies[m]:
            copy.wait_recv()
        total = jnp.zeros((plan.shard, DSTATE), F32)
        product = jnp.ones((plan.gate_rows, DSTATE), F32)
        for d in range(ring):
            pref[m, d] = total
            qpref[m, d] = product
            packet = arecv[m, d].astype(F32)
            gates = (
                packet[plan.shard : plan.shard + plan.gate_rows]
                + packet[plan.shard + plan.gate_rows :]
            )
            total = spread(gates, plan) * total + packet[0 : plan.shard]
            product = product * gates
        tsend[m, 0 : plan.shard] = total.astype(BF16)
        hi_rows, lo_rows = split_two(product)
        tsend[m, plan.shard : plan.packet] = jnp.concatenate([hi_rows, lo_rows], axis=0)
        copies = []
        if m == 0 and plan.reach >= 4:
            hear_word(4)
        for k in range(1, plan.reach + 1):
            copy = pltpu.make_async_remote_copy(
                src_ref=tsend.at[m],
                dst_ref=brecv.at[m, k - 1],
                send_sem=b_send.at[m, k - 1],
                recv_sem=b_recv.at[m, k - 1],
                device_id={"sz": iz + k},
                device_id_type=pl.DeviceIdType.MESH,
            )
            pl.when(iz + k < plan.planes)(copy.start)
            copies.append(copy)
        b_copies.append(copies)

    turn_weights()
    inner_of(0)
    gate_both(0)
    inner_of(1)
    gate_both(1)
    c_copies = []
    for m in range(BATCH):
        for k in range(plan.reach, 0, -1):
            pl.when(iz >= k)(b_copies[m][k - 1].wait_recv)
        incoming = jnp.zeros((plan.shard, DSTATE), F32)
        for k in range(plan.reach, 0, -1):
            packet = brecv[m, k - 1].astype(F32)
            gates = (
                packet[plan.shard : plan.shard + plan.gate_rows]
                + packet[plan.shard + plan.gate_rows :]
            )
            fresh = jnp.where(iz >= k, packet[0 : plan.shard], 0.0)
            incoming = spread(gates, plan) * incoming + fresh
            incoming = jnp.where(iz >= k, incoming, 0.0)
        for d in range(ring):
            entering = pref[m, d] + spread(qpref[m, d], plan) * incoming
            hsend[m, d] = entering.astype(BF16)
        home = pl.ds(pl.multiple_of(rank * plan.shard, 16), plan.shard)
        copies = exchange(m, hsend, lambda to, m=m: hstate.at[m, home], c_send, c_recv)
        for copy in copies:
            copy.start()
        c_copies.append(copies)
        hstate[m, home] = hsend[m, rank]

    def arrow(chunk, step, upward):
        if upward:
            owner = lax.rem(me + plan.far - step, members)
            first, buffer, send, got, to = 0, up_recv, up_send, up_got, up
        else:
            owner = lax.rem(me + members - plan.far + step, members)
            first, buffer, send, got, to = plan.out // 2, dn_recv, dn_send, dn_got, down
        rows = pl.ds(first, plan.out // 2) if step == 0 else pl.ds(0, plan.out)
        return pltpu.make_async_remote_copy(
            src_ref=part.at[chunk, owner, rows],
            dst_ref=buffer.at[chunk, step, rows],
            send_sem=send.at[chunk, step],
            recv_sem=got.at[chunk, step],
            device_id=to,
            device_id_type=pl.DeviceIdType.MESH,
        )

    arrows = {}
    s_copies = []
    gain = gain_ref[...].reshape(1, ch)

    def project(m, owner):
        rows = pl.ds(pl.multiple_of(owner * plan.out, 16), plan.out)
        tile = dot(wt[rows, :], gated[m], LANES).astype(BF16)
        part[2 * m, owner] = tile[:, 0:HALF]
        part[2 * m + 1, owner] = tile[:, HALF:LENGTH]

    def carry(m):
        for copy in c_copies[m]:
            copy.wait_recv()
        squares = jnp.zeros((LENGTH, 128), F32)
        outer = dot(conv[m, :, ch + DSTATE : ch + 2 * DSTATE], hstate[m], LANES)
        for j in range(plan.pairs):
            at = slice(j * 128, (j + 1) * 128)
            mixed = y[m, :, at] + zg[m, :, at] * outer[:, at]
            squares = squares + mixed * mixed
            gated[m, :, at] = (mixed * gain[:, at]).astype(BF16)
        project(m, lax.rem(me + plan.far, members))
        for chunk in (2 * m, 2 * m + 1):
            for upward in (True, False):
                arrows[chunk, 0, upward] = arrow(chunk, 0, upward)
                arrows[chunk, 0, upward].start()
        square_hi, square_lo = split_two(squares)
        ones = jnp.ones((8, 128), BF16)
        square_rows = dot(ones, square_hi, LANES) + dot(ones, square_lo, LANES)
        ssend[m] = square_rows[0:1]
        for k in range(1, members):
            copy = pltpu.make_async_remote_copy(
                src_ref=ssend.at[m],
                dst_ref=srecv.at[m, k],
                send_sem=s_send.at[m, k],
                recv_sem=s_recv.at[m, k],
                device_id={"mp": lax.rem(me + k, members)},
                device_id_type=pl.DeviceIdType.MESH,
            )
            copy.start()
            s_copies.append(copy)

    half = plan.out // 2

    def ring_step(m, step):
        owners = {
            True: lax.rem(me + plan.far - step, members),
            False: lax.rem(me + members - plan.far + step, members),
        }
        for upward in (True, False):
            project(m, owners[upward])
        for chunk in (2 * m, 2 * m + 1):
            for upward in (True, False):
                arrows[chunk, step - 1, upward].wait_recv()
                buffer = up_recv if upward else dn_recv
                owner = owners[upward]
                if step == 1:
                    rows = slice(0, half) if upward else slice(half, plan.out)
                else:
                    rows = slice(0, plan.out)
                total = part[chunk, owner, rows].astype(F32) + buffer[chunk, step - 1, rows].astype(F32)
                part[chunk, owner, rows] = total.astype(BF16)
                arrows[chunk, step, upward] = arrow(chunk, step, upward)
                arrows[chunk, step, upward].start()

    carry(0)
    if plan.far > 1:
        ring_step(0, 1)
    carry(1)
    for step in range(1, plan.far):
        if step > 1:
            ring_step(0, step)
        ring_step(1, step)
    for m in range(BATCH):
        project(m, me)

    for copy in s_copies:
        copy.wait_recv()
    last = plan.far - 1
    for m in range(BATCH):
        square = ssend[m]
        for k in range(1, members):
            square = square + srecv[m, k]
        scale = lax.rsqrt(square / INNER + EPSILON)
        for side in range(2):
            chunk = 2 * m + side
            total = part[chunk, me].astype(F32)
            if last == 0:
                arrows[chunk, last, True].wait_recv()
                arrows[chunk, last, False].wait_recv()
                total = total + jnp.concatenate(
                    [up_recv[chunk, 0, 0:half], dn_recv[chunk, 0, half : plan.out]], axis=0
                ).astype(F32)
            else:
                for upward in (True, False):
                    arrows[chunk, last, upward].wait_recv()
                    buffer = up_recv if upward else dn_recv
                    total = total + buffer[chunk, last].astype(F32)
            at = slice(side * HALF, (side + 1) * HALF)
            out_ref[m, :, at] = (total * scale[:, at]).astype(BF16)

    def sent():
        for copy in halos:
            copy.wait_send()

    pl.when(has_next)(sent)
    for group in (*a_copies, *c_copies, s_copies, list(arrows.values())):
        for copy in group:
            copy.wait_send()
    for m in range(BATCH):
        for k in range(1, plan.reach + 1):
            pl.when(iz + k < plan.planes)(b_copies[m][k - 1].wait_send)


def shards(
    plan,
    x_inner,
    z_gate,
    b_input,
    c_input,
    dt_raw,
    doc_ids,
    conv_x,
    conv_b,
    conv_c,
    dt_bias,
    decay_rate,
    norm_gain,
    w_out,
):
    hbm = pl.BlockSpec(memory_space=pltpu.HBM)
    smem = pl.BlockSpec(memory_space=pltpu.SMEM)
    vmem = pl.BlockSpec(memory_space=pltpu.VMEM)
    ch, ring, members = plan.channels, plan.ring, plan.members
    chunks = 2 * BATCH
    dma = pltpu.SemaphoreType.DMA
    reach = max(plan.reach, 1)
    scratch = [
        pltpu.VMEM((BATCH, LENGTH, plan.conv), BF16),
        pltpu.VMEM((BATCH, HALO, plan.conv), BF16),
        pltpu.VMEM((BATCH, LENGTH), jnp.int32),
        pltpu.VMEM((BATCH, 128), jnp.int32),
        pltpu.VMEM((plan.heads, BATCH, LENGTH), F32),
        pltpu.VMEM((TAPS, plan.conv), BF16),
        pltpu.VMEM((BATCH, LENGTH, ch), BF16),
        pltpu.VMEM((ch, plan.width), BF16),
        pltpu.VMEM((plan.width, ch), BF16),
        pltpu.VMEM((BATCH, LENGTH, plan.conv), BF16),
        pltpu.VMEM((BATCH, TAPS - 1, LENGTH, 128), F32),
        pltpu.VMEM((BATCH, LENGTH, ch), BF16),
        pltpu.VMEM((BATCH, LENGTH, ch), F32),
        pltpu.VMEM((BATCH, LENGTH, LENGTH), F32),
        pltpu.VMEM((BATCH, LENGTH, ch), F32),
        pltpu.VMEM((BATCH, LENGTH, ch), BF16),
        pltpu.VMEM((BATCH, ring, plan.packet, DSTATE), BF16),
        pltpu.VMEM((BATCH, ring, plan.packet, DSTATE), BF16),
        pltpu.VMEM((BATCH, ring, plan.shard, DSTATE), F32),
        pltpu.VMEM((BATCH, ring, plan.gate_rows, DSTATE), F32),
        pltpu.VMEM((BATCH, plan.packet, DSTATE), BF16),
        pltpu.VMEM((BATCH, reach, plan.packet, DSTATE), BF16),
        pltpu.VMEM((BATCH, ring, plan.shard, DSTATE), BF16),
        pltpu.VMEM((BATCH, ch, DSTATE), BF16),
        pltpu.VMEM((chunks, members, plan.out, HALF), BF16),
        pltpu.VMEM((chunks, plan.far, plan.out, HALF), BF16),
        pltpu.VMEM((chunks, plan.far, plan.out, HALF), BF16),
        pltpu.VMEM((BATCH, 1, LENGTH), F32),
        pltpu.VMEM((BATCH, members, 1, LENGTH), F32),
        dma((13,)),
        dma((BATCH + 1,)),
        dma((BATCH + 1,)),
        dma((BATCH, ring)),
        dma((BATCH, ring)),
        dma((BATCH, reach)),
        dma((BATCH, reach)),
        dma((BATCH, ring)),
        dma((BATCH, ring)),
        dma((BATCH, members)),
        dma((BATCH, members)),
        dma((chunks, plan.far)),
        dma((chunks, plan.far)),
        dma((chunks, plan.far)),
        dma((chunks, plan.far)),
        pltpu.SemaphoreType.REGULAR((5,)),
    ]
    out = pl.pallas_call(
        functools.partial(layer_kernel, plan),
        name="mixer_layer",
        out_shape=pltpu.VMEM((BATCH, plan.out, LENGTH), BF16),
        in_specs=[hbm] * 9 + [smem, smem, vmem, hbm],
        out_specs=vmem,
        scratch_shapes=scratch,
        compiler_params=pltpu.CompilerParams(
            collective_id=0, has_side_effects=True, vmem_limit_bytes=60 * 1024 * 1024
        ),
    )(
        x_inner,
        z_gate,
        b_input,
        c_input,
        jnp.transpose(dt_raw, (2, 0, 1)),
        doc_ids,
        conv_x,
        conv_b,
        conv_c,
        dt_bias,
        decay_rate,
        norm_gain,
        w_out,
    )
    return jnp.transpose(out, (0, 2, 1))


def solution(mesh):
    members = mesh.shape["mp"]
    line = Mesh(mesh.devices.reshape(*SPLIT, members), (*SEQ, "mp"))

    def layer(*arrays):
        channels = arrays[0].shape[2] // members
        plan = Plan(SPLIT, members, channels, arrays[12].shape[1])
        placed = (
            P(None, SEQ, "mp"),
            P(None, SEQ, "mp"),
            P(None, SEQ, None),
            P(None, SEQ, None),
            P(None, SEQ, "mp"),
            P(None, SEQ),
            P(None, "mp"),
            P(),
            P(),
            P("mp"),
            P("mp"),
            P("mp"),
            P("mp", None),
        )
        return jax.shard_map(
            functools.partial(shards, plan),
            mesh=line,
            in_specs=placed,
            out_specs=P(None, SEQ, "mp"),
            check_vma=False,
        )(*arrays)

    return layer
```

```python
import functools

import jax
import jax.numpy as jnp
from jax import lax
from jax.experimental import pallas as pl
from jax.experimental.pallas import tpu as pltpu
from jax.sharding import Mesh
from jax.sharding import PartitionSpec as P

SPLIT = (8, 4, 2)
SEQ = ("sz", "sx", "sc")
INNER = 5120
EPSILON = 1e-05
BATCH = 2
LENGTH = 256
HALF = 128
HALO = 8
TAPS = 4
HEADDIM = 64
DSTATE = 128
REACH = 8192 // LENGTH
F32 = jnp.float32
BF16 = jnp.bfloat16
LANES = (((1,), (1,)), ((), ()))
ROWS = (((0,), (0,)), ((), ()))


def dot(a, b, dims):
    return lax.dot_general(a, b, dims, preferred_element_type=F32)


def split_two(value):
    high = value.astype(BF16)
    return high, (value - high.astype(F32)).astype(BF16)


def silu(value):
    return value / (1.0 + jnp.exp(-value))


class Plan:
    def __init__(self, split, members, channels, width):
        self.planes, self.xs, self.cores = split
        self.ring = self.xs * self.cores
        self.members = members
        self.channels = channels
        self.heads = channels // HEADDIM
        self.pairs = self.heads // 2
        self.conv = channels + 2 * DSTATE
        self.shard = channels // self.ring
        self.groups = self.shard // 16
        self.gate_rows = max(8, 1 << (self.groups - 1).bit_length())
        self.packet = self.shard + 2 * self.gate_rows
        assert REACH <= 4 * self.ring or self.planes <= 5
        self.width = width
        self.out = width // members
        self.far = members // 2


def spread(rows, plan):
    return jnp.concatenate(
        [jnp.broadcast_to(rows[q : q + 1], (16, DSTATE)) for q in range(plan.groups)], axis=0
    )


def pair_columns(cols, first, lane):
    a = jnp.broadcast_to(cols[:, first : first + 1], (cols.shape[0], 128))
    b = jnp.broadcast_to(cols[:, first + 1 : first + 2], (cols.shape[0], 128))
    return jnp.where(lane < HEADDIM, a, b)


def layer_kernel(
    plan,
    x_hbm,
    z_hbm,
    b_hbm,
    c_hbm,
    dt_hbm,
    doc_hbm,
    cx_hbm,
    cb_hbm,
    cc_hbm,
    bias_ref,
    rate_ref,
    gain_ref,
    w_hbm,
    out_ref,
    xbc,
    halo,
    docs_ref,
    doc_halo,
    dt_ref,
    taps,
    z_ref,
    w_ref,
    wt,
    conv,
    masks,
    xw,
    y,
    scores,
    zg,
    gated,
    fsend,
    arecv,
    pref,
    qpref,
    tsend,
    usend,
    ptot,
    qtot,
    brecv,
    hsend,
    hstate,
    part,
    up_recv,
    dn_recv,
    ssend,
    srecv,
    load_sem,
    halo_send,
    halo_recv,
    a_send,
    a_recv,
    b_send,
    b_recv,
    c_send,
    c_recv,
    s_send,
    s_recv,
    up_send,
    up_got,
    dn_send,
    dn_got,
    word,
):
    ch, nh, ring, members = plan.channels, plan.heads, plan.ring, plan.members
    iz, ix, ic = lax.axis_index("sz"), lax.axis_index("sx"), lax.axis_index("sc")
    me = lax.axis_index("mp")
    rank = ix * plan.cores + ic
    place = iz * ring + rank
    blocks = plan.planes * ring

    def in_plane(r):
        return {"sx": r // plan.cores, "sc": r % plan.cores}

    def in_line(j):
        return {"sz": j // ring, "sx": (j % ring) // plan.cores, "sc": j % plan.cores}

    after, prior = in_line(place + 1), in_line(place - 1)
    up = {"mp": lax.rem(me + 1, members)}
    down = {"mp": lax.rem(me + members - 1, members)}

    has_next, has_prior = place + 1 < blocks, place > 0

    def one(flag):
        return jnp.where(flag, 1, 0)

    barrier = pltpu.get_barrier_semaphore()

    def greet(peer):
        pl.semaphore_signal(barrier, inc=1, device_id=peer, device_id_type=pl.DeviceIdType.MESH)

    for k in range(1, ring):
        greet(in_plane(lax.rem(rank + k, ring)))
    for k in range(1, members):
        greet({"mp": lax.rem(me + k, members)})
    pl.when(has_prior)(lambda: greet(prior))
    count = ring - 1 + members - 1 + one(has_next)
    above, below = {"sz": iz + 1}, {"sz": iz - 1}
    has_above, has_below = iz + 1 < plan.planes, iz > 0
    pl.when(has_below)(lambda: greet(below))
    pl.when(has_above)(lambda: greet(above))
    count = count + one(has_above) + one(has_below)

    def tell_below(at):
        pl.semaphore_signal(
            word.at[at], inc=1, device_id=below, device_id_type=pl.DeviceIdType.MESH
        )

    loads = []

    def load(src, dst):
        copy = pltpu.make_async_copy(src, dst, load_sem.at[len(loads)])
        copy.start()
        loads.append(copy)
        return copy

    done = []

    def need(copy):
        if not any(copy is other for other in done):
            copy.wait()
            done.append(copy)

    def got_waits():
        for copy in loads:
            need(copy)

    got_dt = load(dt_hbm, dt_ref)
    got_docs = load(doc_hbm, docs_ref)
    got_taps = [
        load(cx_hbm, taps.at[:, pl.ds(0, ch)]),
        load(cb_hbm, taps.at[:, pl.ds(ch, DSTATE)]),
        load(cc_hbm, taps.at[:, pl.ds(ch + DSTATE, DSTATE)]),
    ]
    got_rows = []
    for m in range(BATCH):
        got_rows.append(
            [
                load(x_hbm.at[m], xbc.at[m, :, pl.ds(0, ch)]),
                load(b_hbm.at[m], xbc.at[m, :, pl.ds(ch, DSTATE)]),
                load(c_hbm.at[m], xbc.at[m, :, pl.ds(ch + DSTATE, DSTATE)]),
            ]
        )
    got_z = load(z_hbm, z_ref)
    got_w = load(w_hbm, w_ref)

    need(got_docs)
    for copy in (*got_rows[0], *got_rows[1]):
        need(copy)
    pl.semaphore_wait(barrier, count)
    pl.when(has_below & has_above)(lambda: tell_below(0))

    halos = []
    for m in range(BATCH):
        halos.append(
            pltpu.make_async_remote_copy(
                src_ref=xbc.at[m, pl.ds(LENGTH - HALO, HALO)],
                dst_ref=halo.at[m],
                send_sem=halo_send.at[m],
                recv_sem=halo_recv.at[m],
                device_id=after,
                device_id_type=pl.DeviceIdType.MESH,
            )
        )
    halos.append(
        pltpu.make_async_remote_copy(
            src_ref=docs_ref.at[:, pl.ds(LENGTH - 128, 128)],
            dst_ref=doc_halo,
            send_sem=halo_send.at[BATCH],
            recv_sem=halo_recv.at[BATCH],
            device_id=after,
            device_id_type=pl.DeviceIdType.MESH,
        )
    )
    def send_halo():
        for copy in (halos[BATCH], *halos[:BATCH]):
            copy.start()

    pl.when(has_next)(send_halo)

    lane = lax.broadcasted_iota(jnp.int32, (LENGTH, 128), 1)

    docs = docs_ref[...].astype(F32)
    marks = []
    for m in range(BATCH):
        own = docs[m : m + 1]
        marks.append(own)
        for k in range(1, TAPS):
            marks.append(jnp.where(pltpu.roll(own, k, 1) == own, 1.0, 0.0))
    mark_cols = jnp.concatenate(marks, axis=0).T
    for m in range(BATCH):
        for k in range(1, TAPS):
            at = m * TAPS + k
            masks[m, k - 1] = jnp.broadcast_to(mark_cols[:, at : at + 1], (LENGTH, 128))
    need(got_dt)
    head_row = lax.broadcasted_iota(jnp.int32, (16, LENGTH), 0)
    bias = jnp.zeros((16, LENGTH), F32)
    rate = jnp.zeros((16, LENGTH), F32)
    for h in range(nh):
        bias = jnp.where(head_row == h, bias_ref[h], bias)
        rate = jnp.where(head_row == h, rate_ref[h], rate)
    step_rows, log_parts = [], []
    for m in range(BATCH):
        raw = dt_ref[:, m, :]
        if nh < 16:
            raw = jnp.concatenate([raw, jnp.zeros((16 - nh, LENGTH), F32)], axis=0)
        shifted = raw + bias
        step = jnp.maximum(shifted, 0.0) + jnp.log1p(jnp.exp(-jnp.abs(shifted)))
        step_rows.append(step)
        log_parts.append(-(step * rate))
    log_step = jnp.concatenate(log_parts, axis=0)
    hi = log_step.astype(BF16)
    rest = log_step - hi.astype(F32)
    mid = rest.astype(BF16)
    low = (rest - mid.astype(F32)).astype(BF16)
    before = lax.broadcasted_iota(jnp.int32, (LENGTH, LENGTH), 0) <= lax.broadcasted_iota(
        jnp.int32, (LENGTH, LENGTH), 1
    )
    upper = jnp.where(before, 1.0, 0.0).astype(BF16)
    sums = dot(jnp.concatenate([low, mid, hi], axis=0), upper, (((1,), (0,)), ((), ())))
    span = BATCH * 16
    log_cum = sums[0:span] + sums[span : 2 * span] + sums[2 * span : 3 * span]
    log_rows = [log_cum[m * 16 : (m + 1) * 16] for m in range(BATCH)]
    row_mats = list(log_rows)
    ends = []
    for m in range(BATCH):
        end = log_rows[m][:, LENGTH - 1 : LENGTH]
        ends.append(end)
        keep = jnp.where(docs[m : m + 1] == docs[m : m + 1, LENGTH - 1 : LENGTH], 1.0, 0.0)
        row_mats.append(jnp.exp(jnp.minimum(end - log_rows[m], 0.0)) * step_rows[m] * keep)
    for m in range(BATCH):
        row_mats.append(jnp.exp(log_rows[m]))
    row_mats.append(jnp.zeros((128 - 3 * span, LENGTH), F32))
    cols = jnp.concatenate(row_mats, axis=0).T
    log_col, weight_col, entry_col = 0, span, 2 * span

    for copy in got_taps:
        need(copy)
    tap = taps[...].astype(F32)
    tiles = plan.conv // 128
    def convolve(m):
        for j in range(tiles):
            at = slice(j * 128, (j + 1) * 128)
            rows = xbc[m, :, at].astype(F32)
            total = rows * tap[TAPS - 1 : TAPS, at]
            for k in range(1, TAPS):
                weight = tap[TAPS - 1 - k : TAPS - k, at]
                total = total + (pltpu.roll(rows, k, 0) * weight) * masks[m, k - 1]
            total = silu(total)
            conv[m, :, at] = total.astype(BF16)
            if j < plan.pairs:
                scale = pair_columns(cols, weight_col + m * 16 + 2 * j, lane)
                xw[m, :, at] = (total.astype(BF16).astype(F32) * scale).astype(BF16)

    def turn_weights():
        need(got_w)
        for j in range(plan.width // 128):
            wt[j * 128 : (j + 1) * 128, :] = w_ref[:, j * 128 : (j + 1) * 128].T

    def gate_inputs(m):
        need(got_z)
        for j in range(plan.pairs):
            at = slice(j * 128, (j + 1) * 128)
            zg[m, :, at] = silu(z_ref[m, :, at].astype(F32))

    convolve(0)
    pl.when(has_prior)(halos[BATCH].wait_recv)
    doc_before = jnp.where(has_prior, doc_halo[...].astype(F32), -1.0)
    edge_marks = []
    joined = jnp.concatenate([doc_before, docs[:, 0:128]], axis=1)
    for k in range(1, TAPS):
        edge_marks.append(jnp.where(pltpu.roll(joined, k, 1) == joined, 1.0, 0.0))
    edge_rows = jnp.concatenate(
        edge_marks + [jnp.zeros((16 - BATCH * (TAPS - 1), LENGTH), F32)], axis=0
    )[:, 128:256]
    edge_rows = jnp.concatenate([edge_rows, jnp.zeros((112, 128), F32)], axis=0)
    edge_cols = edge_rows.T[0:HALO]

    def exchange(m, source, target, peers_send, peers_recv):
        copies = []
        for k in range(1, ring):
            to = lax.rem(rank + k, ring)
            copies.append(
                pltpu.make_async_remote_copy(
                    src_ref=source.at[m, to],
                    dst_ref=target(to),
                    send_sem=peers_send.at[m, k],
                    recv_sem=peers_recv.at[m, k],
                    device_id=in_plane(to),
                    device_id_type=pl.DeviceIdType.MESH,
                )
            )
        return copies

    group_row = lax.broadcasted_iota(jnp.int32, (ring * plan.gate_rows, 16), 0)
    group_head = lax.broadcasted_iota(jnp.int32, (ring * plan.gate_rows, 16), 1)
    bits = plan.gate_rows.bit_length() - 1
    shard_of, group_of = group_row >> bits, group_row & (plan.gate_rows - 1)
    picks = (((shard_of * plan.groups + group_of) >> 2) == group_head) & (group_of < plan.groups)
    pick = jnp.where(picks, 1.0, 0.0).astype(BF16)
    a_copies = []
    for m in range(BATCH):
        if m > 0:
            convolve(m)
        pl.when(has_prior)(halos[m].wait_recv)
        for j in range(tiles):
            at = slice(j * 128, (j + 1) * 128)
            lead = jnp.where(has_prior, halo[m, :, at].astype(F32), 0.0)
            own = xbc[m, 0:HALO, at].astype(F32)
            both = jnp.concatenate([lead, own], axis=0)
            total = own * tap[TAPS - 1 : TAPS, at]
            for k in range(1, TAPS):
                weight = tap[TAPS - 1 - k : TAPS - k, at]
                same = edge_cols[:, (k - 1) * BATCH + m : (k - 1) * BATCH + m + 1]
                total = total + (pltpu.roll(both, k, 0)[HALO : 2 * HALO] * weight) * same
            total = silu(total)
            conv[m, 0:HALO, at] = total.astype(BF16)
            if j < plan.pairs:
                scale = pair_columns(cols[0:HALO], weight_col + m * 16 + 2 * j, lane[0:HALO])
                xw[m, 0:HALO, at] = (total.astype(BF16).astype(F32) * scale).astype(BF16)
        state = dot(xw[m], conv[m, :, ch : ch + DSTATE], ROWS).astype(BF16)
        carried_end = docs[m : m + 1, LENGTH - 1 : LENGTH] == doc_before[m : m + 1, 127:128]
        gate = jnp.broadcast_to(jnp.exp(ends[m]) * jnp.where(carried_end, 1.0, 0.0), (16, DSTATE))
        gate_hi, gate_lo = split_two(gate)
        plain = (((1,), (0,)), ((), ()))
        hi_rows = dot(pick, gate_hi, plain).astype(BF16)
        lo_rows = dot(pick, gate_lo, plain).astype(BF16)
        for r in range(ring):
            fsend[m, r, 0 : plan.shard] = state[r * plan.shard : (r + 1) * plan.shard]
            at = slice(r * plan.gate_rows, (r + 1) * plan.gate_rows)
            fsend[m, r, plan.shard : plan.packet] = jnp.concatenate(
                [hi_rows[at], lo_rows[at]], axis=0
            )
        copies = exchange(m, fsend, lambda to, m=m: arecv.at[m, rank], a_send, a_recv)
        for copy in copies:
            copy.start()
        a_copies.append(copies)
        arecv[m, pl.ds(rank, 1)] = fsend[m, pl.ds(rank, 1)]

    def scores_of(m):
        t_pos = lax.broadcasted_iota(jnp.int32, (LENGTH, LENGTH), 0)
        s_pos = lax.broadcasted_iota(jnp.int32, (LENGTH, LENGTH), 1)
        doc_t = mark_cols[:, m * TAPS : m * TAPS + 1]
        keep = (s_pos <= t_pos) & (doc_t == docs[m : m + 1])
        full = dot(conv[m, :, ch + DSTATE : ch + 2 * DSTATE], conv[m, :, ch : ch + DSTATE], LANES)
        scores[m] = jnp.where(keep, full, 0.0)

    def inner_of(m):
        low_lane = lane < HEADDIM
        for j in range(plan.pairs):
            at = slice(j * 128, (j + 1) * 128)
            xs = conv[m, :, at]
            xs_a = jnp.where(low_lane, xs, jnp.zeros_like(xs))
            xs_b = jnp.where(low_lane, jnp.zeros_like(xs), xs)
            for half in range(2):
                t0, s1 = half * HALF, (half + 1) * HALF
                base = scores[m, t0 : t0 + HALF, 0:s1]
                mixes = []
                for h in (2 * j, 2 * j + 1):
                    t_log = cols[t0 : t0 + HALF, log_col + m * 16 + h : log_col + m * 16 + h + 1]
                    s_log = log_rows[m][h : h + 1, 0:s1]
                    decay = jnp.exp(jnp.minimum(t_log - s_log, 0.0))
                    mixes.append((base * step_rows[m][h : h + 1, 0:s1] * decay).astype(BF16))
                y[m, t0 : t0 + HALF, at] = dot(
                    jnp.concatenate(mixes, axis=1),
                    jnp.concatenate([xs_a[0:s1], xs_b[0:s1]], axis=0),
                    (((1,), (0,)), ((), ())),
                )

    def gate_both(m):
        carried = mark_cols[:, m * TAPS : m * TAPS + 1] == doc_before[m : m + 1, 127:128]
        for j in range(plan.pairs):
            at = slice(j * 128, (j + 1) * 128)
            opened = zg[m, :, at]
            y[m, :, at] = y[m, :, at] * opened
            entry = pair_columns(cols, entry_col + m * 16 + 2 * j, lane)
            zg[m, :, at] = jnp.where(carried, entry, 0.0) * opened

    def unpack(packet):
        packet = packet.astype(F32)
        split = plan.shard + plan.gate_rows
        return packet[0 : plan.shard], packet[plan.shard : split] + packet[split:]

    def pack(ref, m, total, product):
        ref[m, 0 : plan.shard] = total.astype(BF16)
        hi_rows, lo_rows = split_two(product)
        ref[m, plan.shard : plan.packet] = jnp.concatenate([hi_rows, lo_rows], axis=0)

    def ahead(source, m, slot, k):
        return pltpu.make_async_remote_copy(
            src_ref=source.at[m],
            dst_ref=brecv.at[m, slot],
            send_sem=b_send.at[m, slot],
            recv_sem=b_recv.at[m, slot],
            device_id={"sz": iz + k},
            device_id_type=pl.DeviceIdType.MESH,
        )

    jumps = [(0, 1), (1, 1), (2, 3)]
    b_copies = [
        [ahead(tsend if slot == 0 else usend, m, slot, k) for slot, k in jumps] for m in range(BATCH)
    ]

    def goes(k):
        return iz + k < plan.planes

    def plane_total(m):
        for copy in a_copies[m]:
            copy.wait_recv()
        total = jnp.zeros((plan.shard, DSTATE), F32)
        product = jnp.ones((plan.gate_rows, DSTATE), F32)
        for d in range(ring):
            pref[m, d] = total
            qpref[m, d] = product
            fresh, gates = unpack(arecv[m, d])
            total = spread(gates, plan) * total + fresh
            product = product * gates
        pack(tsend, m, total, product)
        ptot[m] = total
        qtot[m] = product
        pl.when(has_above)(b_copies[m][0].start)

    def two_planes(m):
        pl.when(has_below)(b_copies[m][0].wait_recv)
        lower, gates = unpack(brecv[m, 0])
        lower = jnp.where(has_below, lower, 0.0)
        gates = jnp.where(has_below, gates, 0.0)
        product = qtot[m]
        pack(usend, m, spread(product, plan) * lower + ptot[m], product * gates)
        pl.when(has_above)(b_copies[m][1].start)
        pl.when(goes(3))(b_copies[m][2].start)

    gate_inputs(0)
    scores_of(0)
    pl.when(goes(2))(lambda: pl.semaphore_wait(word.at[0], 1))
    pl.when(has_below & goes(2))(lambda: tell_below(1))
    inner_of(0)
    gate_both(0)
    plane_total(0)
    plane_total(1)
    scores_of(1)
    inner_of(1)
    pl.when(goes(3))(lambda: pl.semaphore_wait(word.at[1], 1))
    two_planes(0)
    two_planes(1)
    gate_inputs(1)
    gate_both(1)
    turn_weights()
    c_copies = []
    for m in range(BATCH):
        pl.when(has_below)(b_copies[m][1].wait_recv)
        pl.when(iz >= 3)(b_copies[m][2].wait_recv)
        near, gates = unpack(brecv[m, 1])
        remote, _ = unpack(brecv[m, 2])
        incoming = spread(gates, plan) * jnp.where(iz >= 3, remote, 0.0) + near
        incoming = jnp.where(has_below, incoming, 0.0)
        for d in range(ring):
            entering = pref[m, d] + spread(qpref[m, d], plan) * incoming
            hsend[m, d] = entering.astype(BF16)
        home = pl.ds(pl.multiple_of(rank * plan.shard, 16), plan.shard)
        copies = exchange(m, hsend, lambda to, m=m: hstate.at[m, home], c_send, c_recv)
        for copy in copies:
            copy.start()
        c_copies.append(copies)
        hstate[m, home] = hsend[m, rank]

    def arrow(chunk, step, upward):
        if upward:
            owner = lax.rem(me + plan.far - step, members)
            first, buffer, send, got, to = 0, up_recv, up_send, up_got, up
        else:
            owner = lax.rem(me + members - plan.far + step, members)
            first, buffer, send, got, to = plan.out // 2, dn_recv, dn_send, dn_got, down
        rows = pl.ds(first, plan.out // 2) if step == 0 else pl.ds(0, plan.out)
        return pltpu.make_async_remote_copy(
            src_ref=part.at[chunk, owner, rows],
            dst_ref=buffer.at[chunk, step, rows],
            send_sem=send.at[chunk, step],
            recv_sem=got.at[chunk, step],
            device_id=to,
            device_id_type=pl.DeviceIdType.MESH,
        )

    arrows = {}
    s_copies = []
    gain = gain_ref[...].reshape(1, ch)

    def project(m, owner):
        rows = pl.ds(pl.multiple_of(owner * plan.out, 16), plan.out)
        tile = dot(wt[rows, :], gated[m], LANES).astype(BF16)
        part[2 * m, owner] = tile[:, 0:HALF]
        part[2 * m + 1, owner] = tile[:, HALF:LENGTH]

    def carry(m):
        for copy in c_copies[m]:
            copy.wait_recv()
        squares = jnp.zeros((LENGTH, 128), F32)
        outer = dot(conv[m, :, ch + DSTATE : ch + 2 * DSTATE], hstate[m], LANES)
        for j in range(plan.pairs):
            at = slice(j * 128, (j + 1) * 128)
            mixed = y[m, :, at] + zg[m, :, at] * outer[:, at]
            squares = squares + mixed * mixed
            gated[m, :, at] = (mixed * gain[:, at]).astype(BF16)
        project(m, lax.rem(me + plan.far, members))
        for chunk in (2 * m, 2 * m + 1):
            for upward in (True, False):
                arrows[chunk, 0, upward] = arrow(chunk, 0, upward)
                arrows[chunk, 0, upward].start()
        square_hi, square_lo = split_two(squares)
        ones = jnp.ones((8, 128), BF16)
        square_rows = dot(ones, square_hi, LANES) + dot(ones, square_lo, LANES)
        ssend[m] = square_rows[0:1]
        for k in range(1, members):
            copy = pltpu.make_async_remote_copy(
                src_ref=ssend.at[m],
                dst_ref=srecv.at[m, k],
                send_sem=s_send.at[m, k],
                recv_sem=s_recv.at[m, k],
                device_id={"mp": lax.rem(me + k, members)},
                device_id_type=pl.DeviceIdType.MESH,
            )
            copy.start()
            s_copies.append(copy)

    half = plan.out // 2

    def ring_step(m, step):
        owners = {
            True: lax.rem(me + plan.far - step, members),
            False: lax.rem(me + members - plan.far + step, members),
        }
        for upward in (True, False):
            project(m, owners[upward])
        for chunk in (2 * m, 2 * m + 1):
            for upward in (True, False):
                arrows[chunk, step - 1, upward].wait_recv()
                buffer = up_recv if upward else dn_recv
                owner = owners[upward]
                if step == 1:
                    rows = slice(0, half) if upward else slice(half, plan.out)
                else:
                    rows = slice(0, plan.out)
                total = part[chunk, owner, rows].astype(F32) + buffer[chunk, step - 1, rows].astype(F32)
                part[chunk, owner, rows] = total.astype(BF16)
                arrows[chunk, step, upward] = arrow(chunk, step, upward)
                arrows[chunk, step, upward].start()

    carry(0)
    if plan.far > 1:
        ring_step(0, 1)
    carry(1)
    for step in range(1, plan.far):
        if step > 1:
            ring_step(0, step)
        ring_step(1, step)
    for m in range(BATCH):
        project(m, me)

    for copy in s_copies:
        copy.wait_recv()
    last = plan.far - 1
    for m in range(BATCH):
        square = ssend[m]
        for k in range(1, members):
            square = square + srecv[m, k]
        scale = lax.rsqrt(square / INNER + EPSILON)
        for side in range(2):
            chunk = 2 * m + side
            total = part[chunk, me].astype(F32)
            if last == 0:
                arrows[chunk, last, True].wait_recv()
                arrows[chunk, last, False].wait_recv()
                total = total + jnp.concatenate(
                    [up_recv[chunk, 0, 0:half], dn_recv[chunk, 0, half : plan.out]], axis=0
                ).astype(F32)
            else:
                for upward in (True, False):
                    arrows[chunk, last, upward].wait_recv()
                    buffer = up_recv if upward else dn_recv
                    total = total + buffer[chunk, last].astype(F32)
            at = slice(side * HALF, (side + 1) * HALF)
            out_ref[m, :, at] = (total * scale[:, at]).astype(BF16)

    def sent():
        for copy in halos:
            copy.wait_send()

    pl.when(has_next)(sent)
    for group in (*a_copies, *c_copies, s_copies, list(arrows.values())):
        for copy in group:
            copy.wait_send()
    for m in range(BATCH):
        for slot, k in jumps:
            pl.when(goes(k))(b_copies[m][slot].wait_send)


def shards(
    plan,
    x_inner,
    z_gate,
    b_input,
    c_input,
    dt_raw,
    doc_ids,
    conv_x,
    conv_b,
    conv_c,
    dt_bias,
    decay_rate,
    norm_gain,
    w_out,
):
    hbm = pl.BlockSpec(memory_space=pltpu.HBM)
    smem = pl.BlockSpec(memory_space=pltpu.SMEM)
    vmem = pl.BlockSpec(memory_space=pltpu.VMEM)
    ch, ring, members = plan.channels, plan.ring, plan.members
    chunks = 2 * BATCH
    dma = pltpu.SemaphoreType.DMA
    scratch = [
        pltpu.VMEM((BATCH, LENGTH, plan.conv), BF16),
        pltpu.VMEM((BATCH, HALO, plan.conv), BF16),
        pltpu.VMEM((BATCH, LENGTH), jnp.int32),
        pltpu.VMEM((BATCH, 128), jnp.int32),
        pltpu.VMEM((plan.heads, BATCH, LENGTH), F32),
        pltpu.VMEM((TAPS, plan.conv), BF16),
        pltpu.VMEM((BATCH, LENGTH, ch), BF16),
        pltpu.VMEM((ch, plan.width), BF16),
        pltpu.VMEM((plan.width, ch), BF16),
        pltpu.VMEM((BATCH, LENGTH, plan.conv), BF16),
        pltpu.VMEM((BATCH, TAPS - 1, LENGTH, 128), F32),
        pltpu.VMEM((BATCH, LENGTH, ch), BF16),
        pltpu.VMEM((BATCH, LENGTH, ch), F32),
        pltpu.VMEM((BATCH, LENGTH, LENGTH), F32),
        pltpu.VMEM((BATCH, LENGTH, ch), F32),
        pltpu.VMEM((BATCH, LENGTH, ch), BF16),
        pltpu.VMEM((BATCH, ring, plan.packet, DSTATE), BF16),
        pltpu.VMEM((BATCH, ring, plan.packet, DSTATE), BF16),
        pltpu.VMEM((BATCH, ring, plan.shard, DSTATE), F32),
        pltpu.VMEM((BATCH, ring, plan.gate_rows, DSTATE), F32),
        pltpu.VMEM((BATCH, plan.packet, DSTATE), BF16),
        pltpu.VMEM((BATCH, plan.packet, DSTATE), BF16),
        pltpu.VMEM((BATCH, plan.shard, DSTATE), F32),
        pltpu.VMEM((BATCH, plan.gate_rows, DSTATE), F32),
        pltpu.VMEM((BATCH, 3, plan.packet, DSTATE), BF16),
        pltpu.VMEM((BATCH, ring, plan.shard, DSTATE), BF16),
        pltpu.VMEM((BATCH, ch, DSTATE), BF16),
        pltpu.VMEM((chunks, members, plan.out, HALF), BF16),
        pltpu.VMEM((chunks, plan.far, plan.out, HALF), BF16),
        pltpu.VMEM((chunks, plan.far, plan.out, HALF), BF16),
        pltpu.VMEM((BATCH, 1, LENGTH), F32),
        pltpu.VMEM((BATCH, members, 1, LENGTH), F32),
        dma((13,)),
        dma((BATCH + 1,)),
        dma((BATCH + 1,)),
        dma((BATCH, ring)),
        dma((BATCH, ring)),
        dma((BATCH, 3)),
        dma((BATCH, 3)),
        dma((BATCH, ring)),
        dma((BATCH, ring)),
        dma((BATCH, members)),
        dma((BATCH, members)),
        dma((chunks, plan.far)),
        dma((chunks, plan.far)),
        dma((chunks, plan.far)),
        dma((chunks, plan.far)),
        pltpu.SemaphoreType.REGULAR((2,)),
    ]
    out = pl.pallas_call(
        functools.partial(layer_kernel, plan),
        name="mixer_layer",
        out_shape=pltpu.VMEM((BATCH, plan.out, LENGTH), BF16),
        in_specs=[hbm] * 9 + [smem, smem, vmem, hbm],
        out_specs=vmem,
        scratch_shapes=scratch,
        compiler_params=pltpu.CompilerParams(
            collective_id=0, has_side_effects=True, vmem_limit_bytes=60 * 1024 * 1024
        ),
    )(
        x_inner,
        z_gate,
        b_input,
        c_input,
        jnp.transpose(dt_raw, (2, 0, 1)),
        doc_ids,
        conv_x,
        conv_b,
        conv_c,
        dt_bias,
        decay_rate,
        norm_gain,
        w_out,
    )
    return jnp.transpose(out, (0, 2, 1))


def solution(mesh):
    members = mesh.shape["mp"]
    line = Mesh(mesh.devices.reshape(*SPLIT, members), (*SEQ, "mp"))

    def layer(*arrays):
        channels = arrays[0].shape[2] // members
        plan = Plan(SPLIT, members, channels, arrays[12].shape[1])
        placed = (
            P(None, SEQ, "mp"),
            P(None, SEQ, "mp"),
            P(None, SEQ, None),
            P(None, SEQ, None),
            P(None, SEQ, "mp"),
            P(None, SEQ),
            P(None, "mp"),
            P(),
            P(),
            P("mp"),
            P("mp"),
            P("mp"),
            P("mp", None),
        )
        return jax.shard_map(
            functools.partial(shards, plan),
            mesh=line,
            in_specs=placed,
            out_specs=P(None, SEQ, "mp"),
            check_vma=False,
        )(*arrays)

    return layer
```

```python
import functools

import jax
import jax.numpy as jnp
from jax import lax
from jax.experimental import pallas as pl
from jax.experimental.pallas import tpu as pltpu
from jax.sharding import Mesh
from jax.sharding import PartitionSpec as P

SPLIT = (8, 4, 2)
SEQ = ("sz", "sx", "sc")
INNER = 5120
EPSILON = 1e-05
BATCH = 2
LENGTH = 256
HALF = 128
QUARTERS = 4
HALO = 8
TAPS = 4
HEADDIM = 64
DSTATE = 128
REACH = 8192 // LENGTH
F32 = jnp.float32
BF16 = jnp.bfloat16
LANES = (((1,), (1,)), ((), ()))
ROWS = (((0,), (0,)), ((), ()))


def dot(a, b, dims):
    return lax.dot_general(a, b, dims, preferred_element_type=F32)


def split_two(value):
    high = value.astype(BF16)
    return high, (value - high.astype(F32)).astype(BF16)


def silu(value):
    return value / (1.0 + jnp.exp(-value))


class Plan:
    def __init__(self, split, members, channels, width):
        self.planes, self.xs, self.cores = split
        self.ring = self.xs * self.cores
        self.members = members
        self.channels = channels
        self.heads = channels // HEADDIM
        self.pairs = self.heads // 2
        self.conv = channels + 2 * DSTATE
        self.shard = channels // self.ring
        self.groups = self.shard // 16
        self.gate_rows = max(8, 1 << (self.groups - 1).bit_length())
        self.packet = self.shard + 2 * self.gate_rows
        assert REACH <= 4 * self.ring or self.planes <= 5
        self.width = width
        self.out = width // members
        self.far = members // 2


def spread(rows, plan):
    return jnp.concatenate(
        [jnp.broadcast_to(rows[q : q + 1], (16, DSTATE)) for q in range(plan.groups)], axis=0
    )


def pair_columns(cols, first, lane):
    a = jnp.broadcast_to(cols[:, first : first + 1], (cols.shape[0], 128))
    b = jnp.broadcast_to(cols[:, first + 1 : first + 2], (cols.shape[0], 128))
    return jnp.where(lane < HEADDIM, a, b)


def layer_kernel(
    plan,
    x_hbm,
    z_hbm,
    b_hbm,
    c_hbm,
    dt_hbm,
    doc_hbm,
    cx_hbm,
    cb_hbm,
    cc_hbm,
    bias_ref,
    rate_ref,
    gain_ref,
    w_hbm,
    out_ref,
    xbc,
    halo,
    docs_ref,
    doc_halo,
    dt_ref,
    taps,
    z_ref,
    w_ref,
    wt,
    conv,
    masks,
    xw,
    y,
    scores,
    zg,
    gated,
    fsend,
    arecv,
    pref,
    qpref,
    tsend,
    usend,
    ptot,
    qtot,
    brecv,
    hsend,
    hstate,
    part,
    up_recv,
    dn_recv,
    ssend,
    srecv,
    load_sem,
    halo_send,
    halo_recv,
    a_send,
    a_recv,
    b_send,
    b_recv,
    c_send,
    c_recv,
    s_send,
    s_recv,
    up_send,
    up_got,
    dn_send,
    dn_got,
    word,
):
    ch, nh, ring, members = plan.channels, plan.heads, plan.ring, plan.members
    iz, ix, ic = lax.axis_index("sz"), lax.axis_index("sx"), lax.axis_index("sc")
    me = lax.axis_index("mp")
    rank = ix * plan.cores + ic
    place = iz * ring + rank
    blocks = plan.planes * ring

    def in_plane(r):
        return {"sx": r // plan.cores, "sc": r % plan.cores}

    def in_line(j):
        return {"sz": j // ring, "sx": (j % ring) // plan.cores, "sc": j % plan.cores}

    after, prior = in_line(place + 1), in_line(place - 1)
    up = {"mp": lax.rem(me + 1, members)}
    down = {"mp": lax.rem(me + members - 1, members)}

    has_next, has_prior = place + 1 < blocks, place > 0

    def one(flag):
        return jnp.where(flag, 1, 0)

    barrier = pltpu.get_barrier_semaphore()

    def greet(peer):
        pl.semaphore_signal(barrier, inc=1, device_id=peer, device_id_type=pl.DeviceIdType.MESH)

    for k in range(1, ring):
        greet(in_plane(lax.rem(rank + k, ring)))
    for k in range(1, members):
        greet({"mp": lax.rem(me + k, members)})
    pl.when(has_prior)(lambda: greet(prior))
    count = ring - 1 + members - 1 + one(has_next)
    above, below = {"sz": iz + 1}, {"sz": iz - 1}
    has_above, has_below = iz + 1 < plan.planes, iz > 0
    pl.when(has_below)(lambda: greet(below))
    pl.when(has_above)(lambda: greet(above))
    count = count + one(has_above) + one(has_below)

    def tell_below(at):
        pl.semaphore_signal(
            word.at[at], inc=1, device_id=below, device_id_type=pl.DeviceIdType.MESH
        )

    loads = []

    def load(src, dst):
        copy = pltpu.make_async_copy(src, dst, load_sem.at[len(loads)])
        copy.start()
        loads.append(copy)
        return copy

    done = []

    def need(copy):
        if not any(copy is other for other in done):
            copy.wait()
            done.append(copy)

    def got_waits():
        for copy in loads:
            need(copy)

    got_dt = load(dt_hbm, dt_ref)
    got_docs = load(doc_hbm, docs_ref)
    got_taps = [
        load(cx_hbm, taps.at[:, pl.ds(0, ch)]),
        load(cb_hbm, taps.at[:, pl.ds(ch, DSTATE)]),
        load(cc_hbm, taps.at[:, pl.ds(ch + DSTATE, DSTATE)]),
    ]
    got_rows = []
    for m in range(BATCH):
        got_rows.append(
            [
                load(x_hbm.at[m], xbc.at[m, :, pl.ds(0, ch)]),
                load(b_hbm.at[m], xbc.at[m, :, pl.ds(ch, DSTATE)]),
                load(c_hbm.at[m], xbc.at[m, :, pl.ds(ch + DSTATE, DSTATE)]),
            ]
        )
    got_z = load(z_hbm, z_ref)
    got_w = load(w_hbm, w_ref)

    need(got_docs)
    for copy in (*got_rows[0], *got_rows[1]):
        need(copy)
    pl.semaphore_wait(barrier, count)
    pl.when(has_below & has_above)(lambda: tell_below(0))

    halos = []
    for m in range(BATCH):
        halos.append(
            pltpu.make_async_remote_copy(
                src_ref=xbc.at[m, pl.ds(LENGTH - HALO, HALO)],
                dst_ref=halo.at[m],
                send_sem=halo_send.at[m],
                recv_sem=halo_recv.at[m],
                device_id=after,
                device_id_type=pl.DeviceIdType.MESH,
            )
        )
    halos.append(
        pltpu.make_async_remote_copy(
            src_ref=docs_ref.at[:, pl.ds(LENGTH - 128, 128)],
            dst_ref=doc_halo,
            send_sem=halo_send.at[BATCH],
            recv_sem=halo_recv.at[BATCH],
            device_id=after,
            device_id_type=pl.DeviceIdType.MESH,
        )
    )
    def send_halo():
        for copy in (halos[BATCH], *halos[:BATCH]):
            copy.start()

    pl.when(has_next)(send_halo)

    lane = lax.broadcasted_iota(jnp.int32, (LENGTH, 128), 1)

    docs = docs_ref[...].astype(F32)
    marks = []
    for m in range(BATCH):
        own = docs[m : m + 1]
        marks.append(own)
        for k in range(1, TAPS):
            marks.append(jnp.where(pltpu.roll(own, k, 1) == own, 1.0, 0.0))
    mark_cols = jnp.concatenate(marks, axis=0).T
    for m in range(BATCH):
        for k in range(1, TAPS):
            at = m * TAPS + k
            masks[m, k - 1] = jnp.broadcast_to(mark_cols[:, at : at + 1], (LENGTH, 128))
    need(got_dt)
    head_row = lax.broadcasted_iota(jnp.int32, (16, LENGTH), 0)
    bias = jnp.zeros((16, LENGTH), F32)
    rate = jnp.zeros((16, LENGTH), F32)
    for h in range(nh):
        bias = jnp.where(head_row == h, bias_ref[h], bias)
        rate = jnp.where(head_row == h, rate_ref[h], rate)
    step_rows, log_parts = [], []
    for m in range(BATCH):
        raw = dt_ref[:, m, :]
        if nh < 16:
            raw = jnp.concatenate([raw, jnp.zeros((16 - nh, LENGTH), F32)], axis=0)
        shifted = raw + bias
        step = jnp.maximum(shifted, 0.0) + jnp.log1p(jnp.exp(-jnp.abs(shifted)))
        step_rows.append(step)
        log_parts.append(-(step * rate))
    log_step = jnp.concatenate(log_parts, axis=0)
    hi = log_step.astype(BF16)
    rest = log_step - hi.astype(F32)
    mid = rest.astype(BF16)
    low = (rest - mid.astype(F32)).astype(BF16)
    before = lax.broadcasted_iota(jnp.int32, (LENGTH, LENGTH), 0) <= lax.broadcasted_iota(
        jnp.int32, (LENGTH, LENGTH), 1
    )
    upper = jnp.where(before, 1.0, 0.0).astype(BF16)
    sums = dot(jnp.concatenate([low, mid, hi], axis=0), upper, (((1,), (0,)), ((), ())))
    span = BATCH * 16
    log_cum = sums[0:span] + sums[span : 2 * span] + sums[2 * span : 3 * span]
    log_rows = [log_cum[m * 16 : (m + 1) * 16] for m in range(BATCH)]
    row_mats = list(log_rows)
    ends = []
    for m in range(BATCH):
        end = log_rows[m][:, LENGTH - 1 : LENGTH]
        ends.append(end)
        keep = jnp.where(docs[m : m + 1] == docs[m : m + 1, LENGTH - 1 : LENGTH], 1.0, 0.0)
        row_mats.append(jnp.exp(jnp.minimum(end - log_rows[m], 0.0)) * step_rows[m] * keep)
    for m in range(BATCH):
        row_mats.append(jnp.exp(log_rows[m]))
    row_mats.append(jnp.zeros((128 - 3 * span, LENGTH), F32))
    cols = jnp.concatenate(row_mats, axis=0).T
    log_col, weight_col, entry_col = 0, span, 2 * span

    for copy in got_taps:
        need(copy)
    tap = taps[...].astype(F32)
    tiles = plan.conv // 128
    def convolve(m):
        for j in range(tiles):
            at = slice(j * 128, (j + 1) * 128)
            rows = xbc[m, :, at].astype(F32)
            total = rows * tap[TAPS - 1 : TAPS, at]
            for k in range(1, TAPS):
                weight = tap[TAPS - 1 - k : TAPS - k, at]
                total = total + (pltpu.roll(rows, k, 0) * weight) * masks[m, k - 1]
            total = silu(total)
            conv[m, :, at] = total.astype(BF16)
            if j < plan.pairs:
                scale = pair_columns(cols, weight_col + m * 16 + 2 * j, lane)
                xw[m, :, at] = (total.astype(BF16).astype(F32) * scale).astype(BF16)

    def turn_weights():
        need(got_w)
        for j in range(plan.width // 128):
            wt[j * 128 : (j + 1) * 128, :] = w_ref[:, j * 128 : (j + 1) * 128].T

    def gate_inputs(m):
        need(got_z)
        for j in range(plan.pairs):
            at = slice(j * 128, (j + 1) * 128)
            zg[m, :, at] = silu(z_ref[m, :, at].astype(F32))

    convolve(0)
    pl.when(has_prior)(halos[BATCH].wait_recv)
    doc_before = jnp.where(has_prior, doc_halo[...].astype(F32), -1.0)
    edge_marks = []
    joined = jnp.concatenate([doc_before, docs[:, 0:128]], axis=1)
    for k in range(1, TAPS):
        edge_marks.append(jnp.where(pltpu.roll(joined, k, 1) == joined, 1.0, 0.0))
    edge_rows = jnp.concatenate(
        edge_marks + [jnp.zeros((16 - BATCH * (TAPS - 1), LENGTH), F32)], axis=0
    )[:, 128:256]
    edge_rows = jnp.concatenate([edge_rows, jnp.zeros((112, 128), F32)], axis=0)
    edge_cols = edge_rows.T[0:HALO]

    def exchange(m, source, target, peers_send, peers_recv):
        copies = []
        for k in range(1, ring):
            to = lax.rem(rank + k, ring)
            copies.append(
                pltpu.make_async_remote_copy(
                    src_ref=source.at[m, to],
                    dst_ref=target(to),
                    send_sem=peers_send.at[m, k],
                    recv_sem=peers_recv.at[m, k],
                    device_id=in_plane(to),
                    device_id_type=pl.DeviceIdType.MESH,
                )
            )
        return copies

    group_row = lax.broadcasted_iota(jnp.int32, (ring * plan.gate_rows, 16), 0)
    group_head = lax.broadcasted_iota(jnp.int32, (ring * plan.gate_rows, 16), 1)
    bits = plan.gate_rows.bit_length() - 1
    shard_of, group_of = group_row >> bits, group_row & (plan.gate_rows - 1)
    picks = (((shard_of * plan.groups + group_of) >> 2) == group_head) & (group_of < plan.groups)
    pick = jnp.where(picks, 1.0, 0.0).astype(BF16)
    a_copies = []
    for m in range(BATCH):
        if m > 0:
            convolve(m)
        pl.when(has_prior)(halos[m].wait_recv)
        for j in range(tiles):
            at = slice(j * 128, (j + 1) * 128)
            lead = jnp.where(has_prior, halo[m, :, at].astype(F32), 0.0)
            own = xbc[m, 0:HALO, at].astype(F32)
            both = jnp.concatenate([lead, own], axis=0)
            total = own * tap[TAPS - 1 : TAPS, at]
            for k in range(1, TAPS):
                weight = tap[TAPS - 1 - k : TAPS - k, at]
                same = edge_cols[:, (k - 1) * BATCH + m : (k - 1) * BATCH + m + 1]
                total = total + (pltpu.roll(both, k, 0)[HALO : 2 * HALO] * weight) * same
            total = silu(total)
            conv[m, 0:HALO, at] = total.astype(BF16)
            if j < plan.pairs:
                scale = pair_columns(cols[0:HALO], weight_col + m * 16 + 2 * j, lane[0:HALO])
                xw[m, 0:HALO, at] = (total.astype(BF16).astype(F32) * scale).astype(BF16)
        state = dot(xw[m], conv[m, :, ch : ch + DSTATE], ROWS).astype(BF16)
        carried_end = docs[m : m + 1, LENGTH - 1 : LENGTH] == doc_before[m : m + 1, 127:128]
        gate = jnp.broadcast_to(jnp.exp(ends[m]) * jnp.where(carried_end, 1.0, 0.0), (16, DSTATE))
        gate_hi, gate_lo = split_two(gate)
        plain = (((1,), (0,)), ((), ()))
        hi_rows = dot(pick, gate_hi, plain).astype(BF16)
        lo_rows = dot(pick, gate_lo, plain).astype(BF16)
        for r in range(ring):
            fsend[m, r, 0 : plan.shard] = state[r * plan.shard : (r + 1) * plan.shard]
            at = slice(r * plan.gate_rows, (r + 1) * plan.gate_rows)
            fsend[m, r, plan.shard : plan.packet] = jnp.concatenate(
                [hi_rows[at], lo_rows[at]], axis=0
            )
        copies = exchange(m, fsend, lambda to, m=m: arecv.at[m, rank], a_send, a_recv)
        for copy in copies:
            copy.start()
        a_copies.append(copies)
        arecv[m, pl.ds(rank, 1)] = fsend[m, pl.ds(rank, 1)]

    def scores_of(m):
        t_pos = lax.broadcasted_iota(jnp.int32, (LENGTH, LENGTH), 0)
        s_pos = lax.broadcasted_iota(jnp.int32, (LENGTH, LENGTH), 1)
        doc_t = mark_cols[:, m * TAPS : m * TAPS + 1]
        keep = (s_pos <= t_pos) & (doc_t == docs[m : m + 1])
        full = dot(conv[m, :, ch + DSTATE : ch + 2 * DSTATE], conv[m, :, ch : ch + DSTATE], LANES)
        scores[m] = jnp.where(keep, full, 0.0)

    def inner_of(m):
        low_lane = lane < HEADDIM
        for j in range(plan.pairs):
            at = slice(j * 128, (j + 1) * 128)
            xs = conv[m, :, at]
            xs_a = jnp.where(low_lane, xs, jnp.zeros_like(xs))
            xs_b = jnp.where(low_lane, jnp.zeros_like(xs), xs)
            for half in range(2):
                t0, s1 = half * HALF, (half + 1) * HALF
                base = scores[m, t0 : t0 + HALF, 0:s1]
                mixes = []
                for h in (2 * j, 2 * j + 1):
                    t_log = cols[t0 : t0 + HALF, log_col + m * 16 + h : log_col + m * 16 + h + 1]
                    s_log = log_rows[m][h : h + 1, 0:s1]
                    decay = jnp.exp(jnp.minimum(t_log - s_log, 0.0))
                    mixes.append((base * step_rows[m][h : h + 1, 0:s1] * decay).astype(BF16))
                y[m, t0 : t0 + HALF, at] = dot(
                    jnp.concatenate(mixes, axis=1),
                    jnp.concatenate([xs_a[0:s1], xs_b[0:s1]], axis=0),
                    (((1,), (0,)), ((), ())),
                )

    def gate_both(m):
        carried = mark_cols[:, m * TAPS : m * TAPS + 1] == doc_before[m : m + 1, 127:128]
        for j in range(plan.pairs):
            at = slice(j * 128, (j + 1) * 128)
            opened = zg[m, :, at]
            y[m, :, at] = y[m, :, at] * opened
            entry = pair_columns(cols, entry_col + m * 16 + 2 * j, lane)
            zg[m, :, at] = jnp.where(carried, entry, 0.0) * opened

    def unpack(packet):
        packet = packet.astype(F32)
        split = plan.shard + plan.gate_rows
        return packet[0 : plan.shard], packet[plan.shard : split] + packet[split:]

    def pack(ref, m, total, product):
        ref[m, 0 : plan.shard] = total.astype(BF16)
        hi_rows, lo_rows = split_two(product)
        ref[m, plan.shard : plan.packet] = jnp.concatenate([hi_rows, lo_rows], axis=0)

    def ahead(source, m, slot, k):
        return pltpu.make_async_remote_copy(
            src_ref=source.at[m],
            dst_ref=brecv.at[m, slot],
            send_sem=b_send.at[m, slot],
            recv_sem=b_recv.at[m, slot],
            device_id={"sz": iz + k},
            device_id_type=pl.DeviceIdType.MESH,
        )

    jumps = [(0, 1), (1, 1), (2, 3)]
    b_copies = [
        [ahead(tsend if slot == 0 else usend, m, slot, k) for slot, k in jumps] for m in range(BATCH)
    ]

    def goes(k):
        return iz + k < plan.planes

    def plane_total(m):
        for copy in a_copies[m]:
            copy.wait_recv()
        total = jnp.zeros((plan.shard, DSTATE), F32)
        product = jnp.ones((plan.gate_rows, DSTATE), F32)
        for d in range(ring):
            pref[m, d] = total
            qpref[m, d] = product
            fresh, gates = unpack(arecv[m, d])
            total = spread(gates, plan) * total + fresh
            product = product * gates
        pack(tsend, m, total, product)
        ptot[m] = total
        qtot[m] = product
        pl.when(has_above)(b_copies[m][0].start)

    def two_planes(m):
        pl.when(has_below)(b_copies[m][0].wait_recv)
        lower, gates = unpack(brecv[m, 0])
        lower = jnp.where(has_below, lower, 0.0)
        gates = jnp.where(has_below, gates, 0.0)
        product = qtot[m]
        pack(usend, m, spread(product, plan) * lower + ptot[m], product * gates)
        pl.when(has_above)(b_copies[m][1].start)
        pl.when(goes(3))(b_copies[m][2].start)

    gate_inputs(0)
    scores_of(0)
    pl.when(goes(2))(lambda: pl.semaphore_wait(word.at[0], 1))
    pl.when(has_below & goes(2))(lambda: tell_below(1))
    inner_of(0)
    gate_both(0)
    plane_total(0)
    plane_total(1)
    scores_of(1)
    inner_of(1)
    pl.when(goes(3))(lambda: pl.semaphore_wait(word.at[1], 1))
    two_planes(0)
    two_planes(1)
    gate_inputs(1)
    gate_both(1)
    turn_weights()
    c_copies = []
    for m in range(BATCH):
        pl.when(has_below)(b_copies[m][1].wait_recv)
        pl.when(iz >= 3)(b_copies[m][2].wait_recv)
        near, gates = unpack(brecv[m, 1])
        remote, _ = unpack(brecv[m, 2])
        incoming = spread(gates, plan) * jnp.where(iz >= 3, remote, 0.0) + near
        incoming = jnp.where(has_below, incoming, 0.0)
        for d in range(ring):
            entering = pref[m, d] + spread(qpref[m, d], plan) * incoming
            hsend[m, d] = entering.astype(BF16)
        home = pl.ds(pl.multiple_of(rank * plan.shard, 16), plan.shard)
        copies = exchange(m, hsend, lambda to, m=m: hstate.at[m, home], c_send, c_recv)
        for copy in copies:
            copy.start()
        c_copies.append(copies)
        hstate[m, home] = hsend[m, rank]

    quarter = plan.out // QUARTERS

    def hops(q, upward):
        return plan.far if (q < QUARTERS // 2) == upward else plan.far - 1

    def owner_at(distance, upward):
        return lax.rem(me + distance if upward else me + members - distance, members)

    def arrow(m, q, hop, upward):
        buffer, send, got, to = (
            (up_recv, up_send, up_got, up) if upward else (dn_recv, dn_send, dn_got, down)
        )
        rows = pl.ds(q * quarter, quarter)
        return pltpu.make_async_remote_copy(
            src_ref=part.at[m, owner_at(hops(q, upward) - hop, upward), rows],
            dst_ref=buffer.at[m, hop, rows],
            send_sem=send.at[m, q, hop],
            recv_sem=got.at[m, q, hop],
            device_id=to,
            device_id_type=pl.DeviceIdType.MESH,
        )

    arrows = {}
    s_copies = []
    gain = gain_ref[...].reshape(1, ch)

    def project(m, distance, upward):
        owner = owner_at(distance, upward)
        rows = pl.ds(pl.multiple_of(owner * plan.out, 16), plan.out)
        part[m, owner] = dot(wt[rows, :], gated[m], LANES).astype(BF16)

    def shoot(m, hop, upward, pieces):
        for q in pieces:
            if hop < hops(q, upward):
                if hop > 0:
                    arrows[m, q, hop - 1, upward].wait_recv()
                    buffer = up_recv if upward else dn_recv
                    owner = owner_at(hops(q, upward) - hop, upward)
                    rows = slice(q * quarter, (q + 1) * quarter)
                    total = part[m, owner, rows].astype(F32) + buffer[m, hop - 1, rows].astype(F32)
                    part[m, owner, rows] = total.astype(BF16)
                arrows[m, q, hop, upward] = arrow(m, q, hop, upward)
                arrows[m, q, hop, upward].start()

    early, late = range(QUARTERS // 2), range(QUARTERS // 2, QUARTERS)

    def first_round(m):
        project(m, plan.far, True)
        shoot(m, 0, True, early)
        shoot(m, 0, False, late)
        if plan.far > 1:
            project(m, plan.far - 1, True)
            shoot(m, 0, True, late)
            project(m, plan.far - 1, False)
            shoot(m, 0, False, early)

    def next_round(m, hop):
        if hop + 1 < plan.far:
            project(m, plan.far - 1 - hop, True)
            project(m, plan.far - 1 - hop, False)
        shoot(m, hop, True, early)
        shoot(m, hop, False, late)
        shoot(m, hop, True, late)
        shoot(m, hop, False, early)

    def carry(m):
        for copy in c_copies[m]:
            copy.wait_recv()
        squares = jnp.zeros((LENGTH, 128), F32)
        outer = dot(conv[m, :, ch + DSTATE : ch + 2 * DSTATE], hstate[m], LANES)
        for j in range(plan.pairs):
            at = slice(j * 128, (j + 1) * 128)
            mixed = y[m, :, at] + zg[m, :, at] * outer[:, at]
            squares = squares + mixed * mixed
            gated[m, :, at] = (mixed * gain[:, at]).astype(BF16)
        first_round(m)
        square_hi, square_lo = split_two(squares)
        ones = jnp.ones((8, 128), BF16)
        square_rows = dot(ones, square_hi, LANES) + dot(ones, square_lo, LANES)
        ssend[m] = square_rows[0:1]
        for k in range(1, members):
            copy = pltpu.make_async_remote_copy(
                src_ref=ssend.at[m],
                dst_ref=srecv.at[m, k],
                send_sem=s_send.at[m, k],
                recv_sem=s_recv.at[m, k],
                device_id={"mp": lax.rem(me + k, members)},
                device_id_type=pl.DeviceIdType.MESH,
            )
            copy.start()
            s_copies.append(copy)

    carry(0)
    carry(1)
    for hop in range(1, plan.far):
        for m in range(BATCH):
            next_round(m, hop)
    for m in range(BATCH):
        project(m, 0, True)

    for copy in s_copies:
        copy.wait_recv()
    for m in range(BATCH):
        square = ssend[m]
        for k in range(1, members):
            square = square + srecv[m, k]
        scale = lax.rsqrt(square / INNER + EPSILON)
        for q in (*late, *early):
            rows = slice(q * quarter, (q + 1) * quarter)
            total = part[m, me, rows].astype(F32)
            for upward in (True, False):
                last = hops(q, upward) - 1
                if last >= 0:
                    arrows[m, q, last, upward].wait_recv()
                    buffer = up_recv if upward else dn_recv
                    total = total + buffer[m, last, rows].astype(F32)
            out_ref[m, rows, :] = (total * scale).astype(BF16)

    def sent():
        for copy in halos:
            copy.wait_send()

    pl.when(has_next)(sent)
    for group in (*a_copies, *c_copies, s_copies, list(arrows.values())):
        for copy in group:
            copy.wait_send()
    for m in range(BATCH):
        for slot, k in jumps:
            pl.when(goes(k))(b_copies[m][slot].wait_send)


def shards(
    plan,
    x_inner,
    z_gate,
    b_input,
    c_input,
    dt_raw,
    doc_ids,
    conv_x,
    conv_b,
    conv_c,
    dt_bias,
    decay_rate,
    norm_gain,
    w_out,
):
    hbm = pl.BlockSpec(memory_space=pltpu.HBM)
    smem = pl.BlockSpec(memory_space=pltpu.SMEM)
    vmem = pl.BlockSpec(memory_space=pltpu.VMEM)
    ch, ring, members = plan.channels, plan.ring, plan.members
    dma = pltpu.SemaphoreType.DMA
    scratch = [
        pltpu.VMEM((BATCH, LENGTH, plan.conv), BF16),
        pltpu.VMEM((BATCH, HALO, plan.conv), BF16),
        pltpu.VMEM((BATCH, LENGTH), jnp.int32),
        pltpu.VMEM((BATCH, 128), jnp.int32),
        pltpu.VMEM((plan.heads, BATCH, LENGTH), F32),
        pltpu.VMEM((TAPS, plan.conv), BF16),
        pltpu.VMEM((BATCH, LENGTH, ch), BF16),
        pltpu.VMEM((ch, plan.width), BF16),
        pltpu.VMEM((plan.width, ch), BF16),
        pltpu.VMEM((BATCH, LENGTH, plan.conv), BF16),
        pltpu.VMEM((BATCH, TAPS - 1, LENGTH, 128), F32),
        pltpu.VMEM((BATCH, LENGTH, ch), BF16),
        pltpu.VMEM((BATCH, LENGTH, ch), F32),
        pltpu.VMEM((BATCH, LENGTH, LENGTH), F32),
        pltpu.VMEM((BATCH, LENGTH, ch), F32),
        pltpu.VMEM((BATCH, LENGTH, ch), BF16),
        pltpu.VMEM((BATCH, ring, plan.packet, DSTATE), BF16),
        pltpu.VMEM((BATCH, ring, plan.packet, DSTATE), BF16),
        pltpu.VMEM((BATCH, ring, plan.shard, DSTATE), F32),
        pltpu.VMEM((BATCH, ring, plan.gate_rows, DSTATE), F32),
        pltpu.VMEM((BATCH, plan.packet, DSTATE), BF16),
        pltpu.VMEM((BATCH, plan.packet, DSTATE), BF16),
        pltpu.VMEM((BATCH, plan.shard, DSTATE), F32),
        pltpu.VMEM((BATCH, plan.gate_rows, DSTATE), F32),
        pltpu.VMEM((BATCH, 3, plan.packet, DSTATE), BF16),
        pltpu.VMEM((BATCH, ring, plan.shard, DSTATE), BF16),
        pltpu.VMEM((BATCH, ch, DSTATE), BF16),
        pltpu.VMEM((BATCH, members, plan.out, LENGTH), BF16),
        pltpu.VMEM((BATCH, plan.far, plan.out, LENGTH), BF16),
        pltpu.VMEM((BATCH, plan.far, plan.out, LENGTH), BF16),
        pltpu.VMEM((BATCH, 1, LENGTH), F32),
        pltpu.VMEM((BATCH, members, 1, LENGTH), F32),
        dma((13,)),
        dma((BATCH + 1,)),
        dma((BATCH + 1,)),
        dma((BATCH, ring)),
        dma((BATCH, ring)),
        dma((BATCH, 3)),
        dma((BATCH, 3)),
        dma((BATCH, ring)),
        dma((BATCH, ring)),
        dma((BATCH, members)),
        dma((BATCH, members)),
        dma((BATCH, QUARTERS, plan.far)),
        dma((BATCH, QUARTERS, plan.far)),
        dma((BATCH, QUARTERS, plan.far)),
        dma((BATCH, QUARTERS, plan.far)),
        pltpu.SemaphoreType.REGULAR((2,)),
    ]
    out = pl.pallas_call(
        functools.partial(layer_kernel, plan),
        name="mixer_layer",
        out_shape=pltpu.VMEM((BATCH, plan.out, LENGTH), BF16),
        in_specs=[hbm] * 9 + [smem, smem, vmem, hbm],
        out_specs=vmem,
        scratch_shapes=scratch,
        compiler_params=pltpu.CompilerParams(
            collective_id=0, has_side_effects=True, vmem_limit_bytes=60 * 1024 * 1024
        ),
    )(
        x_inner,
        z_gate,
        b_input,
        c_input,
        jnp.transpose(dt_raw, (2, 0, 1)),
        doc_ids,
        conv_x,
        conv_b,
        conv_c,
        dt_bias,
        decay_rate,
        norm_gain,
        w_out,
    )
    return jnp.transpose(out, (0, 2, 1))


def solution(mesh):
    members = mesh.shape["mp"]
    line = Mesh(mesh.devices.reshape(*SPLIT, members), (*SEQ, "mp"))

    def layer(*arrays):
        channels = arrays[0].shape[2] // members
        plan = Plan(SPLIT, members, channels, arrays[12].shape[1])
        placed = (
            P(None, SEQ, "mp"),
            P(None, SEQ, "mp"),
            P(None, SEQ, None),
            P(None, SEQ, None),
            P(None, SEQ, "mp"),
            P(None, SEQ),
            P(None, "mp"),
            P(),
            P(),
            P("mp"),
            P("mp"),
            P("mp"),
            P("mp", None),
        )
        return jax.shard_map(
            functools.partial(shards, plan),
            mesh=line,
            in_specs=placed,
            out_specs=P(None, SEQ, "mp"),
            check_vma=False,
        )(*arrays)

    return layer
```

```python
import functools

import jax
import jax.numpy as jnp
from jax import lax
from jax.experimental import pallas as pl
from jax.experimental.pallas import tpu as pltpu
from jax.sharding import Mesh
from jax.sharding import PartitionSpec as P

SPLIT = (8, 4, 2)
SEQ = ("sz", "sx", "sc")
INNER = 5120
EPSILON = 1e-05
BATCH = 2
LENGTH = 256
HALF = 128
QUARTERS = 4
HALO = 8
TAPS = 4
HEADDIM = 64
DSTATE = 128
REACH = 8192 // LENGTH
F32 = jnp.float32
BF16 = jnp.bfloat16
LANES = (((1,), (1,)), ((), ()))
ROWS = (((0,), (0,)), ((), ()))


def dot(a, b, dims):
    return lax.dot_general(a, b, dims, preferred_element_type=F32)


def split_two(value):
    high = value.astype(BF16)
    return high, (value - high.astype(F32)).astype(BF16)


def silu(value):
    return value / (1.0 + jnp.exp(-value))


class Plan:
    def __init__(self, split, members, channels, width):
        self.planes, self.xs, self.cores = split
        self.ring = self.xs * self.cores
        self.members = members
        self.channels = channels
        self.heads = channels // HEADDIM
        self.pairs = self.heads // 2
        self.conv = channels + 2 * DSTATE
        self.shard = channels // self.ring
        self.groups = self.shard // 16
        self.gate_rows = max(8, 1 << (self.groups - 1).bit_length())
        self.packet = self.shard + 2 * self.gate_rows
        assert REACH <= 4 * self.ring or self.planes <= 5
        self.width = width
        self.out = width // members
        self.far = members // 2


def spread(rows, plan):
    return jnp.concatenate(
        [jnp.broadcast_to(rows[q : q + 1], (16, DSTATE)) for q in range(plan.groups)], axis=0
    )


def pair_columns(cols, first, lane):
    a = jnp.broadcast_to(cols[:, first : first + 1], (cols.shape[0], 128))
    b = jnp.broadcast_to(cols[:, first + 1 : first + 2], (cols.shape[0], 128))
    return jnp.where(lane < HEADDIM, a, b)


def layer_kernel(
    plan,
    x_hbm,
    z_hbm,
    b_hbm,
    c_hbm,
    dt_hbm,
    doc_hbm,
    cx_hbm,
    cb_hbm,
    cc_hbm,
    bias_hbm,
    rate_hbm,
    gain_hbm,
    w_hbm,
    out_ref,
    bias_ref,
    rate_ref,
    gain_ref,
    xbc,
    halo,
    docs_ref,
    doc_halo,
    dt_ref,
    taps,
    z_ref,
    w_ref,
    wt,
    conv,
    masks,
    xw,
    y,
    scores,
    zg,
    gated,
    fsend,
    arecv,
    pref,
    qpref,
    tsend,
    usend,
    ptot,
    qtot,
    brecv,
    hsend,
    hstate,
    part,
    up_recv,
    dn_recv,
    ssend,
    srecv,
    load_sem,
    halo_send,
    halo_recv,
    a_send,
    a_recv,
    b_send,
    b_recv,
    c_send,
    c_recv,
    s_send,
    s_recv,
    up_send,
    up_got,
    dn_send,
    dn_got,
    word,
):
    ch, nh, ring, members = plan.channels, plan.heads, plan.ring, plan.members
    iz, ix, ic = lax.axis_index("sz"), lax.axis_index("sx"), lax.axis_index("sc")
    me = lax.axis_index("mp")
    rank = ix * plan.cores + ic
    place = iz * ring + rank
    blocks = plan.planes * ring

    def in_plane(r):
        return {"sx": r // plan.cores, "sc": r % plan.cores}

    def in_line(j):
        return {"sz": j // ring, "sx": (j % ring) // plan.cores, "sc": j % plan.cores}

    after, prior = in_line(place + 1), in_line(place - 1)
    up = {"mp": lax.rem(me + 1, members)}
    down = {"mp": lax.rem(me + members - 1, members)}

    has_next, has_prior = place + 1 < blocks, place > 0

    def one(flag):
        return jnp.where(flag, 1, 0)

    barrier = pltpu.get_barrier_semaphore()

    def greet(peer):
        pl.semaphore_signal(barrier, inc=1, device_id=peer, device_id_type=pl.DeviceIdType.MESH)

    for k in range(1, ring):
        greet(in_plane(lax.rem(rank + k, ring)))
    for k in range(1, members):
        greet({"mp": lax.rem(me + k, members)})
    pl.when(has_prior)(lambda: greet(prior))
    count = ring - 1 + members - 1 + one(has_next)
    above, below = {"sz": iz + 1}, {"sz": iz - 1}
    has_above, has_below = iz + 1 < plan.planes, iz > 0
    pl.when(has_below)(lambda: greet(below))
    pl.when(has_above)(lambda: greet(above))
    count = count + one(has_above) + one(has_below)

    def tell_below(at):
        pl.semaphore_signal(
            word.at[at], inc=1, device_id=below, device_id_type=pl.DeviceIdType.MESH
        )

    loads = []

    def load(src, dst):
        copy = pltpu.make_async_copy(src, dst, load_sem.at[len(loads)])
        copy.start()
        loads.append(copy)
        return copy

    done = []

    def need(copy):
        if not any(copy is other for other in done):
            copy.wait()
            done.append(copy)

    def got_waits():
        for copy in loads:
            need(copy)

    got_docs = load(doc_hbm, docs_ref)
    got_rows = []
    for m in range(BATCH):
        got_rows.append(
            [
                load(x_hbm.at[m], xbc.at[m, :, pl.ds(0, ch)]),
                load(b_hbm.at[m], xbc.at[m, :, pl.ds(ch, DSTATE)]),
                load(c_hbm.at[m], xbc.at[m, :, pl.ds(ch + DSTATE, DSTATE)]),
            ]
        )
    got_dt = [load(dt_hbm, dt_ref), load(bias_hbm, bias_ref), load(rate_hbm, rate_ref)]
    got_taps = [
        load(cx_hbm, taps.at[:, pl.ds(0, ch)]),
        load(cb_hbm, taps.at[:, pl.ds(ch, DSTATE)]),
        load(cc_hbm, taps.at[:, pl.ds(ch + DSTATE, DSTATE)]),
    ]
    got_gain = load(gain_hbm, gain_ref)
    got_z = load(z_hbm, z_ref)
    got_w = load(w_hbm, w_ref)

    need(got_docs)
    for copy in (*got_rows[0], *got_rows[1]):
        need(copy)
    pl.semaphore_wait(barrier, count)
    pl.when(has_below & has_above)(lambda: tell_below(0))

    halos = []
    for m in range(BATCH):
        halos.append(
            pltpu.make_async_remote_copy(
                src_ref=xbc.at[m, pl.ds(LENGTH - HALO, HALO)],
                dst_ref=halo.at[m],
                send_sem=halo_send.at[m],
                recv_sem=halo_recv.at[m],
                device_id=after,
                device_id_type=pl.DeviceIdType.MESH,
            )
        )
    halos.append(
        pltpu.make_async_remote_copy(
            src_ref=docs_ref.at[:, pl.ds(LENGTH - 128, 128)],
            dst_ref=doc_halo,
            send_sem=halo_send.at[BATCH],
            recv_sem=halo_recv.at[BATCH],
            device_id=after,
            device_id_type=pl.DeviceIdType.MESH,
        )
    )
    def send_halo():
        for copy in (halos[BATCH], *halos[:BATCH]):
            copy.start()

    pl.when(has_next)(send_halo)

    lane = lax.broadcasted_iota(jnp.int32, (LENGTH, 128), 1)

    docs = docs_ref[...].astype(F32)
    marks = []
    for m in range(BATCH):
        own = docs[m : m + 1]
        marks.append(own)
        for k in range(1, TAPS):
            marks.append(jnp.where(pltpu.roll(own, k, 1) == own, 1.0, 0.0))
    mark_cols = jnp.concatenate(marks, axis=0).T
    for m in range(BATCH):
        for k in range(1, TAPS):
            at = m * TAPS + k
            masks[m, k - 1] = jnp.broadcast_to(mark_cols[:, at : at + 1], (LENGTH, 128))
    for copy in got_dt:
        need(copy)
    head_row = lax.broadcasted_iota(jnp.int32, (16, LENGTH), 0)
    bias = jnp.zeros((16, LENGTH), F32)
    rate = jnp.zeros((16, LENGTH), F32)
    for h in range(nh):
        bias = jnp.where(head_row == h, bias_ref[h], bias)
        rate = jnp.where(head_row == h, rate_ref[h], rate)
    step_rows, log_parts = [], []
    for m in range(BATCH):
        raw = dt_ref[:, m, :]
        if nh < 16:
            raw = jnp.concatenate([raw, jnp.zeros((16 - nh, LENGTH), F32)], axis=0)
        shifted = raw + bias
        step = jnp.maximum(shifted, 0.0) + jnp.log1p(jnp.exp(-jnp.abs(shifted)))
        step_rows.append(step)
        log_parts.append(-(step * rate))
    log_step = jnp.concatenate(log_parts, axis=0)
    hi = log_step.astype(BF16)
    rest = log_step - hi.astype(F32)
    mid = rest.astype(BF16)
    low = (rest - mid.astype(F32)).astype(BF16)
    before = lax.broadcasted_iota(jnp.int32, (LENGTH, LENGTH), 0) <= lax.broadcasted_iota(
        jnp.int32, (LENGTH, LENGTH), 1
    )
    upper = jnp.where(before, 1.0, 0.0).astype(BF16)
    sums = dot(jnp.concatenate([low, mid, hi], axis=0), upper, (((1,), (0,)), ((), ())))
    span = BATCH * 16
    log_cum = sums[0:span] + sums[span : 2 * span] + sums[2 * span : 3 * span]
    log_rows = [log_cum[m * 16 : (m + 1) * 16] for m in range(BATCH)]
    row_mats = list(log_rows)
    ends = []
    for m in range(BATCH):
        end = log_rows[m][:, LENGTH - 1 : LENGTH]
        ends.append(end)
        keep = jnp.where(docs[m : m + 1] == docs[m : m + 1, LENGTH - 1 : LENGTH], 1.0, 0.0)
        row_mats.append(jnp.exp(jnp.minimum(end - log_rows[m], 0.0)) * step_rows[m] * keep)
    for m in range(BATCH):
        row_mats.append(jnp.exp(log_rows[m]))
    row_mats.append(jnp.zeros((128 - 3 * span, LENGTH), F32))
    cols = jnp.concatenate(row_mats, axis=0).T
    log_col, weight_col, entry_col = 0, span, 2 * span

    for copy in got_taps:
        need(copy)
    tap = taps[...].astype(F32)
    tiles = plan.conv // 128
    def convolve(m):
        for j in range(tiles):
            at = slice(j * 128, (j + 1) * 128)
            rows = xbc[m, :, at].astype(F32)
            total = rows * tap[TAPS - 1 : TAPS, at]
            for k in range(1, TAPS):
                weight = tap[TAPS - 1 - k : TAPS - k, at]
                total = total + (pltpu.roll(rows, k, 0) * weight) * masks[m, k - 1]
            total = silu(total)
            conv[m, :, at] = total.astype(BF16)
            if j < plan.pairs:
                scale = pair_columns(cols, weight_col + m * 16 + 2 * j, lane)
                xw[m, :, at] = (total.astype(BF16).astype(F32) * scale).astype(BF16)

    def turn_weights():
        need(got_w)
        for j in range(plan.width // 128):
            wt[j * 128 : (j + 1) * 128, :] = w_ref[:, j * 128 : (j + 1) * 128].T

    def gate_inputs(m):
        need(got_z)
        for j in range(plan.pairs):
            at = slice(j * 128, (j + 1) * 128)
            zg[m, :, at] = silu(z_ref[m, :, at].astype(F32))

    convolve(0)
    pl.when(has_prior)(halos[BATCH].wait_recv)
    doc_before = jnp.where(has_prior, doc_halo[...].astype(F32), -1.0)
    edge_marks = []
    joined = jnp.concatenate([doc_before, docs[:, 0:128]], axis=1)
    for k in range(1, TAPS):
        edge_marks.append(jnp.where(pltpu.roll(joined, k, 1) == joined, 1.0, 0.0))
    edge_rows = jnp.concatenate(
        edge_marks + [jnp.zeros((16 - BATCH * (TAPS - 1), LENGTH), F32)], axis=0
    )[:, 128:256]
    edge_rows = jnp.concatenate([edge_rows, jnp.zeros((112, 128), F32)], axis=0)
    edge_cols = edge_rows.T[0:HALO]

    def exchange(m, source, target, peers_send, peers_recv):
        copies = []
        for k in range(1, ring):
            to = lax.rem(rank + k, ring)
            copies.append(
                pltpu.make_async_remote_copy(
                    src_ref=source.at[m, to],
                    dst_ref=target(to),
                    send_sem=peers_send.at[m, k],
                    recv_sem=peers_recv.at[m, k],
                    device_id=in_plane(to),
                    device_id_type=pl.DeviceIdType.MESH,
                )
            )
        return copies

    group_row = lax.broadcasted_iota(jnp.int32, (ring * plan.gate_rows, 16), 0)
    group_head = lax.broadcasted_iota(jnp.int32, (ring * plan.gate_rows, 16), 1)
    bits = plan.gate_rows.bit_length() - 1
    shard_of, group_of = group_row >> bits, group_row & (plan.gate_rows - 1)
    picks = (((shard_of * plan.groups + group_of) >> 2) == group_head) & (group_of < plan.groups)
    pick = jnp.where(picks, 1.0, 0.0).astype(BF16)
    a_copies = []
    for m in range(BATCH):
        if m > 0:
            convolve(m)
        pl.when(has_prior)(halos[m].wait_recv)
        for j in range(tiles):
            at = slice(j * 128, (j + 1) * 128)
            lead = jnp.where(has_prior, halo[m, :, at].astype(F32), 0.0)
            own = xbc[m, 0:HALO, at].astype(F32)
            both = jnp.concatenate([lead, own], axis=0)
            total = own * tap[TAPS - 1 : TAPS, at]
            for k in range(1, TAPS):
                weight = tap[TAPS - 1 - k : TAPS - k, at]
                same = edge_cols[:, (k - 1) * BATCH + m : (k - 1) * BATCH + m + 1]
                total = total + (pltpu.roll(both, k, 0)[HALO : 2 * HALO] * weight) * same
            total = silu(total)
            conv[m, 0:HALO, at] = total.astype(BF16)
            if j < plan.pairs:
                scale = pair_columns(cols[0:HALO], weight_col + m * 16 + 2 * j, lane[0:HALO])
                xw[m, 0:HALO, at] = (total.astype(BF16).astype(F32) * scale).astype(BF16)
        state = dot(xw[m], conv[m, :, ch : ch + DSTATE], ROWS).astype(BF16)
        carried_end = docs[m : m + 1, LENGTH - 1 : LENGTH] == doc_before[m : m + 1, 127:128]
        gate = jnp.broadcast_to(jnp.exp(ends[m]) * jnp.where(carried_end, 1.0, 0.0), (16, DSTATE))
        gate_hi, gate_lo = split_two(gate)
        plain = (((1,), (0,)), ((), ()))
        hi_rows = dot(pick, gate_hi, plain).astype(BF16)
        lo_rows = dot(pick, gate_lo, plain).astype(BF16)
        for r in range(ring):
            fsend[m, r, 0 : plan.shard] = state[r * plan.shard : (r + 1) * plan.shard]
            at = slice(r * plan.gate_rows, (r + 1) * plan.gate_rows)
            fsend[m, r, plan.shard : plan.packet] = jnp.concatenate(
                [hi_rows[at], lo_rows[at]], axis=0
            )
        copies = exchange(m, fsend, lambda to, m=m: arecv.at[m, rank], a_send, a_recv)
        for copy in copies:
            copy.start()
        a_copies.append(copies)
        arecv[m, pl.ds(rank, 1)] = fsend[m, pl.ds(rank, 1)]

    def scores_of(m):
        t_pos = lax.broadcasted_iota(jnp.int32, (LENGTH, LENGTH), 0)
        s_pos = lax.broadcasted_iota(jnp.int32, (LENGTH, LENGTH), 1)
        doc_t = mark_cols[:, m * TAPS : m * TAPS + 1]
        keep = (s_pos <= t_pos) & (doc_t == docs[m : m + 1])
        full = dot(conv[m, :, ch + DSTATE : ch + 2 * DSTATE], conv[m, :, ch : ch + DSTATE], LANES)
        scores[m] = jnp.where(keep, full, 0.0)

    def inner_of(m):
        low_lane = lane < HEADDIM
        for j in range(plan.pairs):
            at = slice(j * 128, (j + 1) * 128)
            xs = conv[m, :, at]
            xs_a = jnp.where(low_lane, xs, jnp.zeros_like(xs))
            xs_b = jnp.where(low_lane, jnp.zeros_like(xs), xs)
            for half in range(2):
                t0, s1 = half * HALF, (half + 1) * HALF
                base = scores[m, t0 : t0 + HALF, 0:s1]
                mixes = []
                for h in (2 * j, 2 * j + 1):
                    t_log = cols[t0 : t0 + HALF, log_col + m * 16 + h : log_col + m * 16 + h + 1]
                    s_log = log_rows[m][h : h + 1, 0:s1]
                    decay = jnp.exp(jnp.minimum(t_log - s_log, 0.0))
                    mixes.append((base * step_rows[m][h : h + 1, 0:s1] * decay).astype(BF16))
                y[m, t0 : t0 + HALF, at] = dot(
                    jnp.concatenate(mixes, axis=1),
                    jnp.concatenate([xs_a[0:s1], xs_b[0:s1]], axis=0),
                    (((1,), (0,)), ((), ())),
                )

    def gate_both(m):
        carried = mark_cols[:, m * TAPS : m * TAPS + 1] == doc_before[m : m + 1, 127:128]
        for j in range(plan.pairs):
            at = slice(j * 128, (j + 1) * 128)
            opened = zg[m, :, at]
            y[m, :, at] = y[m, :, at] * opened
            entry = pair_columns(cols, entry_col + m * 16 + 2 * j, lane)
            zg[m, :, at] = jnp.where(carried, entry, 0.0) * opened

    def unpack(packet):
        packet = packet.astype(F32)
        split = plan.shard + plan.gate_rows
        return packet[0 : plan.shard], packet[plan.shard : split] + packet[split:]

    def pack(ref, m, total, product):
        ref[m, 0 : plan.shard] = total.astype(BF16)
        hi_rows, lo_rows = split_two(product)
        ref[m, plan.shard : plan.packet] = jnp.concatenate([hi_rows, lo_rows], axis=0)

    def ahead(source, m, slot, k):
        return pltpu.make_async_remote_copy(
            src_ref=source.at[m],
            dst_ref=brecv.at[m, slot],
            send_sem=b_send.at[m, slot],
            recv_sem=b_recv.at[m, slot],
            device_id={"sz": iz + k},
            device_id_type=pl.DeviceIdType.MESH,
        )

    jumps = [(0, 1), (1, 1), (2, 3)]
    b_copies = [
        [ahead(tsend if slot == 0 else usend, m, slot, k) for slot, k in jumps] for m in range(BATCH)
    ]

    def goes(k):
        return iz + k < plan.planes

    def plane_total(m):
        for copy in a_copies[m]:
            copy.wait_recv()
        total = jnp.zeros((plan.shard, DSTATE), F32)
        product = jnp.ones((plan.gate_rows, DSTATE), F32)
        for d in range(ring):
            pref[m, d] = total
            qpref[m, d] = product
            fresh, gates = unpack(arecv[m, d])
            total = spread(gates, plan) * total + fresh
            product = product * gates
        pack(tsend, m, total, product)
        ptot[m] = total
        qtot[m] = product
        pl.when(has_above)(b_copies[m][0].start)

    def two_planes(m):
        pl.when(has_below)(b_copies[m][0].wait_recv)
        lower, gates = unpack(brecv[m, 0])
        lower = jnp.where(has_below, lower, 0.0)
        gates = jnp.where(has_below, gates, 0.0)
        product = qtot[m]
        pack(usend, m, spread(product, plan) * lower + ptot[m], product * gates)
        pl.when(has_above)(b_copies[m][1].start)
        pl.when(goes(3))(b_copies[m][2].start)

    gate_inputs(0)
    scores_of(0)
    pl.when(goes(2))(lambda: pl.semaphore_wait(word.at[0], 1))
    pl.when(has_below & goes(2))(lambda: tell_below(1))
    inner_of(0)
    gate_both(0)
    plane_total(0)
    plane_total(1)
    scores_of(1)
    inner_of(1)
    pl.when(goes(3))(lambda: pl.semaphore_wait(word.at[1], 1))
    two_planes(0)
    two_planes(1)
    gate_inputs(1)
    gate_both(1)
    turn_weights()
    c_copies = []
    for m in range(BATCH):
        pl.when(has_below)(b_copies[m][1].wait_recv)
        pl.when(iz >= 3)(b_copies[m][2].wait_recv)
        near, gates = unpack(brecv[m, 1])
        remote, _ = unpack(brecv[m, 2])
        incoming = spread(gates, plan) * jnp.where(iz >= 3, remote, 0.0) + near
        incoming = jnp.where(has_below, incoming, 0.0)
        for d in range(ring):
            entering = pref[m, d] + spread(qpref[m, d], plan) * incoming
            hsend[m, d] = entering.astype(BF16)
        home = pl.ds(pl.multiple_of(rank * plan.shard, 16), plan.shard)
        copies = exchange(m, hsend, lambda to, m=m: hstate.at[m, home], c_send, c_recv)
        for copy in copies:
            copy.start()
        c_copies.append(copies)
        hstate[m, home] = hsend[m, rank]

    quarter = plan.out // QUARTERS

    def hops(q, upward):
        return plan.far if (q < QUARTERS // 2) == upward else plan.far - 1

    def owner_at(distance, upward):
        return lax.rem(me + distance if upward else me + members - distance, members)

    def arrow(m, q, hop, upward):
        buffer, send, got, to = (
            (up_recv, up_send, up_got, up) if upward else (dn_recv, dn_send, dn_got, down)
        )
        rows = pl.ds(q * quarter, quarter)
        return pltpu.make_async_remote_copy(
            src_ref=part.at[m, owner_at(hops(q, upward) - hop, upward), rows],
            dst_ref=buffer.at[m, hop, rows],
            send_sem=send.at[m, q, hop],
            recv_sem=got.at[m, q, hop],
            device_id=to,
            device_id_type=pl.DeviceIdType.MESH,
        )

    arrows = {}
    s_copies = []
    need(got_gain)
    gain = gain_ref[...].reshape(1, ch)

    def project(m, distance, upward):
        owner = owner_at(distance, upward)
        rows = pl.ds(pl.multiple_of(owner * plan.out, 16), plan.out)
        part[m, owner] = dot(wt[rows, :], gated[m], LANES).astype(BF16)

    def shoot(m, hop, upward, pieces):
        for q in pieces:
            if hop < hops(q, upward):
                if hop > 0:
                    arrows[m, q, hop - 1, upward].wait_recv()
                    buffer = up_recv if upward else dn_recv
                    owner = owner_at(hops(q, upward) - hop, upward)
                    rows = slice(q * quarter, (q + 1) * quarter)
                    total = part[m, owner, rows].astype(F32) + buffer[m, hop - 1, rows].astype(F32)
                    part[m, owner, rows] = total.astype(BF16)
                arrows[m, q, hop, upward] = arrow(m, q, hop, upward)
                arrows[m, q, hop, upward].start()

    early, late = range(QUARTERS // 2), range(QUARTERS // 2, QUARTERS)

    def first_round(m):
        project(m, plan.far, True)
        shoot(m, 0, True, early)
        shoot(m, 0, False, late)
        if plan.far > 1:
            project(m, plan.far - 1, True)
            shoot(m, 0, True, late)
            project(m, plan.far - 1, False)
            shoot(m, 0, False, early)

    def next_round(m, hop):
        if hop + 1 < plan.far:
            project(m, plan.far - 1 - hop, True)
            project(m, plan.far - 1 - hop, False)
        shoot(m, hop, True, early)
        shoot(m, hop, False, late)
        shoot(m, hop, True, late)
        shoot(m, hop, False, early)

    def carry(m):
        for copy in c_copies[m]:
            copy.wait_recv()
        squares = jnp.zeros((LENGTH, 128), F32)
        outer = dot(conv[m, :, ch + DSTATE : ch + 2 * DSTATE], hstate[m], LANES)
        for j in range(plan.pairs):
            at = slice(j * 128, (j + 1) * 128)
            mixed = y[m, :, at] + zg[m, :, at] * outer[:, at]
            squares = squares + mixed * mixed
            gated[m, :, at] = (mixed * gain[:, at]).astype(BF16)
        first_round(m)
        square_hi, square_lo = split_two(squares)
        ones = jnp.ones((8, 128), BF16)
        square_rows = dot(ones, square_hi, LANES) + dot(ones, square_lo, LANES)
        ssend[m] = square_rows[0:1]
        for k in range(1, members):
            copy = pltpu.make_async_remote_copy(
                src_ref=ssend.at[m],
                dst_ref=srecv.at[m, k],
                send_sem=s_send.at[m, k],
                recv_sem=s_recv.at[m, k],
                device_id={"mp": lax.rem(me + k, members)},
                device_id_type=pl.DeviceIdType.MESH,
            )
            copy.start()
            s_copies.append(copy)

    carry(0)
    carry(1)
    for hop in range(1, plan.far):
        for m in range(BATCH):
            next_round(m, hop)
    for m in range(BATCH):
        project(m, 0, True)

    for copy in s_copies:
        copy.wait_recv()
    for m in range(BATCH):
        square = ssend[m]
        for k in range(1, members):
            square = square + srecv[m, k]
        scale = lax.rsqrt(square / INNER + EPSILON)
        for q in (*late, *early):
            rows = slice(q * quarter, (q + 1) * quarter)
            total = part[m, me, rows].astype(F32)
            for upward in (True, False):
                last = hops(q, upward) - 1
                if last >= 0:
                    arrows[m, q, last, upward].wait_recv()
                    buffer = up_recv if upward else dn_recv
                    total = total + buffer[m, last, rows].astype(F32)
            out_ref[m, rows, :] = (total * scale).astype(BF16)

    def sent():
        for copy in halos:
            copy.wait_send()

    pl.when(has_next)(sent)
    for group in (*a_copies, *c_copies, s_copies, list(arrows.values())):
        for copy in group:
            copy.wait_send()
    for m in range(BATCH):
        for slot, k in jumps:
            pl.when(goes(k))(b_copies[m][slot].wait_send)


def shards(
    plan,
    x_inner,
    z_gate,
    b_input,
    c_input,
    dt_raw,
    doc_ids,
    conv_x,
    conv_b,
    conv_c,
    dt_bias,
    decay_rate,
    norm_gain,
    w_out,
):
    hbm = pl.BlockSpec(memory_space=pltpu.HBM)
    vmem = pl.BlockSpec(memory_space=pltpu.VMEM)
    ch, ring, members = plan.channels, plan.ring, plan.members
    dma = pltpu.SemaphoreType.DMA
    scratch = [
        pltpu.SMEM((plan.heads,), F32),
        pltpu.SMEM((plan.heads,), F32),
        pltpu.VMEM((ch,), F32),
        pltpu.VMEM((BATCH, LENGTH, plan.conv), BF16),
        pltpu.VMEM((BATCH, HALO, plan.conv), BF16),
        pltpu.VMEM((BATCH, LENGTH), jnp.int32),
        pltpu.VMEM((BATCH, 128), jnp.int32),
        pltpu.VMEM((plan.heads, BATCH, LENGTH), F32),
        pltpu.VMEM((TAPS, plan.conv), BF16),
        pltpu.VMEM((BATCH, LENGTH, ch), BF16),
        pltpu.VMEM((ch, plan.width), BF16),
        pltpu.VMEM((plan.width, ch), BF16),
        pltpu.VMEM((BATCH, LENGTH, plan.conv), BF16),
        pltpu.VMEM((BATCH, TAPS - 1, LENGTH, 128), F32),
        pltpu.VMEM((BATCH, LENGTH, ch), BF16),
        pltpu.VMEM((BATCH, LENGTH, ch), F32),
        pltpu.VMEM((BATCH, LENGTH, LENGTH), F32),
        pltpu.VMEM((BATCH, LENGTH, ch), F32),
        pltpu.VMEM((BATCH, LENGTH, ch), BF16),
        pltpu.VMEM((BATCH, ring, plan.packet, DSTATE), BF16),
        pltpu.VMEM((BATCH, ring, plan.packet, DSTATE), BF16),
        pltpu.VMEM((BATCH, ring, plan.shard, DSTATE), F32),
        pltpu.VMEM((BATCH, ring, plan.gate_rows, DSTATE), F32),
        pltpu.VMEM((BATCH, plan.packet, DSTATE), BF16),
        pltpu.VMEM((BATCH, plan.packet, DSTATE), BF16),
        pltpu.VMEM((BATCH, plan.shard, DSTATE), F32),
        pltpu.VMEM((BATCH, plan.gate_rows, DSTATE), F32),
        pltpu.VMEM((BATCH, 3, plan.packet, DSTATE), BF16),
        pltpu.VMEM((BATCH, ring, plan.shard, DSTATE), BF16),
        pltpu.VMEM((BATCH, ch, DSTATE), BF16),
        pltpu.VMEM((BATCH, members, plan.out, LENGTH), BF16),
        pltpu.VMEM((BATCH, plan.far, plan.out, LENGTH), BF16),
        pltpu.VMEM((BATCH, plan.far, plan.out, LENGTH), BF16),
        pltpu.VMEM((BATCH, 1, LENGTH), F32),
        pltpu.VMEM((BATCH, members, 1, LENGTH), F32),
        dma((16,)),
        dma((BATCH + 1,)),
        dma((BATCH + 1,)),
        dma((BATCH, ring)),
        dma((BATCH, ring)),
        dma((BATCH, 3)),
        dma((BATCH, 3)),
        dma((BATCH, ring)),
        dma((BATCH, ring)),
        dma((BATCH, members)),
        dma((BATCH, members)),
        dma((BATCH, QUARTERS, plan.far)),
        dma((BATCH, QUARTERS, plan.far)),
        dma((BATCH, QUARTERS, plan.far)),
        dma((BATCH, QUARTERS, plan.far)),
        pltpu.SemaphoreType.REGULAR((2,)),
    ]
    out = pl.pallas_call(
        functools.partial(layer_kernel, plan),
        name="mixer_layer",
        out_shape=pltpu.VMEM((BATCH, plan.out, LENGTH), BF16),
        in_specs=[hbm] * 13,
        out_specs=vmem,
        scratch_shapes=scratch,
        compiler_params=pltpu.CompilerParams(
            collective_id=0, has_side_effects=True, vmem_limit_bytes=60 * 1024 * 1024
        ),
    )(
        x_inner,
        z_gate,
        b_input,
        c_input,
        jnp.transpose(dt_raw, (2, 0, 1)),
        doc_ids,
        conv_x,
        conv_b,
        conv_c,
        dt_bias,
        decay_rate,
        norm_gain,
        w_out,
    )
    return jnp.transpose(out, (0, 2, 1))


def solution(mesh):
    members = mesh.shape["mp"]
    line = Mesh(mesh.devices.reshape(*SPLIT, members), (*SEQ, "mp"))

    def layer(*arrays):
        channels = arrays[0].shape[2] // members
        plan = Plan(SPLIT, members, channels, arrays[12].shape[1])
        placed = (
            P(None, SEQ, "mp"),
            P(None, SEQ, "mp"),
            P(None, SEQ, None),
            P(None, SEQ, None),
            P(None, SEQ, "mp"),
            P(None, SEQ),
            P(None, "mp"),
            P(),
            P(),
            P("mp"),
            P("mp"),
            P("mp"),
            P("mp", None),
        )
        return jax.shard_map(
            functools.partial(shards, plan),
            mesh=line,
            in_specs=placed,
            out_specs=P(None, SEQ, "mp"),
            check_vma=False,
        )(*arrays)

    return layer
```

```python
import functools

import jax
import jax.numpy as jnp
from jax import lax
from jax.experimental import pallas as pl
from jax.experimental.pallas import tpu as pltpu
from jax.sharding import Mesh
from jax.sharding import PartitionSpec as P

SPLIT = (8, 4, 2)
SEQ = ("sz", "sx", "sc")
INNER = 5120
EPSILON = 1e-05
BATCH = 2
LENGTH = 256
HALF = 128
QUARTERS = 4
HALO = 8
TAPS = 4
HEADDIM = 64
DSTATE = 128
REACH = 8192 // LENGTH
F32 = jnp.float32
BF16 = jnp.bfloat16
LANES = (((1,), (1,)), ((), ()))
ROWS = (((0,), (0,)), ((), ()))


def dot(a, b, dims):
    return lax.dot_general(a, b, dims, preferred_element_type=F32)


def split_two(value):
    high = value.astype(BF16)
    return high, (value - high.astype(F32)).astype(BF16)


def silu(value):
    return value / (1.0 + jnp.exp(-value))


class Plan:
    def __init__(self, split, members, channels, width):
        self.planes, self.xs, self.cores = split
        self.ring = self.xs * self.cores
        self.members = members
        self.channels = channels
        self.heads = channels // HEADDIM
        self.pairs = self.heads // 2
        self.conv = channels + 2 * DSTATE
        self.shard = channels // self.ring
        self.groups = self.shard // 16
        self.gate_rows = max(8, 1 << (self.groups - 1).bit_length())
        self.packet = self.shard + 2 * self.gate_rows
        assert REACH <= 4 * self.ring or self.planes <= 5
        self.width = width
        self.out = width // members
        self.far = members // 2


def spread(rows, plan):
    return jnp.concatenate(
        [jnp.broadcast_to(rows[q : q + 1], (16, DSTATE)) for q in range(plan.groups)], axis=0
    )


def pair_columns(cols, first, lane):
    a = jnp.broadcast_to(cols[:, first : first + 1], (cols.shape[0], 128))
    b = jnp.broadcast_to(cols[:, first + 1 : first + 2], (cols.shape[0], 128))
    return jnp.where(lane < HEADDIM, a, b)


def layer_kernel(
    plan,
    x_hbm,
    z_hbm,
    b_hbm,
    c_hbm,
    dt_hbm,
    doc_hbm,
    cx_hbm,
    cb_hbm,
    cc_hbm,
    bias_hbm,
    rate_hbm,
    gain_hbm,
    w_hbm,
    out_ref,
    bias_ref,
    rate_ref,
    gain_ref,
    xbc,
    halo,
    docs_ref,
    doc_halo,
    dt_ref,
    taps,
    z_ref,
    w_ref,
    wt,
    conv,
    masks,
    main_state,
    xw,
    y,
    scores,
    zg,
    gated,
    fsend,
    arecv,
    pref,
    qpref,
    tsend,
    usend,
    ptot,
    qtot,
    brecv,
    hsend,
    hstate,
    part,
    up_recv,
    dn_recv,
    ssend,
    srecv,
    load_sem,
    halo_send,
    halo_recv,
    a_send,
    a_recv,
    b_send,
    b_recv,
    c_send,
    c_recv,
    s_send,
    s_recv,
    up_send,
    up_got,
    dn_send,
    dn_got,
    word,
):
    ch, nh, ring, members = plan.channels, plan.heads, plan.ring, plan.members
    iz, ix, ic = lax.axis_index("sz"), lax.axis_index("sx"), lax.axis_index("sc")
    me = lax.axis_index("mp")
    rank = ix * plan.cores + ic
    place = iz * ring + rank
    blocks = plan.planes * ring

    def in_plane(r):
        return {"sx": r // plan.cores, "sc": r % plan.cores}

    def in_line(j):
        return {"sz": j // ring, "sx": (j % ring) // plan.cores, "sc": j % plan.cores}

    after, prior = in_line(place + 1), in_line(place - 1)
    up = {"mp": lax.rem(me + 1, members)}
    down = {"mp": lax.rem(me + members - 1, members)}

    has_next, has_prior = place + 1 < blocks, place > 0

    def one(flag):
        return jnp.where(flag, 1, 0)

    barrier = pltpu.get_barrier_semaphore()

    def greet(peer):
        pl.semaphore_signal(barrier, inc=1, device_id=peer, device_id_type=pl.DeviceIdType.MESH)

    for k in range(1, ring):
        greet(in_plane(lax.rem(rank + k, ring)))
    for k in range(1, members):
        greet({"mp": lax.rem(me + k, members)})
    pl.when(has_prior)(lambda: greet(prior))
    count = ring - 1 + members - 1 + one(has_next)
    above, below = {"sz": iz + 1}, {"sz": iz - 1}
    has_above, has_below = iz + 1 < plan.planes, iz > 0
    pl.when(has_below)(lambda: greet(below))
    pl.when(has_above)(lambda: greet(above))
    count = count + one(has_above) + one(has_below)

    def tell_below(at):
        pl.semaphore_signal(
            word.at[at], inc=1, device_id=below, device_id_type=pl.DeviceIdType.MESH
        )

    loads = []

    def load(src, dst):
        copy = pltpu.make_async_copy(src, dst, load_sem.at[len(loads)])
        copy.start()
        loads.append(copy)
        return copy

    done = []

    def need(copy):
        if not any(copy is other for other in done):
            copy.wait()
            done.append(copy)

    def got_waits():
        for copy in loads:
            need(copy)

    got_docs = load(doc_hbm, docs_ref)
    got_rows = []
    for m in range(BATCH):
        got_rows.append(
            [
                load(x_hbm.at[m], xbc.at[m, :, pl.ds(0, ch)]),
                load(b_hbm.at[m], xbc.at[m, :, pl.ds(ch, DSTATE)]),
                load(c_hbm.at[m], xbc.at[m, :, pl.ds(ch + DSTATE, DSTATE)]),
            ]
        )
    got_dt = [load(dt_hbm, dt_ref), load(bias_hbm, bias_ref), load(rate_hbm, rate_ref)]
    got_taps = [
        load(cx_hbm, taps.at[:, pl.ds(0, ch)]),
        load(cb_hbm, taps.at[:, pl.ds(ch, DSTATE)]),
        load(cc_hbm, taps.at[:, pl.ds(ch + DSTATE, DSTATE)]),
    ]
    got_gain = load(gain_hbm, gain_ref)

    need(got_docs)
    for copy in (*got_rows[0], *got_rows[1]):
        need(copy)
    got_z = load(z_hbm, z_ref)
    got_w = load(w_hbm, w_ref)
    pl.semaphore_wait(barrier, count)
    pl.when(has_below & has_above)(lambda: tell_below(0))

    halos = []
    for m in range(BATCH):
        halos.append(
            pltpu.make_async_remote_copy(
                src_ref=xbc.at[m, pl.ds(LENGTH - HALO, HALO)],
                dst_ref=halo.at[m],
                send_sem=halo_send.at[m],
                recv_sem=halo_recv.at[m],
                device_id=after,
                device_id_type=pl.DeviceIdType.MESH,
            )
        )
    halos.append(
        pltpu.make_async_remote_copy(
            src_ref=docs_ref.at[:, pl.ds(LENGTH - 128, 128)],
            dst_ref=doc_halo,
            send_sem=halo_send.at[BATCH],
            recv_sem=halo_recv.at[BATCH],
            device_id=after,
            device_id_type=pl.DeviceIdType.MESH,
        )
    )
    def send_halo():
        for copy in (halos[BATCH], *halos[:BATCH]):
            copy.start()

    pl.when(has_next)(send_halo)

    lane = lax.broadcasted_iota(jnp.int32, (LENGTH, 128), 1)

    docs = docs_ref[...].astype(F32)
    marks = []
    for m in range(BATCH):
        own = docs[m : m + 1]
        marks.append(own)
        for k in range(1, TAPS):
            marks.append(jnp.where(pltpu.roll(own, k, 1) == own, 1.0, 0.0))
    mark_cols = jnp.concatenate(marks, axis=0).T
    for m in range(BATCH):
        for k in range(1, TAPS):
            at = m * TAPS + k
            masks[m, k - 1] = jnp.broadcast_to(mark_cols[:, at : at + 1], (LENGTH, 128))
    for copy in got_dt:
        need(copy)
    head_row = lax.broadcasted_iota(jnp.int32, (16, LENGTH), 0)
    bias = jnp.zeros((16, LENGTH), F32)
    rate = jnp.zeros((16, LENGTH), F32)
    for h in range(nh):
        bias = jnp.where(head_row == h, bias_ref[h], bias)
        rate = jnp.where(head_row == h, rate_ref[h], rate)
    step_rows, log_parts = [], []
    for m in range(BATCH):
        raw = dt_ref[:, m, :]
        if nh < 16:
            raw = jnp.concatenate([raw, jnp.zeros((16 - nh, LENGTH), F32)], axis=0)
        shifted = raw + bias
        step = jnp.maximum(shifted, 0.0) + jnp.log1p(jnp.exp(-jnp.abs(shifted)))
        step_rows.append(step)
        log_parts.append(-(step * rate))
    log_step = jnp.concatenate(log_parts, axis=0)
    hi = log_step.astype(BF16)
    rest = log_step - hi.astype(F32)
    mid = rest.astype(BF16)
    low = (rest - mid.astype(F32)).astype(BF16)
    before = lax.broadcasted_iota(jnp.int32, (LENGTH, LENGTH), 0) <= lax.broadcasted_iota(
        jnp.int32, (LENGTH, LENGTH), 1
    )
    upper = jnp.where(before, 1.0, 0.0).astype(BF16)
    sums = dot(jnp.concatenate([low, mid, hi], axis=0), upper, (((1,), (0,)), ((), ())))
    span = BATCH * 16
    log_cum = sums[0:span] + sums[span : 2 * span] + sums[2 * span : 3 * span]
    log_rows = [log_cum[m * 16 : (m + 1) * 16] for m in range(BATCH)]
    row_mats = list(log_rows)
    ends = []
    for m in range(BATCH):
        end = log_rows[m][:, LENGTH - 1 : LENGTH]
        ends.append(end)
        keep = jnp.where(docs[m : m + 1] == docs[m : m + 1, LENGTH - 1 : LENGTH], 1.0, 0.0)
        row_mats.append(jnp.exp(jnp.minimum(end - log_rows[m], 0.0)) * step_rows[m] * keep)
    for m in range(BATCH):
        row_mats.append(jnp.exp(log_rows[m]))
    row_mats.append(jnp.zeros((128 - 3 * span, LENGTH), F32))
    cols = jnp.concatenate(row_mats, axis=0).T
    log_col, weight_col, entry_col = 0, span, 2 * span

    for copy in got_taps:
        need(copy)
    tap = taps[...].astype(F32)
    tiles = plan.conv // 128
    def convolve(m):
        for j in range(tiles):
            at = slice(j * 128, (j + 1) * 128)
            rows = xbc[m, :, at].astype(F32)
            total = rows * tap[TAPS - 1 : TAPS, at]
            for k in range(1, TAPS):
                weight = tap[TAPS - 1 - k : TAPS - k, at]
                total = total + (pltpu.roll(rows, k, 0) * weight) * masks[m, k - 1]
            total = silu(total)
            conv[m, :, at] = total.astype(BF16)
            if j < plan.pairs:
                scale = pair_columns(cols, weight_col + m * 16 + 2 * j, lane)
                xw[m, :, at] = (total.astype(BF16).astype(F32) * scale).astype(BF16)
        xw[m, 0:HALO, :] = jnp.zeros((HALO, ch), BF16)
        main_state[m] = dot(xw[m], conv[m, :, ch : ch + DSTATE], ROWS)

    def turn_weights():
        need(got_w)
        for j in range(plan.width // 128):
            wt[j * 128 : (j + 1) * 128, :] = w_ref[:, j * 128 : (j + 1) * 128].T

    def gate_inputs(m):
        need(got_z)
        for j in range(plan.pairs):
            at = slice(j * 128, (j + 1) * 128)
            zg[m, :, at] = silu(z_ref[m, :, at].astype(F32))

    group_row = lax.broadcasted_iota(jnp.int32, (ring * plan.gate_rows, 16), 0)
    group_head = lax.broadcasted_iota(jnp.int32, (ring * plan.gate_rows, 16), 1)
    bits = plan.gate_rows.bit_length() - 1
    shard_of, group_of = group_row >> bits, group_row & (plan.gate_rows - 1)
    picks = (((shard_of * plan.groups + group_of) >> 2) == group_head) & (group_of < plan.groups)
    pick = jnp.where(picks, 1.0, 0.0).astype(BF16)
    plain = (((1,), (0,)), ((), ()))
    gate_parts = []
    for m in range(BATCH):
        gate_hi, gate_lo = split_two(jnp.broadcast_to(jnp.exp(ends[m]), (16, DSTATE)))
        gate_parts.append((dot(pick, gate_hi, plain), dot(pick, gate_lo, plain)))
    convolve(0)
    pl.when(has_prior)(halos[BATCH].wait_recv)
    doc_before = jnp.where(has_prior, doc_halo[...].astype(F32), -1.0)
    row8 = lax.broadcasted_iota(jnp.int32, (HALO, 128), 0)

    def edge_mask(m, k):
        mask = masks[m, k - 1, 0:HALO]
        for t in range(k):
            at = 128 - k + t
            same = docs[m : m + 1, t : t + 1] == doc_before[m : m + 1, at : at + 1]
            mask = jnp.where(row8 == t, jnp.where(same, 1.0, 0.0), mask)
        return mask

    def exchange(m, source, target, peers_send, peers_recv):
        copies = []
        for k in range(1, ring):
            to = lax.rem(rank + k, ring)
            copies.append(
                pltpu.make_async_remote_copy(
                    src_ref=source.at[m, to],
                    dst_ref=target(to),
                    send_sem=peers_send.at[m, k],
                    recv_sem=peers_recv.at[m, k],
                    device_id=in_plane(to),
                    device_id_type=pl.DeviceIdType.MESH,
                )
            )
        return copies

    a_copies = []
    for m in range(BATCH):
        if m > 0:
            convolve(m)
        pl.when(has_prior)(halos[m].wait_recv)
        same = [None, *(edge_mask(m, k) for k in range(1, TAPS))]
        scaled = []
        for j in range(tiles):
            at = slice(j * 128, (j + 1) * 128)
            lead = jnp.where(has_prior, halo[m, :, at].astype(F32), 0.0)
            own = xbc[m, 0:HALO, at].astype(F32)
            both = jnp.concatenate([lead, own], axis=0)
            total = own * tap[TAPS - 1 : TAPS, at]
            for k in range(1, TAPS):
                weight = tap[TAPS - 1 - k : TAPS - k, at]
                total = total + (pltpu.roll(both, k, 0)[HALO : 2 * HALO] * weight) * same[k]
            total = silu(total).astype(BF16)
            conv[m, 0:HALO, at] = total
            if j < plan.pairs:
                scale = pair_columns(cols[0:HALO], weight_col + m * 16 + 2 * j, lane[0:HALO])
                scaled.append((total.astype(F32) * scale).astype(BF16))
            if j == plan.pairs:
                first_b = total
        edge_state = dot(jnp.concatenate(scaled, axis=1), first_b, ROWS)
        state = (main_state[m] + edge_state).astype(BF16)
        carried_end = docs[m : m + 1, LENGTH - 1 : LENGTH] == doc_before[m : m + 1, 127:128]
        carried_end = jnp.where(carried_end, 1.0, 0.0)
        hi_rows = (gate_parts[m][0] * carried_end).astype(BF16)
        lo_rows = (gate_parts[m][1] * carried_end).astype(BF16)
        for r in range(ring):
            fsend[m, r, 0 : plan.shard] = state[r * plan.shard : (r + 1) * plan.shard]
            at = slice(r * plan.gate_rows, (r + 1) * plan.gate_rows)
            fsend[m, r, plan.shard : plan.packet] = jnp.concatenate(
                [hi_rows[at], lo_rows[at]], axis=0
            )
        copies = exchange(m, fsend, lambda to, m=m: arecv.at[m, rank], a_send, a_recv)
        for copy in copies:
            copy.start()
        a_copies.append(copies)
        arecv[m, pl.ds(rank, 1)] = fsend[m, pl.ds(rank, 1)]

    def scores_of(m):
        t_pos = lax.broadcasted_iota(jnp.int32, (LENGTH, LENGTH), 0)
        s_pos = lax.broadcasted_iota(jnp.int32, (LENGTH, LENGTH), 1)
        doc_t = mark_cols[:, m * TAPS : m * TAPS + 1]
        keep = (s_pos <= t_pos) & (doc_t == docs[m : m + 1])
        full = dot(conv[m, :, ch + DSTATE : ch + 2 * DSTATE], conv[m, :, ch : ch + DSTATE], LANES)
        scores[m] = jnp.where(keep, full, 0.0)

    def inner_of(m):
        low_lane = lane < HEADDIM
        for j in range(plan.pairs):
            at = slice(j * 128, (j + 1) * 128)
            xs = conv[m, :, at]
            xs_a = jnp.where(low_lane, xs, jnp.zeros_like(xs))
            xs_b = jnp.where(low_lane, jnp.zeros_like(xs), xs)
            for half in range(2):
                t0, s1 = half * HALF, (half + 1) * HALF
                base = scores[m, t0 : t0 + HALF, 0:s1]
                mixes = []
                for h in (2 * j, 2 * j + 1):
                    t_log = cols[t0 : t0 + HALF, log_col + m * 16 + h : log_col + m * 16 + h + 1]
                    s_log = log_rows[m][h : h + 1, 0:s1]
                    decay = jnp.exp(jnp.minimum(t_log - s_log, 0.0))
                    mixes.append((base * step_rows[m][h : h + 1, 0:s1] * decay).astype(BF16))
                y[m, t0 : t0 + HALF, at] = dot(
                    jnp.concatenate(mixes, axis=1),
                    jnp.concatenate([xs_a[0:s1], xs_b[0:s1]], axis=0),
                    (((1,), (0,)), ((), ())),
                )

    def gate_both(m):
        carried = mark_cols[:, m * TAPS : m * TAPS + 1] == doc_before[m : m + 1, 127:128]
        for j in range(plan.pairs):
            at = slice(j * 128, (j + 1) * 128)
            opened = zg[m, :, at]
            y[m, :, at] = y[m, :, at] * opened
            entry = pair_columns(cols, entry_col + m * 16 + 2 * j, lane)
            zg[m, :, at] = jnp.where(carried, entry, 0.0) * opened

    def unpack(packet):
        packet = packet.astype(F32)
        split = plan.shard + plan.gate_rows
        return packet[0 : plan.shard], packet[plan.shard : split] + packet[split:]

    def pack(ref, m, total, product):
        ref[m, 0 : plan.shard] = total.astype(BF16)
        hi_rows, lo_rows = split_two(product)
        ref[m, plan.shard : plan.packet] = jnp.concatenate([hi_rows, lo_rows], axis=0)

    def ahead(source, m, slot, k):
        return pltpu.make_async_remote_copy(
            src_ref=source.at[m],
            dst_ref=brecv.at[m, slot],
            send_sem=b_send.at[m, slot],
            recv_sem=b_recv.at[m, slot],
            device_id={"sz": iz + k},
            device_id_type=pl.DeviceIdType.MESH,
        )

    jumps = [(0, 1), (1, 1), (2, 3)]
    b_copies = [
        [ahead(tsend if slot == 0 else usend, m, slot, k) for slot, k in jumps] for m in range(BATCH)
    ]

    def goes(k):
        return iz + k < plan.planes

    def plane_total(m):
        for copy in a_copies[m]:
            copy.wait_recv()
        total = jnp.zeros((plan.shard, DSTATE), F32)
        product = jnp.ones((plan.gate_rows, DSTATE), F32)
        for d in range(ring):
            pref[m, d] = total
            qpref[m, d] = product
            fresh, gates = unpack(arecv[m, d])
            total = spread(gates, plan) * total + fresh
            product = product * gates
        pack(tsend, m, total, product)
        ptot[m] = total
        qtot[m] = product
        pl.when(has_above)(b_copies[m][0].start)

    def two_planes(m):
        pl.when(has_below)(b_copies[m][0].wait_recv)
        lower, gates = unpack(brecv[m, 0])
        lower = jnp.where(has_below, lower, 0.0)
        gates = jnp.where(has_below, gates, 0.0)
        product = qtot[m]
        pack(usend, m, spread(product, plan) * lower + ptot[m], product * gates)
        pl.when(has_above)(b_copies[m][1].start)
        pl.when(goes(3))(b_copies[m][2].start)

    gate_inputs(0)
    scores_of(0)
    pl.when(goes(2))(lambda: pl.semaphore_wait(word.at[0], 1))
    pl.when(has_below & goes(2))(lambda: tell_below(1))
    inner_of(0)
    gate_both(0)
    plane_total(0)
    plane_total(1)
    scores_of(1)
    inner_of(1)
    pl.when(goes(3))(lambda: pl.semaphore_wait(word.at[1], 1))
    two_planes(0)
    two_planes(1)
    gate_inputs(1)
    gate_both(1)
    turn_weights()
    c_copies = []
    for m in range(BATCH):
        pl.when(has_below)(b_copies[m][1].wait_recv)
        pl.when(iz >= 3)(b_copies[m][2].wait_recv)
        near, gates = unpack(brecv[m, 1])
        remote, _ = unpack(brecv[m, 2])
        incoming = spread(gates, plan) * jnp.where(iz >= 3, remote, 0.0) + near
        incoming = jnp.where(has_below, incoming, 0.0)
        for d in range(ring):
            entering = pref[m, d] + spread(qpref[m, d], plan) * incoming
            hsend[m, d] = entering.astype(BF16)
        home = pl.ds(pl.multiple_of(rank * plan.shard, 16), plan.shard)
        copies = exchange(m, hsend, lambda to, m=m: hstate.at[m, home], c_send, c_recv)
        for copy in copies:
            copy.start()
        c_copies.append(copies)
        hstate[m, home] = hsend[m, rank]

    quarter = plan.out // QUARTERS

    def hops(q, upward):
        return plan.far if (q < QUARTERS // 2) == upward else plan.far - 1

    def owner_at(distance, upward):
        return lax.rem(me + distance if upward else me + members - distance, members)

    def arrow(m, q, hop, upward):
        buffer, send, got, to = (
            (up_recv, up_send, up_got, up) if upward else (dn_recv, dn_send, dn_got, down)
        )
        rows = pl.ds(q * quarter, quarter)
        return pltpu.make_async_remote_copy(
            src_ref=part.at[m, owner_at(hops(q, upward) - hop, upward), rows],
            dst_ref=buffer.at[m, hop, rows],
            send_sem=send.at[m, q, hop],
            recv_sem=got.at[m, q, hop],
            device_id=to,
            device_id_type=pl.DeviceIdType.MESH,
        )

    arrows = {}
    s_copies = []
    need(got_gain)
    gain = gain_ref[...].reshape(1, ch)

    def project(m, distance, upward):
        owner = owner_at(distance, upward)
        rows = pl.ds(pl.multiple_of(owner * plan.out, 16), plan.out)
        part[m, owner] = dot(wt[rows, :], gated[m], LANES).astype(BF16)

    def shoot(m, hop, upward, pieces):
        for q in pieces:
            if hop < hops(q, upward):
                if hop > 0:
                    arrows[m, q, hop - 1, upward].wait_recv()
                    buffer = up_recv if upward else dn_recv
                    owner = owner_at(hops(q, upward) - hop, upward)
                    rows = slice(q * quarter, (q + 1) * quarter)
                    total = part[m, owner, rows].astype(F32) + buffer[m, hop - 1, rows].astype(F32)
                    part[m, owner, rows] = total.astype(BF16)
                arrows[m, q, hop, upward] = arrow(m, q, hop, upward)
                arrows[m, q, hop, upward].start()

    early, late = range(QUARTERS // 2), range(QUARTERS // 2, QUARTERS)

    def first_round(m):
        project(m, plan.far, True)
        shoot(m, 0, True, early)
        shoot(m, 0, False, late)
        if plan.far > 1:
            project(m, plan.far - 1, True)
            shoot(m, 0, True, late)
            project(m, plan.far - 1, False)
            shoot(m, 0, False, early)

    def next_round(m, hop):
        if hop + 1 < plan.far:
            project(m, plan.far - 1 - hop, True)
            project(m, plan.far - 1 - hop, False)
        shoot(m, hop, True, early)
        shoot(m, hop, False, late)
        shoot(m, hop, True, late)
        shoot(m, hop, False, early)

    def carry(m):
        for copy in c_copies[m]:
            copy.wait_recv()
        squares = jnp.zeros((LENGTH, 128), F32)
        outer = dot(conv[m, :, ch + DSTATE : ch + 2 * DSTATE], hstate[m], LANES)
        for j in range(plan.pairs):
            at = slice(j * 128, (j + 1) * 128)
            mixed = y[m, :, at] + zg[m, :, at] * outer[:, at]
            squares = squares + mixed * mixed
            gated[m, :, at] = (mixed * gain[:, at]).astype(BF16)
        first_round(m)
        square_hi, square_lo = split_two(squares)
        ones = jnp.ones((8, 128), BF16)
        square_rows = dot(ones, square_hi, LANES) + dot(ones, square_lo, LANES)
        ssend[m] = square_rows[0:1]
        for k in range(1, members):
            copy = pltpu.make_async_remote_copy(
                src_ref=ssend.at[m],
                dst_ref=srecv.at[m, k],
                send_sem=s_send.at[m, k],
                recv_sem=s_recv.at[m, k],
                device_id={"mp": lax.rem(me + k, members)},
                device_id_type=pl.DeviceIdType.MESH,
            )
            copy.start()
            s_copies.append(copy)

    carry(0)
    carry(1)
    for hop in range(1, plan.far):
        for m in range(BATCH):
            next_round(m, hop)
    for m in range(BATCH):
        project(m, 0, True)

    for copy in s_copies:
        copy.wait_recv()
    for m in range(BATCH):
        square = ssend[m]
        for k in range(1, members):
            square = square + srecv[m, k]
        scale = lax.rsqrt(square / INNER + EPSILON)
        for q in (*late, *early):
            rows = slice(q * quarter, (q + 1) * quarter)
            total = part[m, me, rows].astype(F32)
            for upward in (True, False):
                last = hops(q, upward) - 1
                if last >= 0:
                    arrows[m, q, last, upward].wait_recv()
                    buffer = up_recv if upward else dn_recv
                    total = total + buffer[m, last, rows].astype(F32)
            out_ref[m, rows, :] = (total * scale).astype(BF16)

    def sent():
        for copy in halos:
            copy.wait_send()

    pl.when(has_next)(sent)
    for group in (*a_copies, *c_copies, s_copies, list(arrows.values())):
        for copy in group:
            copy.wait_send()
    for m in range(BATCH):
        for slot, k in jumps:
            pl.when(goes(k))(b_copies[m][slot].wait_send)


def shards(
    plan,
    x_inner,
    z_gate,
    b_input,
    c_input,
    dt_raw,
    doc_ids,
    conv_x,
    conv_b,
    conv_c,
    dt_bias,
    decay_rate,
    norm_gain,
    w_out,
):
    hbm = pl.BlockSpec(memory_space=pltpu.HBM)
    vmem = pl.BlockSpec(memory_space=pltpu.VMEM)
    ch, ring, members = plan.channels, plan.ring, plan.members
    dma = pltpu.SemaphoreType.DMA
    scratch = [
        pltpu.SMEM((plan.heads,), F32),
        pltpu.SMEM((plan.heads,), F32),
        pltpu.VMEM((ch,), F32),
        pltpu.VMEM((BATCH, LENGTH, plan.conv), BF16),
        pltpu.VMEM((BATCH, HALO, plan.conv), BF16),
        pltpu.VMEM((BATCH, LENGTH), jnp.int32),
        pltpu.VMEM((BATCH, 128), jnp.int32),
        pltpu.VMEM((plan.heads, BATCH, LENGTH), F32),
        pltpu.VMEM((TAPS, plan.conv), BF16),
        pltpu.VMEM((BATCH, LENGTH, ch), BF16),
        pltpu.VMEM((ch, plan.width), BF16),
        pltpu.VMEM((plan.width, ch), BF16),
        pltpu.VMEM((BATCH, LENGTH, plan.conv), BF16),
        pltpu.VMEM((BATCH, TAPS - 1, LENGTH, 128), F32),
        pltpu.VMEM((BATCH, ch, DSTATE), F32),
        pltpu.VMEM((BATCH, LENGTH, ch), BF16),
        pltpu.VMEM((BATCH, LENGTH, ch), F32),
        pltpu.VMEM((BATCH, LENGTH, LENGTH), F32),
        pltpu.VMEM((BATCH, LENGTH, ch), F32),
        pltpu.VMEM((BATCH, LENGTH, ch), BF16),
        pltpu.VMEM((BATCH, ring, plan.packet, DSTATE), BF16),
        pltpu.VMEM((BATCH, ring, plan.packet, DSTATE), BF16),
        pltpu.VMEM((BATCH, ring, plan.shard, DSTATE), F32),
        pltpu.VMEM((BATCH, ring, plan.gate_rows, DSTATE), F32),
        pltpu.VMEM((BATCH, plan.packet, DSTATE), BF16),
        pltpu.VMEM((BATCH, plan.packet, DSTATE), BF16),
        pltpu.VMEM((BATCH, plan.shard, DSTATE), F32),
        pltpu.VMEM((BATCH, plan.gate_rows, DSTATE), F32),
        pltpu.VMEM((BATCH, 3, plan.packet, DSTATE), BF16),
        pltpu.VMEM((BATCH, ring, plan.shard, DSTATE), BF16),
        pltpu.VMEM((BATCH, ch, DSTATE), BF16),
        pltpu.VMEM((BATCH, members, plan.out, LENGTH), BF16),
        pltpu.VMEM((BATCH, plan.far, plan.out, LENGTH), BF16),
        pltpu.VMEM((BATCH, plan.far, plan.out, LENGTH), BF16),
        pltpu.VMEM((BATCH, 1, LENGTH), F32),
        pltpu.VMEM((BATCH, members, 1, LENGTH), F32),
        dma((16,)),
        dma((BATCH + 1,)),
        dma((BATCH + 1,)),
        dma((BATCH, ring)),
        dma((BATCH, ring)),
        dma((BATCH, 3)),
        dma((BATCH, 3)),
        dma((BATCH, ring)),
        dma((BATCH, ring)),
        dma((BATCH, members)),
        dma((BATCH, members)),
        dma((BATCH, QUARTERS, plan.far)),
        dma((BATCH, QUARTERS, plan.far)),
        dma((BATCH, QUARTERS, plan.far)),
        dma((BATCH, QUARTERS, plan.far)),
        pltpu.SemaphoreType.REGULAR((2,)),
    ]
    out = pl.pallas_call(
        functools.partial(layer_kernel, plan),
        name="mixer_layer",
        out_shape=pltpu.VMEM((BATCH, plan.out, LENGTH), BF16),
        in_specs=[hbm] * 13,
        out_specs=vmem,
        scratch_shapes=scratch,
        compiler_params=pltpu.CompilerParams(
            collective_id=0, has_side_effects=True, vmem_limit_bytes=60 * 1024 * 1024
        ),
    )(
        x_inner,
        z_gate,
        b_input,
        c_input,
        jnp.transpose(dt_raw, (2, 0, 1)),
        doc_ids,
        conv_x,
        conv_b,
        conv_c,
        dt_bias,
        decay_rate,
        norm_gain,
        w_out,
    )
    return jnp.transpose(out, (0, 2, 1))


def solution(mesh):
    members = mesh.shape["mp"]
    line = Mesh(mesh.devices.reshape(*SPLIT, members), (*SEQ, "mp"))

    def layer(*arrays):
        channels = arrays[0].shape[2] // members
        plan = Plan(SPLIT, members, channels, arrays[12].shape[1])
        placed = (
            P(None, SEQ, "mp"),
            P(None, SEQ, "mp"),
            P(None, SEQ, None),
            P(None, SEQ, None),
            P(None, SEQ, "mp"),
            P(None, SEQ),
            P(None, "mp"),
            P(),
            P(),
            P("mp"),
            P("mp"),
            P("mp"),
            P("mp", None),
        )
        return jax.shard_map(
            functools.partial(shards, plan),
            mesh=line,
            in_specs=placed,
            out_specs=P(None, SEQ, "mp"),
            check_vma=False,
        )(*arrays)

    return layer
```

```python
import functools

import jax
import jax.numpy as jnp
from jax import lax
from jax.experimental import pallas as pl
from jax.experimental.pallas import tpu as pltpu
from jax.sharding import Mesh
from jax.sharding import PartitionSpec as P

SPLIT = (8, 4, 2)
SEQ = ("sz", "sx", "sc")
INNER = 5120
EPSILON = 1e-05
BATCH = 2
LENGTH = 256
HALF = 128
QUARTERS = 4
HALO = 8
TAPS = 4
HEADDIM = 64
DSTATE = 128
REACH = 8192 // LENGTH
F32 = jnp.float32
BF16 = jnp.bfloat16
LANES = (((1,), (1,)), ((), ()))
ROWS = (((0,), (0,)), ((), ()))


def dot(a, b, dims):
    return lax.dot_general(a, b, dims, preferred_element_type=F32)


def split_two(value):
    high = value.astype(BF16)
    return high, (value - high.astype(F32)).astype(BF16)


def silu(value):
    return value / (1.0 + jnp.exp(-value))


class Plan:
    def __init__(self, split, members, channels, width):
        self.planes, self.xs, self.cores = split
        self.ring = self.xs * self.cores
        self.members = members
        self.channels = channels
        self.heads = channels // HEADDIM
        self.pairs = self.heads // 2
        self.conv = channels + 2 * DSTATE
        self.shard = channels // self.ring
        self.groups = self.shard // 16
        self.gate_rows = max(8, 1 << (self.groups - 1).bit_length())
        self.packet = self.shard + 2 * self.gate_rows
        assert REACH <= 4 * self.ring or self.planes <= 5
        self.width = width
        self.out = width // members
        self.far = members // 2


def spread(rows, plan):
    return jnp.concatenate(
        [jnp.broadcast_to(rows[q : q + 1], (16, DSTATE)) for q in range(plan.groups)], axis=0
    )


def pair_columns(cols, first, lane):
    a = jnp.broadcast_to(cols[:, first : first + 1], (cols.shape[0], 128))
    b = jnp.broadcast_to(cols[:, first + 1 : first + 2], (cols.shape[0], 128))
    return jnp.where(lane < HEADDIM, a, b)


def layer_kernel(
    plan,
    x_hbm,
    z_hbm,
    b_hbm,
    c_hbm,
    dt_hbm,
    doc_hbm,
    cx_hbm,
    cb_hbm,
    cc_hbm,
    bias_hbm,
    rate_hbm,
    gain_hbm,
    w_hbm,
    out_ref,
    bias_ref,
    rate_ref,
    gain_ref,
    xbc,
    halo,
    docs_ref,
    doc_halo,
    dt_ref,
    taps,
    z_ref,
    w_ref,
    wt,
    conv,
    masks,
    main_state,
    xw,
    y,
    scores,
    zg,
    gated,
    fsend,
    arecv,
    pref,
    qpref,
    tsend,
    usend,
    ptot,
    qtot,
    brecv,
    hsend,
    hstate,
    part,
    up_recv,
    dn_recv,
    ssend,
    srecv,
    load_sem,
    halo_send,
    halo_recv,
    a_send,
    a_recv,
    b_send,
    b_recv,
    c_send,
    c_recv,
    s_send,
    s_recv,
    up_send,
    up_got,
    dn_send,
    dn_got,
    word,
):
    ch, nh, ring, members = plan.channels, plan.heads, plan.ring, plan.members
    iz, ix, ic = lax.axis_index("sz"), lax.axis_index("sx"), lax.axis_index("sc")
    me = lax.axis_index("mp")
    rank = ix * plan.cores + ic
    place = iz * ring + rank
    blocks = plan.planes * ring

    def in_plane(r):
        return {"sx": r // plan.cores, "sc": r % plan.cores}

    def in_line(j):
        return {"sz": j // ring, "sx": (j % ring) // plan.cores, "sc": j % plan.cores}

    after, prior = in_line(place + 1), in_line(place - 1)
    up = {"mp": lax.rem(me + 1, members)}
    down = {"mp": lax.rem(me + members - 1, members)}

    has_next, has_prior = place + 1 < blocks, place > 0

    def one(flag):
        return jnp.where(flag, 1, 0)

    barrier = pltpu.get_barrier_semaphore()

    def greet(peer):
        pl.semaphore_signal(barrier, inc=1, device_id=peer, device_id_type=pl.DeviceIdType.MESH)

    for k in range(1, ring):
        greet(in_plane(lax.rem(rank + k, ring)))
    greet(up)
    greet(down)
    pl.when(has_prior)(lambda: greet(prior))
    count = ring - 1 + 2 + one(has_next)
    above, below = {"sz": iz + 1}, {"sz": iz - 1}
    has_above, has_below = iz + 1 < plan.planes, iz > 0
    pl.when(has_below)(lambda: greet(below))
    pl.when(has_above)(lambda: greet(above))
    count = count + one(has_above) + one(has_below)

    def tell_below(at):
        pl.semaphore_signal(
            word.at[at], inc=1, device_id=below, device_id_type=pl.DeviceIdType.MESH
        )

    loads = []

    def load(src, dst):
        copy = pltpu.make_async_copy(src, dst, load_sem.at[len(loads)])
        copy.start()
        loads.append(copy)
        return copy

    done = []

    def need(copy):
        if not any(copy is other for other in done):
            copy.wait()
            done.append(copy)

    def got_waits():
        for copy in loads:
            need(copy)

    got_docs = load(doc_hbm, docs_ref)
    got_rows = []
    for m in range(BATCH):
        got_rows.append(
            [
                load(x_hbm.at[m], xbc.at[m, :, pl.ds(0, ch)]),
                load(b_hbm.at[m], xbc.at[m, :, pl.ds(ch, DSTATE)]),
                load(c_hbm.at[m], xbc.at[m, :, pl.ds(ch + DSTATE, DSTATE)]),
            ]
        )
    got_dt = [load(dt_hbm, dt_ref), load(bias_hbm, bias_ref), load(rate_hbm, rate_ref)]
    got_taps = [
        load(cx_hbm, taps.at[:, pl.ds(0, ch)]),
        load(cb_hbm, taps.at[:, pl.ds(ch, DSTATE)]),
        load(cc_hbm, taps.at[:, pl.ds(ch + DSTATE, DSTATE)]),
    ]
    got_gain = load(gain_hbm, gain_ref)

    need(got_docs)
    for copy in (*got_rows[0], *got_rows[1]):
        need(copy)
    got_z = load(z_hbm, z_ref)
    got_w = load(w_hbm, w_ref)
    pl.semaphore_wait(barrier, count)
    pl.when(has_below & has_above)(lambda: tell_below(0))

    halos = []
    for m in range(BATCH):
        halos.append(
            pltpu.make_async_remote_copy(
                src_ref=xbc.at[m, pl.ds(LENGTH - HALO, HALO)],
                dst_ref=halo.at[m],
                send_sem=halo_send.at[m],
                recv_sem=halo_recv.at[m],
                device_id=after,
                device_id_type=pl.DeviceIdType.MESH,
            )
        )
    halos.append(
        pltpu.make_async_remote_copy(
            src_ref=docs_ref.at[:, pl.ds(LENGTH - 128, 128)],
            dst_ref=doc_halo,
            send_sem=halo_send.at[BATCH],
            recv_sem=halo_recv.at[BATCH],
            device_id=after,
            device_id_type=pl.DeviceIdType.MESH,
        )
    )
    def send_halo():
        for copy in (halos[BATCH], *halos[:BATCH]):
            copy.start()

    pl.when(has_next)(send_halo)

    lane = lax.broadcasted_iota(jnp.int32, (LENGTH, 128), 1)

    docs = docs_ref[...].astype(F32)
    marks = []
    for m in range(BATCH):
        own = docs[m : m + 1]
        marks.append(own)
        for k in range(1, TAPS):
            marks.append(jnp.where(pltpu.roll(own, k, 1) == own, 1.0, 0.0))
    mark_cols = jnp.concatenate(marks, axis=0).T
    for m in range(BATCH):
        for k in range(1, TAPS):
            at = m * TAPS + k
            masks[m, k - 1] = jnp.broadcast_to(mark_cols[:, at : at + 1], (LENGTH, 128))
    for copy in got_dt:
        need(copy)
    head_row = lax.broadcasted_iota(jnp.int32, (16, LENGTH), 0)
    bias = jnp.zeros((16, LENGTH), F32)
    rate = jnp.zeros((16, LENGTH), F32)
    for h in range(nh):
        bias = jnp.where(head_row == h, bias_ref[h], bias)
        rate = jnp.where(head_row == h, rate_ref[h], rate)
    step_rows, log_parts = [], []
    for m in range(BATCH):
        raw = dt_ref[:, m, :]
        if nh < 16:
            raw = jnp.concatenate([raw, jnp.zeros((16 - nh, LENGTH), F32)], axis=0)
        shifted = raw + bias
        step = jnp.maximum(shifted, 0.0) + jnp.log1p(jnp.exp(-jnp.abs(shifted)))
        step_rows.append(step)
        log_parts.append(-(step * rate))
    log_step = jnp.concatenate(log_parts, axis=0)
    hi = log_step.astype(BF16)
    rest = log_step - hi.astype(F32)
    mid = rest.astype(BF16)
    low = (rest - mid.astype(F32)).astype(BF16)
    before = lax.broadcasted_iota(jnp.int32, (LENGTH, LENGTH), 0) <= lax.broadcasted_iota(
        jnp.int32, (LENGTH, LENGTH), 1
    )
    upper = jnp.where(before, 1.0, 0.0).astype(BF16)
    sums = dot(jnp.concatenate([low, mid, hi], axis=0), upper, (((1,), (0,)), ((), ())))
    span = BATCH * 16
    log_cum = sums[0:span] + sums[span : 2 * span] + sums[2 * span : 3 * span]
    log_rows = [log_cum[m * 16 : (m + 1) * 16] for m in range(BATCH)]
    row_mats = list(log_rows)
    ends = []
    for m in range(BATCH):
        end = log_rows[m][:, LENGTH - 1 : LENGTH]
        ends.append(end)
        keep = jnp.where(docs[m : m + 1] == docs[m : m + 1, LENGTH - 1 : LENGTH], 1.0, 0.0)
        row_mats.append(jnp.exp(jnp.minimum(end - log_rows[m], 0.0)) * step_rows[m] * keep)
    for m in range(BATCH):
        row_mats.append(jnp.exp(log_rows[m]))
    row_mats.append(jnp.zeros((128 - 3 * span, LENGTH), F32))
    cols = jnp.concatenate(row_mats, axis=0).T
    log_col, weight_col, entry_col = 0, span, 2 * span

    for copy in got_taps:
        need(copy)
    tap = taps[...].astype(F32)
    tiles = plan.conv // 128
    def convolve(m):
        for j in range(tiles):
            at = slice(j * 128, (j + 1) * 128)
            rows = xbc[m, :, at].astype(F32)
            total = rows * tap[TAPS - 1 : TAPS, at]
            for k in range(1, TAPS):
                weight = tap[TAPS - 1 - k : TAPS - k, at]
                total = total + (pltpu.roll(rows, k, 0) * weight) * masks[m, k - 1]
            total = silu(total)
            conv[m, :, at] = total.astype(BF16)
            if j < plan.pairs:
                scale = pair_columns(cols, weight_col + m * 16 + 2 * j, lane)
                xw[m, :, at] = (total.astype(BF16).astype(F32) * scale).astype(BF16)
        xw[m, 0:HALO, :] = jnp.zeros((HALO, ch), BF16)
        main_state[m] = dot(xw[m], conv[m, :, ch : ch + DSTATE], ROWS)

    def turn_weights():
        need(got_w)
        for j in range(plan.width // 128):
            wt[j * 128 : (j + 1) * 128, :] = w_ref[:, j * 128 : (j + 1) * 128].T

    def gate_inputs(m):
        need(got_z)
        for j in range(plan.pairs):
            at = slice(j * 128, (j + 1) * 128)
            zg[m, :, at] = silu(z_ref[m, :, at].astype(F32))

    group_row = lax.broadcasted_iota(jnp.int32, (ring * plan.gate_rows, 16), 0)
    group_head = lax.broadcasted_iota(jnp.int32, (ring * plan.gate_rows, 16), 1)
    bits = plan.gate_rows.bit_length() - 1
    shard_of, group_of = group_row >> bits, group_row & (plan.gate_rows - 1)
    picks = (((shard_of * plan.groups + group_of) >> 2) == group_head) & (group_of < plan.groups)
    pick = jnp.where(picks, 1.0, 0.0).astype(BF16)
    plain = (((1,), (0,)), ((), ()))
    gate_parts = []
    for m in range(BATCH):
        gate_hi, gate_lo = split_two(jnp.broadcast_to(jnp.exp(ends[m]), (16, DSTATE)))
        gate_parts.append((dot(pick, gate_hi, plain), dot(pick, gate_lo, plain)))
    convolve(0)
    pl.when(has_prior)(halos[BATCH].wait_recv)
    doc_before = jnp.where(has_prior, doc_halo[...].astype(F32), -1.0)
    row8 = lax.broadcasted_iota(jnp.int32, (HALO, 128), 0)

    def edge_mask(m, k):
        mask = masks[m, k - 1, 0:HALO]
        for t in range(k):
            at = 128 - k + t
            same = docs[m : m + 1, t : t + 1] == doc_before[m : m + 1, at : at + 1]
            mask = jnp.where(row8 == t, jnp.where(same, 1.0, 0.0), mask)
        return mask

    def exchange(m, source, target, peers_send, peers_recv):
        copies = []
        for k in range(1, ring):
            to = lax.rem(rank + k, ring)
            copies.append(
                pltpu.make_async_remote_copy(
                    src_ref=source.at[m, to],
                    dst_ref=target(to),
                    send_sem=peers_send.at[m, k],
                    recv_sem=peers_recv.at[m, k],
                    device_id=in_plane(to),
                    device_id_type=pl.DeviceIdType.MESH,
                )
            )
        return copies

    a_copies = []
    for m in range(BATCH):
        if m > 0:
            convolve(m)
        pl.when(has_prior)(halos[m].wait_recv)
        same = [None, *(edge_mask(m, k) for k in range(1, TAPS))]
        scaled = []
        for j in range(tiles):
            at = slice(j * 128, (j + 1) * 128)
            lead = jnp.where(has_prior, halo[m, :, at].astype(F32), 0.0)
            own = xbc[m, 0:HALO, at].astype(F32)
            both = jnp.concatenate([lead, own], axis=0)
            total = own * tap[TAPS - 1 : TAPS, at]
            for k in range(1, TAPS):
                weight = tap[TAPS - 1 - k : TAPS - k, at]
                total = total + (pltpu.roll(both, k, 0)[HALO : 2 * HALO] * weight) * same[k]
            total = silu(total).astype(BF16)
            conv[m, 0:HALO, at] = total
            if j < plan.pairs:
                scale = pair_columns(cols[0:HALO], weight_col + m * 16 + 2 * j, lane[0:HALO])
                scaled.append((total.astype(F32) * scale).astype(BF16))
            if j == plan.pairs:
                first_b = total
        edge_state = dot(jnp.concatenate(scaled, axis=1), first_b, ROWS)
        state = (main_state[m] + edge_state).astype(BF16)
        carried_end = docs[m : m + 1, LENGTH - 1 : LENGTH] == doc_before[m : m + 1, 127:128]
        carried_end = jnp.where(carried_end, 1.0, 0.0)
        hi_rows = (gate_parts[m][0] * carried_end).astype(BF16)
        lo_rows = (gate_parts[m][1] * carried_end).astype(BF16)
        for r in range(ring):
            fsend[m, r, 0 : plan.shard] = state[r * plan.shard : (r + 1) * plan.shard]
            at = slice(r * plan.gate_rows, (r + 1) * plan.gate_rows)
            fsend[m, r, plan.shard : plan.packet] = jnp.concatenate(
                [hi_rows[at], lo_rows[at]], axis=0
            )
        copies = exchange(m, fsend, lambda to, m=m: arecv.at[m, rank], a_send, a_recv)
        for copy in copies:
            copy.start()
        a_copies.append(copies)
        arecv[m, pl.ds(rank, 1)] = fsend[m, pl.ds(rank, 1)]

    def scores_of(m):
        t_pos = lax.broadcasted_iota(jnp.int32, (LENGTH, LENGTH), 0)
        s_pos = lax.broadcasted_iota(jnp.int32, (LENGTH, LENGTH), 1)
        doc_t = mark_cols[:, m * TAPS : m * TAPS + 1]
        keep = (s_pos <= t_pos) & (doc_t == docs[m : m + 1])
        full = dot(conv[m, :, ch + DSTATE : ch + 2 * DSTATE], conv[m, :, ch : ch + DSTATE], LANES)
        scores[m] = jnp.where(keep, full, 0.0)

    def inner_of(m):
        low_lane = lane < HEADDIM
        for j in range(plan.pairs):
            at = slice(j * 128, (j + 1) * 128)
            xs = conv[m, :, at]
            xs_a = jnp.where(low_lane, xs, jnp.zeros_like(xs))
            xs_b = jnp.where(low_lane, jnp.zeros_like(xs), xs)
            for half in range(2):
                t0, s1 = half * HALF, (half + 1) * HALF
                base = scores[m, t0 : t0 + HALF, 0:s1]
                mixes = []
                for h in (2 * j, 2 * j + 1):
                    t_log = cols[t0 : t0 + HALF, log_col + m * 16 + h : log_col + m * 16 + h + 1]
                    s_log = log_rows[m][h : h + 1, 0:s1]
                    decay = jnp.exp(jnp.minimum(t_log - s_log, 0.0))
                    mixes.append((base * step_rows[m][h : h + 1, 0:s1] * decay).astype(BF16))
                y[m, t0 : t0 + HALF, at] = dot(
                    jnp.concatenate(mixes, axis=1),
                    jnp.concatenate([xs_a[0:s1], xs_b[0:s1]], axis=0),
                    (((1,), (0,)), ((), ())),
                )

    def gate_both(m):
        carried = mark_cols[:, m * TAPS : m * TAPS + 1] == doc_before[m : m + 1, 127:128]
        for j in range(plan.pairs):
            at = slice(j * 128, (j + 1) * 128)
            opened = zg[m, :, at]
            y[m, :, at] = y[m, :, at] * opened
            entry = pair_columns(cols, entry_col + m * 16 + 2 * j, lane)
            zg[m, :, at] = jnp.where(carried, entry, 0.0) * opened

    def unpack(packet):
        packet = packet.astype(F32)
        split = plan.shard + plan.gate_rows
        return packet[0 : plan.shard], packet[plan.shard : split] + packet[split:]

    def pack(ref, m, total, product):
        ref[m, 0 : plan.shard] = total.astype(BF16)
        hi_rows, lo_rows = split_two(product)
        ref[m, plan.shard : plan.packet] = jnp.concatenate([hi_rows, lo_rows], axis=0)

    def ahead(source, m, slot, k):
        return pltpu.make_async_remote_copy(
            src_ref=source.at[m],
            dst_ref=brecv.at[m, slot],
            send_sem=b_send.at[m, slot],
            recv_sem=b_recv.at[m, slot],
            device_id={"sz": iz + k},
            device_id_type=pl.DeviceIdType.MESH,
        )

    jumps = [(0, 1), (1, 1), (2, 3)]
    b_copies = [
        [ahead(tsend if slot == 0 else usend, m, slot, k) for slot, k in jumps] for m in range(BATCH)
    ]

    def goes(k):
        return iz + k < plan.planes

    def plane_total(m):
        for copy in a_copies[m]:
            copy.wait_recv()
        total = jnp.zeros((plan.shard, DSTATE), F32)
        product = jnp.ones((plan.gate_rows, DSTATE), F32)
        for d in range(ring):
            pref[m, d] = total
            qpref[m, d] = product
            fresh, gates = unpack(arecv[m, d])
            total = spread(gates, plan) * total + fresh
            product = product * gates
        pack(tsend, m, total, product)
        ptot[m] = total
        qtot[m] = product
        pl.when(has_above)(b_copies[m][0].start)

    def two_planes(m):
        pl.when(has_below)(b_copies[m][0].wait_recv)
        lower, gates = unpack(brecv[m, 0])
        lower = jnp.where(has_below, lower, 0.0)
        gates = jnp.where(has_below, gates, 0.0)
        product = qtot[m]
        pack(usend, m, spread(product, plan) * lower + ptot[m], product * gates)
        pl.when(has_above)(b_copies[m][1].start)
        pl.when(goes(3))(b_copies[m][2].start)

    gate_inputs(0)
    scores_of(0)
    pl.when(goes(2))(lambda: pl.semaphore_wait(word.at[0], 1))
    pl.when(has_below & goes(2))(lambda: tell_below(1))
    inner_of(0)
    gate_both(0)
    plane_total(0)
    plane_total(1)
    scores_of(1)
    inner_of(1)
    pl.when(goes(3))(lambda: pl.semaphore_wait(word.at[1], 1))
    two_planes(0)
    two_planes(1)
    gate_inputs(1)
    gate_both(1)
    turn_weights()
    c_copies = []
    for m in range(BATCH):
        pl.when(has_below)(b_copies[m][1].wait_recv)
        pl.when(iz >= 3)(b_copies[m][2].wait_recv)
        near, gates = unpack(brecv[m, 1])
        remote, _ = unpack(brecv[m, 2])
        incoming = spread(gates, plan) * jnp.where(iz >= 3, remote, 0.0) + near
        incoming = jnp.where(has_below, incoming, 0.0)
        for d in range(ring):
            entering = pref[m, d] + spread(qpref[m, d], plan) * incoming
            hsend[m, d] = entering.astype(BF16)
        home = pl.ds(pl.multiple_of(rank * plan.shard, 16), plan.shard)
        copies = exchange(m, hsend, lambda to, m=m: hstate.at[m, home], c_send, c_recv)
        for copy in copies:
            copy.start()
        c_copies.append(copies)
        hstate[m, home] = hsend[m, rank]

    quarter = plan.out // QUARTERS

    def hops(q, upward):
        return plan.far if (q < QUARTERS // 2) == upward else plan.far - 1

    def owner_at(distance, upward):
        return lax.rem(me + distance if upward else me + members - distance, members)

    def arrow(m, q, hop, upward):
        buffer, send, got, to = (
            (up_recv, up_send, up_got, up) if upward else (dn_recv, dn_send, dn_got, down)
        )
        rows = pl.ds(q * quarter, quarter)
        return pltpu.make_async_remote_copy(
            src_ref=part.at[m, owner_at(hops(q, upward) - hop, upward), rows],
            dst_ref=buffer.at[m, hop, rows],
            send_sem=send.at[m, q, hop],
            recv_sem=got.at[m, q, hop],
            device_id=to,
            device_id_type=pl.DeviceIdType.MESH,
        )

    arrows = {}
    square_copies = {}
    need(got_gain)
    gain = gain_ref[...].reshape(1, ch)

    def project(m, distance, upward):
        owner = owner_at(distance, upward)
        rows = pl.ds(pl.multiple_of(owner * plan.out, 16), plan.out)
        part[m, owner] = dot(wt[rows, :], gated[m], LANES).astype(BF16)

    def shoot(m, hop, upward, pieces):
        for q in pieces:
            if hop < hops(q, upward):
                if hop > 0:
                    arrows[m, q, hop - 1, upward].wait_recv()
                    buffer = up_recv if upward else dn_recv
                    owner = owner_at(hops(q, upward) - hop, upward)
                    rows = slice(q * quarter, (q + 1) * quarter)
                    total = part[m, owner, rows].astype(F32) + buffer[m, hop - 1, rows].astype(F32)
                    part[m, owner, rows] = total.astype(BF16)
                arrows[m, q, hop, upward] = arrow(m, q, hop, upward)
                arrows[m, q, hop, upward].start()

    early, late = range(QUARTERS // 2), range(QUARTERS // 2, QUARTERS)

    def first_round(m):
        project(m, plan.far, True)
        shoot(m, 0, True, early)
        shoot(m, 0, False, late)
        if plan.far > 1:
            project(m, plan.far - 1, True)
            shoot(m, 0, True, late)
            project(m, plan.far - 1, False)
            shoot(m, 0, False, early)

    def pass_squares(m, hop):
        for side, upward in enumerate((True, False)):
            if hop < (plan.far if upward else plan.far - 1):
                if hop > 0:
                    square_copies[m, hop - 1, upward].wait_recv()
                copy = pltpu.make_async_remote_copy(
                    src_ref=ssend.at[m] if hop == 0 else srecv.at[m, side, hop - 1],
                    dst_ref=srecv.at[m, side, hop],
                    send_sem=s_send.at[m, side, hop],
                    recv_sem=s_recv.at[m, side, hop],
                    device_id=up if upward else down,
                    device_id_type=pl.DeviceIdType.MESH,
                )
                copy.start()
                square_copies[m, hop, upward] = copy

    def next_round(m, hop):
        if hop + 1 < plan.far:
            project(m, plan.far - 1 - hop, True)
            project(m, plan.far - 1 - hop, False)
        shoot(m, hop, True, early)
        shoot(m, hop, False, late)
        shoot(m, hop, True, late)
        shoot(m, hop, False, early)
        pass_squares(m, hop)

    def carry(m):
        for copy in c_copies[m]:
            copy.wait_recv()
        squares = jnp.zeros((LENGTH, 128), F32)
        outer = dot(conv[m, :, ch + DSTATE : ch + 2 * DSTATE], hstate[m], LANES)
        for j in range(plan.pairs):
            at = slice(j * 128, (j + 1) * 128)
            mixed = y[m, :, at] + zg[m, :, at] * outer[:, at]
            squares = squares + mixed * mixed
            gated[m, :, at] = (mixed * gain[:, at]).astype(BF16)
        first_round(m)
        square_hi, square_lo = split_two(squares)
        ones = jnp.ones((8, 128), BF16)
        square_rows = dot(ones, square_hi, LANES) + dot(ones, square_lo, LANES)
        ssend[m] = square_rows[0:1]
        pass_squares(m, 0)

    carry(0)
    carry(1)
    for hop in range(1, plan.far):
        for m in range(BATCH):
            next_round(m, hop)
    for m in range(BATCH):
        project(m, 0, True)

    for m in range(BATCH):
        square = ssend[m]
        for side, upward in enumerate((True, False)):
            last = (plan.far if upward else plan.far - 1) - 1
            if last >= 0:
                square_copies[m, last, upward].wait_recv()
            for hop in range(last + 1):
                square = square + srecv[m, side, hop]
        scale = lax.rsqrt(square / INNER + EPSILON)
        for q in (*late, *early):
            rows = slice(q * quarter, (q + 1) * quarter)
            total = part[m, me, rows].astype(F32)
            for upward in (True, False):
                last = hops(q, upward) - 1
                if last >= 0:
                    arrows[m, q, last, upward].wait_recv()
                    buffer = up_recv if upward else dn_recv
                    total = total + buffer[m, last, rows].astype(F32)
            out_ref[m, rows, :] = (total * scale).astype(BF16)

    def sent():
        for copy in halos:
            copy.wait_send()

    pl.when(has_next)(sent)
    for group in (*a_copies, *c_copies, list(square_copies.values()), list(arrows.values())):
        for copy in group:
            copy.wait_send()
    for m in range(BATCH):
        for slot, k in jumps:
            pl.when(goes(k))(b_copies[m][slot].wait_send)


def shards(
    plan,
    x_inner,
    z_gate,
    b_input,
    c_input,
    dt_raw,
    doc_ids,
    conv_x,
    conv_b,
    conv_c,
    dt_bias,
    decay_rate,
    norm_gain,
    w_out,
):
    hbm = pl.BlockSpec(memory_space=pltpu.HBM)
    vmem = pl.BlockSpec(memory_space=pltpu.VMEM)
    ch, ring, members = plan.channels, plan.ring, plan.members
    dma = pltpu.SemaphoreType.DMA
    scratch = [
        pltpu.SMEM((plan.heads,), F32),
        pltpu.SMEM((plan.heads,), F32),
        pltpu.VMEM((ch,), F32),
        pltpu.VMEM((BATCH, LENGTH, plan.conv), BF16),
        pltpu.VMEM((BATCH, HALO, plan.conv), BF16),
        pltpu.VMEM((BATCH, LENGTH), jnp.int32),
        pltpu.VMEM((BATCH, 128), jnp.int32),
        pltpu.VMEM((plan.heads, BATCH, LENGTH), F32),
        pltpu.VMEM((TAPS, plan.conv), BF16),
        pltpu.VMEM((BATCH, LENGTH, ch), BF16),
        pltpu.VMEM((ch, plan.width), BF16),
        pltpu.VMEM((plan.width, ch), BF16),
        pltpu.VMEM((BATCH, LENGTH, plan.conv), BF16),
        pltpu.VMEM((BATCH, TAPS - 1, LENGTH, 128), F32),
        pltpu.VMEM((BATCH, ch, DSTATE), F32),
        pltpu.VMEM((BATCH, LENGTH, ch), BF16),
        pltpu.VMEM((BATCH, LENGTH, ch), F32),
        pltpu.VMEM((BATCH, LENGTH, LENGTH), F32),
        pltpu.VMEM((BATCH, LENGTH, ch), F32),
        pltpu.VMEM((BATCH, LENGTH, ch), BF16),
        pltpu.VMEM((BATCH, ring, plan.packet, DSTATE), BF16),
        pltpu.VMEM((BATCH, ring, plan.packet, DSTATE), BF16),
        pltpu.VMEM((BATCH, ring, plan.shard, DSTATE), F32),
        pltpu.VMEM((BATCH, ring, plan.gate_rows, DSTATE), F32),
        pltpu.VMEM((BATCH, plan.packet, DSTATE), BF16),
        pltpu.VMEM((BATCH, plan.packet, DSTATE), BF16),
        pltpu.VMEM((BATCH, plan.shard, DSTATE), F32),
        pltpu.VMEM((BATCH, plan.gate_rows, DSTATE), F32),
        pltpu.VMEM((BATCH, 3, plan.packet, DSTATE), BF16),
        pltpu.VMEM((BATCH, ring, plan.shard, DSTATE), BF16),
        pltpu.VMEM((BATCH, ch, DSTATE), BF16),
        pltpu.VMEM((BATCH, members, plan.out, LENGTH), BF16),
        pltpu.VMEM((BATCH, plan.far, plan.out, LENGTH), BF16),
        pltpu.VMEM((BATCH, plan.far, plan.out, LENGTH), BF16),
        pltpu.VMEM((BATCH, 1, LENGTH), F32),
        pltpu.VMEM((BATCH, 2, plan.far, 1, LENGTH), F32),
        dma((16,)),
        dma((BATCH + 1,)),
        dma((BATCH + 1,)),
        dma((BATCH, ring)),
        dma((BATCH, ring)),
        dma((BATCH, 3)),
        dma((BATCH, 3)),
        dma((BATCH, ring)),
        dma((BATCH, ring)),
        dma((BATCH, 2, plan.far)),
        dma((BATCH, 2, plan.far)),
        dma((BATCH, QUARTERS, plan.far)),
        dma((BATCH, QUARTERS, plan.far)),
        dma((BATCH, QUARTERS, plan.far)),
        dma((BATCH, QUARTERS, plan.far)),
        pltpu.SemaphoreType.REGULAR((2,)),
    ]
    out = pl.pallas_call(
        functools.partial(layer_kernel, plan),
        name="mixer_layer",
        out_shape=pltpu.VMEM((BATCH, plan.out, LENGTH), BF16),
        in_specs=[hbm] * 13,
        out_specs=vmem,
        scratch_shapes=scratch,
        compiler_params=pltpu.CompilerParams(
            collective_id=0, has_side_effects=True, vmem_limit_bytes=60 * 1024 * 1024
        ),
    )(
        x_inner,
        z_gate,
        b_input,
        c_input,
        jnp.transpose(dt_raw, (2, 0, 1)),
        doc_ids,
        conv_x,
        conv_b,
        conv_c,
        dt_bias,
        decay_rate,
        norm_gain,
        w_out,
    )
    return jnp.transpose(out, (0, 2, 1))


def solution(mesh):
    members = mesh.shape["mp"]
    line = Mesh(mesh.devices.reshape(*SPLIT, members), (*SEQ, "mp"))

    def layer(*arrays):
        channels = arrays[0].shape[2] // members
        plan = Plan(SPLIT, members, channels, arrays[12].shape[1])
        placed = (
            P(None, SEQ, "mp"),
            P(None, SEQ, "mp"),
            P(None, SEQ, None),
            P(None, SEQ, None),
            P(None, SEQ, "mp"),
            P(None, SEQ),
            P(None, "mp"),
            P(),
            P(),
            P("mp"),
            P("mp"),
            P("mp"),
            P("mp", None),
        )
        return jax.shard_map(
            functools.partial(shards, plan),
            mesh=line,
            in_specs=placed,
            out_specs=P(None, SEQ, "mp"),
            check_vma=False,
        )(*arrays)

    return layer
```

```python
import functools

import jax
import jax.numpy as jnp
from jax import lax
from jax.experimental import pallas as pl
from jax.experimental.pallas import tpu as pltpu
from jax.sharding import Mesh
from jax.sharding import PartitionSpec as P

SPLIT = (8, 4, 2)
SEQ = ("sz", "sx", "sc")
INNER = 5120
EPSILON = 1e-05
BATCH = 2
LENGTH = 256
HALF = 128
QUARTERS = 2
HALO = 8
TAPS = 4
HEADDIM = 64
DSTATE = 128
REACH = 8192 // LENGTH
F32 = jnp.float32
BF16 = jnp.bfloat16
LANES = (((1,), (1,)), ((), ()))
ROWS = (((0,), (0,)), ((), ()))


def dot(a, b, dims):
    return lax.dot_general(a, b, dims, preferred_element_type=F32)


def split_two(value):
    high = value.astype(BF16)
    return high, (value - high.astype(F32)).astype(BF16)


def silu(value):
    return value / (1.0 + jnp.exp(-value))


class Plan:
    def __init__(self, split, members, channels, width):
        self.planes, self.xs, self.cores = split
        self.ring = self.xs * self.cores
        self.members = members
        self.channels = channels
        self.heads = channels // HEADDIM
        self.pairs = self.heads // 2
        self.conv = channels + 2 * DSTATE
        self.shard = channels // self.ring
        self.groups = self.shard // 16
        self.gate_rows = max(8, 1 << (self.groups - 1).bit_length())
        self.packet = self.shard + 2 * self.gate_rows
        assert REACH <= 4 * self.ring or self.planes <= 5
        self.width = width
        self.out = width // members
        self.far = members // 2


def spread(rows, plan):
    return jnp.concatenate(
        [jnp.broadcast_to(rows[q : q + 1], (16, DSTATE)) for q in range(plan.groups)], axis=0
    )


def pair_columns(cols, first, lane):
    a = jnp.broadcast_to(cols[:, first : first + 1], (cols.shape[0], 128))
    b = jnp.broadcast_to(cols[:, first + 1 : first + 2], (cols.shape[0], 128))
    return jnp.where(lane < HEADDIM, a, b)


def layer_kernel(
    plan,
    x_hbm,
    z_hbm,
    b_hbm,
    c_hbm,
    dt_hbm,
    doc_hbm,
    cx_hbm,
    cb_hbm,
    cc_hbm,
    bias_hbm,
    rate_hbm,
    gain_hbm,
    w_hbm,
    out_ref,
    bias_ref,
    rate_ref,
    gain_ref,
    xbc,
    halo,
    docs_ref,
    doc_halo,
    dt_ref,
    taps,
    z_ref,
    w_ref,
    wt,
    conv,
    masks,
    main_state,
    xw,
    y,
    scores,
    zg,
    gated,
    fsend,
    arecv,
    pref,
    qpref,
    tsend,
    usend,
    ptot,
    qtot,
    brecv,
    hsend,
    hstate,
    part,
    up_recv,
    dn_recv,
    ssend,
    srecv,
    load_sem,
    halo_send,
    halo_recv,
    a_send,
    a_recv,
    b_send,
    b_recv,
    c_send,
    c_recv,
    s_send,
    s_recv,
    ring_send,
    up_got,
    dn_got,
    word,
):
    ch, nh, ring, members = plan.channels, plan.heads, plan.ring, plan.members
    iz, ix, ic = lax.axis_index("sz"), lax.axis_index("sx"), lax.axis_index("sc")
    me = lax.axis_index("mp")
    rank = ix * plan.cores + ic
    place = iz * ring + rank
    blocks = plan.planes * ring

    def in_plane(r):
        return {"sx": r // plan.cores, "sc": r % plan.cores}

    def in_line(j):
        return {"sz": j // ring, "sx": (j % ring) // plan.cores, "sc": j % plan.cores}

    after, prior = in_line(place + 1), in_line(place - 1)
    up = {"mp": lax.rem(me + 1, members)}
    down = {"mp": lax.rem(me + members - 1, members)}

    has_next, has_prior = place + 1 < blocks, place > 0

    def one(flag):
        return jnp.where(flag, 1, 0)

    barrier = pltpu.get_barrier_semaphore()

    def greet(peer):
        pl.semaphore_signal(barrier, inc=1, device_id=peer, device_id_type=pl.DeviceIdType.MESH)

    for k in range(1, ring):
        greet(in_plane(lax.rem(rank + k, ring)))
    greet(up)
    greet(down)
    pl.when(has_prior)(lambda: greet(prior))
    count = ring - 1 + 2 + one(has_next)
    above, below = {"sz": iz + 1}, {"sz": iz - 1}
    has_above, has_below = iz + 1 < plan.planes, iz > 0
    pl.when(has_below)(lambda: greet(below))
    pl.when(has_above)(lambda: greet(above))
    count = count + one(has_above) + one(has_below)

    def tell_below(at):
        pl.semaphore_signal(
            word.at[at], inc=1, device_id=below, device_id_type=pl.DeviceIdType.MESH
        )

    loads = []

    def load(src, dst, sem=None):
        copy = pltpu.make_async_copy(src, dst, load_sem.at[len(loads) if sem is None else sem])
        copy.start()
        if sem is None:
            loads.append(copy)
        return copy

    def load_group(copies, whole):
        sem = len(loads)
        for src, dst in copies:
            load(src, dst, sem)
        loads.append(pltpu.make_async_copy(whole, whole, load_sem.at[sem]))
        return loads[-1]

    done = []

    def need(copy):
        if not any(copy is other for other in done):
            copy.wait()
            done.append(copy)

    def got_waits():
        for copy in loads:
            need(copy)

    got_docs = load(doc_hbm, docs_ref)
    row_parts = []
    for m in range(BATCH):
        row_parts += [
            (x_hbm.at[m], xbc.at[m, :, pl.ds(0, ch)]),
            (b_hbm.at[m], xbc.at[m, :, pl.ds(ch, DSTATE)]),
            (c_hbm.at[m], xbc.at[m, :, pl.ds(ch + DSTATE, DSTATE)]),
        ]
    got_rows = load_group(row_parts, xbc)
    got_dt = [load(dt_hbm, dt_ref), load(bias_hbm, bias_ref), load(rate_hbm, rate_ref)]
    got_taps = load_group(
        [
            (cx_hbm, taps.at[:, pl.ds(0, ch)]),
            (cb_hbm, taps.at[:, pl.ds(ch, DSTATE)]),
            (cc_hbm, taps.at[:, pl.ds(ch + DSTATE, DSTATE)]),
        ],
        taps,
    )
    got_gain = load(gain_hbm, gain_ref)

    need(got_docs)
    need(got_rows)
    got_z = load(z_hbm, z_ref)
    got_w = load(w_hbm, w_ref)
    pl.semaphore_wait(barrier, count)
    pl.when(has_below & has_above)(lambda: tell_below(0))

    halos = []
    for m in range(BATCH):
        halos.append(
            pltpu.make_async_remote_copy(
                src_ref=xbc.at[m, pl.ds(LENGTH - HALO, HALO)],
                dst_ref=halo.at[m],
                send_sem=halo_send.at[m],
                recv_sem=halo_recv.at[m],
                device_id=after,
                device_id_type=pl.DeviceIdType.MESH,
            )
        )
    halos.append(
        pltpu.make_async_remote_copy(
            src_ref=docs_ref.at[:, pl.ds(LENGTH - 128, 128)],
            dst_ref=doc_halo,
            send_sem=halo_send.at[BATCH],
            recv_sem=halo_recv.at[BATCH],
            device_id=after,
            device_id_type=pl.DeviceIdType.MESH,
        )
    )
    def send_halo():
        for copy in (halos[BATCH], *halos[:BATCH]):
            copy.start()

    pl.when(has_next)(send_halo)

    lane = lax.broadcasted_iota(jnp.int32, (LENGTH, 128), 1)

    docs = docs_ref[...].astype(F32)
    marks = []
    for m in range(BATCH):
        own = docs[m : m + 1]
        marks.append(own)
        for k in range(1, TAPS):
            marks.append(jnp.where(pltpu.roll(own, k, 1) == own, 1.0, 0.0))
    mark_cols = jnp.concatenate(marks, axis=0).T
    for m in range(BATCH):
        for k in range(1, TAPS):
            at = m * TAPS + k
            masks[m, k - 1] = jnp.broadcast_to(mark_cols[:, at : at + 1], (LENGTH, 128))
    for copy in got_dt:
        need(copy)
    head_row = lax.broadcasted_iota(jnp.int32, (16, LENGTH), 0)
    bias = jnp.zeros((16, LENGTH), F32)
    rate = jnp.zeros((16, LENGTH), F32)
    for h in range(nh):
        bias = jnp.where(head_row == h, bias_ref[h], bias)
        rate = jnp.where(head_row == h, rate_ref[h], rate)
    step_rows, log_parts = [], []
    for m in range(BATCH):
        raw = dt_ref[:, m, :]
        if nh < 16:
            raw = jnp.concatenate([raw, jnp.zeros((16 - nh, LENGTH), F32)], axis=0)
        shifted = raw + bias
        step = jnp.maximum(shifted, 0.0) + jnp.log1p(jnp.exp(-jnp.abs(shifted)))
        step_rows.append(step)
        log_parts.append(-(step * rate))
    log_step = jnp.concatenate(log_parts, axis=0)
    hi = log_step.astype(BF16)
    rest = log_step - hi.astype(F32)
    mid = rest.astype(BF16)
    low = (rest - mid.astype(F32)).astype(BF16)
    before = lax.broadcasted_iota(jnp.int32, (LENGTH, LENGTH), 0) <= lax.broadcasted_iota(
        jnp.int32, (LENGTH, LENGTH), 1
    )
    upper = jnp.where(before, 1.0, 0.0).astype(BF16)
    sums = dot(jnp.concatenate([low, mid, hi], axis=0), upper, (((1,), (0,)), ((), ())))
    span = BATCH * 16
    log_cum = sums[0:span] + sums[span : 2 * span] + sums[2 * span : 3 * span]
    log_rows = [log_cum[m * 16 : (m + 1) * 16] for m in range(BATCH)]
    row_mats = list(log_rows)
    ends = []
    for m in range(BATCH):
        end = log_rows[m][:, LENGTH - 1 : LENGTH]
        ends.append(end)
        keep = jnp.where(docs[m : m + 1] == docs[m : m + 1, LENGTH - 1 : LENGTH], 1.0, 0.0)
        row_mats.append(jnp.exp(jnp.minimum(end - log_rows[m], 0.0)) * step_rows[m] * keep)
    for m in range(BATCH):
        row_mats.append(jnp.exp(log_rows[m]))
    row_mats.append(jnp.zeros((128 - 3 * span, LENGTH), F32))
    cols = jnp.concatenate(row_mats, axis=0).T
    log_col, weight_col, entry_col = 0, span, 2 * span

    need(got_taps)
    tap = taps[...].astype(F32)
    tiles = plan.conv // 128
    def convolve(m):
        for j in range(tiles):
            at = slice(j * 128, (j + 1) * 128)
            rows = xbc[m, :, at].astype(F32)
            total = rows * tap[TAPS - 1 : TAPS, at]
            for k in range(1, TAPS):
                weight = tap[TAPS - 1 - k : TAPS - k, at]
                total = total + (pltpu.roll(rows, k, 0) * weight) * masks[m, k - 1]
            total = silu(total)
            conv[m, :, at] = total.astype(BF16)
            if j < plan.pairs:
                scale = pair_columns(cols, weight_col + m * 16 + 2 * j, lane)
                xw[m, :, at] = (total.astype(BF16).astype(F32) * scale).astype(BF16)
        xw[m, 0:HALO, :] = jnp.zeros((HALO, ch), BF16)
        main_state[m] = dot(xw[m], conv[m, :, ch : ch + DSTATE], ROWS)

    def turn_weights():
        need(got_w)
        for j in range(plan.width // 128):
            wt[j * 128 : (j + 1) * 128, :] = w_ref[:, j * 128 : (j + 1) * 128].T

    def gate_inputs(m):
        need(got_z)
        for j in range(plan.pairs):
            at = slice(j * 128, (j + 1) * 128)
            zg[m, :, at] = silu(z_ref[m, :, at].astype(F32))

    group_row = lax.broadcasted_iota(jnp.int32, (ring * plan.gate_rows, 16), 0)
    group_head = lax.broadcasted_iota(jnp.int32, (ring * plan.gate_rows, 16), 1)
    bits = plan.gate_rows.bit_length() - 1
    shard_of, group_of = group_row >> bits, group_row & (plan.gate_rows - 1)
    picks = (((shard_of * plan.groups + group_of) >> 2) == group_head) & (group_of < plan.groups)
    pick = jnp.where(picks, 1.0, 0.0).astype(BF16)
    plain = (((1,), (0,)), ((), ()))
    gate_parts = []
    for m in range(BATCH):
        gate_hi, gate_lo = split_two(jnp.broadcast_to(jnp.exp(ends[m]), (16, DSTATE)))
        gate_parts.append((dot(pick, gate_hi, plain), dot(pick, gate_lo, plain)))
    convolve(0)
    pl.when(has_prior)(halos[BATCH].wait_recv)
    doc_before = jnp.where(has_prior, doc_halo[...].astype(F32), -1.0)
    row8 = lax.broadcasted_iota(jnp.int32, (HALO, 128), 0)

    def edge_mask(m, k):
        mask = masks[m, k - 1, 0:HALO]
        for t in range(k):
            at = 128 - k + t
            same = docs[m : m + 1, t : t + 1] == doc_before[m : m + 1, at : at + 1]
            mask = jnp.where(row8 == t, jnp.where(same, 1.0, 0.0), mask)
        return mask

    def exchange(m, source, target, peers_send, peers_recv):
        copies = []
        for k in range(1, ring):
            to = lax.rem(rank + k, ring)
            copies.append(
                pltpu.make_async_remote_copy(
                    src_ref=source.at[m, to],
                    dst_ref=target(to),
                    send_sem=peers_send.at[m],
                    recv_sem=peers_recv.at[m],
                    device_id=in_plane(to),
                    device_id_type=pl.DeviceIdType.MESH,
                )
            )
        return copies

    def all_of(m, ref, send_sem, recv_sem):
        return pltpu.make_async_remote_copy(
            src_ref=ref.at[m, pl.ds(0, ring - 1)],
            dst_ref=ref.at[m, pl.ds(0, ring - 1)],
            send_sem=send_sem.at[m],
            recv_sem=recv_sem.at[m],
            device_id=in_plane(lax.rem(rank + 1, ring)),
            device_id_type=pl.DeviceIdType.MESH,
        )

    a_copies = []
    for m in range(BATCH):
        if m > 0:
            convolve(m)
        pl.when(has_prior)(halos[m].wait_recv)
        same = [None, *(edge_mask(m, k) for k in range(1, TAPS))]
        scaled = []
        for j in range(tiles):
            at = slice(j * 128, (j + 1) * 128)
            lead = jnp.where(has_prior, halo[m, :, at].astype(F32), 0.0)
            own = xbc[m, 0:HALO, at].astype(F32)
            both = jnp.concatenate([lead, own], axis=0)
            total = own * tap[TAPS - 1 : TAPS, at]
            for k in range(1, TAPS):
                weight = tap[TAPS - 1 - k : TAPS - k, at]
                total = total + (pltpu.roll(both, k, 0)[HALO : 2 * HALO] * weight) * same[k]
            total = silu(total).astype(BF16)
            conv[m, 0:HALO, at] = total
            if j < plan.pairs:
                scale = pair_columns(cols[0:HALO], weight_col + m * 16 + 2 * j, lane[0:HALO])
                scaled.append((total.astype(F32) * scale).astype(BF16))
            if j == plan.pairs:
                first_b = total
        edge_state = dot(jnp.concatenate(scaled, axis=1), first_b, ROWS)
        state = (main_state[m] + edge_state).astype(BF16)
        carried_end = docs[m : m + 1, LENGTH - 1 : LENGTH] == doc_before[m : m + 1, 127:128]
        carried_end = jnp.where(carried_end, 1.0, 0.0)
        hi_rows = (gate_parts[m][0] * carried_end).astype(BF16)
        lo_rows = (gate_parts[m][1] * carried_end).astype(BF16)
        for r in range(ring):
            fsend[m, r, 0 : plan.shard] = state[r * plan.shard : (r + 1) * plan.shard]
            at = slice(r * plan.gate_rows, (r + 1) * plan.gate_rows)
            fsend[m, r, plan.shard : plan.packet] = jnp.concatenate(
                [hi_rows[at], lo_rows[at]], axis=0
            )
        copies = exchange(m, fsend, lambda to, m=m: arecv.at[m, rank], a_send, a_recv)
        for copy in copies:
            copy.start()
        a_copies.append([all_of(m, arecv, a_send, a_recv)])
        arecv[m, pl.ds(rank, 1)] = fsend[m, pl.ds(rank, 1)]

    def scores_of(m):
        t_pos = lax.broadcasted_iota(jnp.int32, (LENGTH, LENGTH), 0)
        s_pos = lax.broadcasted_iota(jnp.int32, (LENGTH, LENGTH), 1)
        doc_t = mark_cols[:, m * TAPS : m * TAPS + 1]
        keep = (s_pos <= t_pos) & (doc_t == docs[m : m + 1])
        full = dot(conv[m, :, ch + DSTATE : ch + 2 * DSTATE], conv[m, :, ch : ch + DSTATE], LANES)
        scores[m] = jnp.where(keep, full, 0.0)

    def inner_of(m):
        low_lane = lane < HEADDIM
        for j in range(plan.pairs):
            at = slice(j * 128, (j + 1) * 128)
            xs = conv[m, :, at]
            xs_a = jnp.where(low_lane, xs, jnp.zeros_like(xs))
            xs_b = jnp.where(low_lane, jnp.zeros_like(xs), xs)
            for half in range(2):
                t0, s1 = half * HALF, (half + 1) * HALF
                base = scores[m, t0 : t0 + HALF, 0:s1]
                mixes = []
                for h in (2 * j, 2 * j + 1):
                    t_log = cols[t0 : t0 + HALF, log_col + m * 16 + h : log_col + m * 16 + h + 1]
                    s_log = log_rows[m][h : h + 1, 0:s1]
                    decay = jnp.exp(jnp.minimum(t_log - s_log, 0.0))
                    mixes.append((base * step_rows[m][h : h + 1, 0:s1] * decay).astype(BF16))
                y[m, t0 : t0 + HALF, at] = dot(
                    jnp.concatenate(mixes, axis=1),
                    jnp.concatenate([xs_a[0:s1], xs_b[0:s1]], axis=0),
                    (((1,), (0,)), ((), ())),
                )

    def gate_both(m):
        carried = mark_cols[:, m * TAPS : m * TAPS + 1] == doc_before[m : m + 1, 127:128]
        for j in range(plan.pairs):
            at = slice(j * 128, (j + 1) * 128)
            opened = zg[m, :, at]
            y[m, :, at] = y[m, :, at] * opened
            entry = pair_columns(cols, entry_col + m * 16 + 2 * j, lane)
            zg[m, :, at] = jnp.where(carried, entry, 0.0) * opened

    def unpack(packet):
        packet = packet.astype(F32)
        split = plan.shard + plan.gate_rows
        return packet[0 : plan.shard], packet[plan.shard : split] + packet[split:]

    def pack(ref, m, total, product):
        ref[m, 0 : plan.shard] = total.astype(BF16)
        hi_rows, lo_rows = split_two(product)
        ref[m, plan.shard : plan.packet] = jnp.concatenate([hi_rows, lo_rows], axis=0)

    def ahead(source, m, slot, k):
        return pltpu.make_async_remote_copy(
            src_ref=source.at[m],
            dst_ref=brecv.at[m, slot],
            send_sem=b_send.at[m, slot],
            recv_sem=b_recv.at[m, slot],
            device_id={"sz": iz + k},
            device_id_type=pl.DeviceIdType.MESH,
        )

    jumps = [(0, 1), (1, 1), (2, 3)]
    b_copies = [
        [ahead(tsend if slot == 0 else usend, m, slot, k) for slot, k in jumps] for m in range(BATCH)
    ]

    def goes(k):
        return iz + k < plan.planes

    def plane_total(m):
        for copy in a_copies[m]:
            copy.wait_recv()
        total = jnp.zeros((plan.shard, DSTATE), F32)
        product = jnp.ones((plan.gate_rows, DSTATE), F32)
        for d in range(ring):
            pref[m, d] = total
            qpref[m, d] = product
            fresh, gates = unpack(arecv[m, d])
            total = spread(gates, plan) * total + fresh
            product = product * gates
        pack(tsend, m, total, product)
        ptot[m] = total
        qtot[m] = product
        pl.when(has_above)(b_copies[m][0].start)

    def two_planes(m):
        pl.when(has_below)(b_copies[m][0].wait_recv)
        lower, gates = unpack(brecv[m, 0])
        lower = jnp.where(has_below, lower, 0.0)
        gates = jnp.where(has_below, gates, 0.0)
        product = qtot[m]
        pack(usend, m, spread(product, plan) * lower + ptot[m], product * gates)
        pl.when(has_above)(b_copies[m][1].start)
        pl.when(goes(3))(b_copies[m][2].start)

    gate_inputs(0)
    scores_of(0)
    pl.when(goes(2))(lambda: pl.semaphore_wait(word.at[0], 1))
    pl.when(has_below & goes(2))(lambda: tell_below(1))
    inner_of(0)
    gate_both(0)
    plane_total(0)
    plane_total(1)
    scores_of(1)
    inner_of(1)
    pl.when(goes(3))(lambda: pl.semaphore_wait(word.at[1], 1))
    two_planes(0)
    two_planes(1)
    gate_inputs(1)
    gate_both(1)
    turn_weights()
    c_copies = []
    for m in range(BATCH):
        pl.when(has_below)(b_copies[m][1].wait_recv)
        pl.when(iz >= 3)(b_copies[m][2].wait_recv)
        near, gates = unpack(brecv[m, 1])
        remote, _ = unpack(brecv[m, 2])
        incoming = spread(gates, plan) * jnp.where(iz >= 3, remote, 0.0) + near
        incoming = jnp.where(has_below, incoming, 0.0)
        for d in range(ring):
            entering = pref[m, d] + spread(qpref[m, d], plan) * incoming
            hsend[m, d] = entering.astype(BF16)
        home = pl.ds(pl.multiple_of(rank * plan.shard, 16), plan.shard)
        copies = exchange(m, hsend, lambda to, m=m: hstate.at[m, home], c_send, c_recv)
        for copy in copies:
            copy.start()
        c_copies.append([all_of(m, hsend, c_send, c_recv)])
        hstate[m, home] = hsend[m, rank]

    quarter = plan.out // QUARTERS

    def hops(q, upward):
        return plan.far if (q < QUARTERS // 2) == upward else plan.far - 1

    def owner_at(distance, upward):
        return lax.rem(me + distance if upward else me + members - distance, members)

    def arrow(m, q, hop, upward):
        buffer, send, got, to = (
            (up_recv, ring_send.at[0], up_got, up)
            if upward
            else (dn_recv, ring_send.at[1], dn_got, down)
        )
        rows = pl.ds(q * quarter, quarter)
        return pltpu.make_async_remote_copy(
            src_ref=part.at[m, owner_at(hops(q, upward) - hop, upward), rows],
            dst_ref=buffer.at[m, hop, rows],
            send_sem=send,
            recv_sem=got.at[m, q, hop],
            device_id=to,
            device_id_type=pl.DeviceIdType.MESH,
        )

    arrows = {}
    square_copies = {}
    need(got_gain)
    gain = gain_ref[...].reshape(1, ch)

    def project(m, distance, upward):
        owner = owner_at(distance, upward)
        rows = pl.ds(pl.multiple_of(owner * plan.out, 16), plan.out)
        part[m, owner] = dot(wt[rows, :], gated[m], LANES).astype(BF16)

    def shoot(m, hop, upward, pieces):
        for q in pieces:
            if hop < hops(q, upward):
                if hop > 0:
                    arrows[m, q, hop - 1, upward].wait_recv()
                    buffer = up_recv if upward else dn_recv
                    owner = owner_at(hops(q, upward) - hop, upward)
                    rows = slice(q * quarter, (q + 1) * quarter)
                    total = part[m, owner, rows].astype(F32) + buffer[m, hop - 1, rows].astype(F32)
                    part[m, owner, rows] = total.astype(BF16)
                arrows[m, q, hop, upward] = arrow(m, q, hop, upward)
                arrows[m, q, hop, upward].start()

    early, late = range(QUARTERS // 2), range(QUARTERS // 2, QUARTERS)

    def first_round(m):
        project(m, plan.far, True)
        shoot(m, 0, True, early)
        shoot(m, 0, False, late)
        if plan.far > 1:
            project(m, plan.far - 1, True)
            shoot(m, 0, True, late)
            project(m, plan.far - 1, False)
            shoot(m, 0, False, early)

    def pass_squares(m, hop):
        for side, upward in enumerate((True, False)):
            if hop < (plan.far if upward else plan.far - 1):
                if hop > 0:
                    square_copies[m, hop - 1, upward].wait_recv()
                copy = pltpu.make_async_remote_copy(
                    src_ref=ssend.at[m] if hop == 0 else srecv.at[m, side, hop - 1],
                    dst_ref=srecv.at[m, side, hop],
                    send_sem=s_send.at[m, side],
                    recv_sem=s_recv.at[m, side, hop],
                    device_id=up if upward else down,
                    device_id_type=pl.DeviceIdType.MESH,
                )
                copy.start()
                square_copies[m, hop, upward] = copy

    def next_round(m, hop):
        if hop + 1 < plan.far:
            project(m, plan.far - 1 - hop, True)
            project(m, plan.far - 1 - hop, False)
        shoot(m, hop, True, early)
        shoot(m, hop, False, late)
        shoot(m, hop, True, late)
        shoot(m, hop, False, early)
        pass_squares(m, hop)

    def carry(m):
        for copy in c_copies[m]:
            copy.wait_recv()
        squares = jnp.zeros((LENGTH, 128), F32)
        outer = dot(conv[m, :, ch + DSTATE : ch + 2 * DSTATE], hstate[m], LANES)
        for j in range(plan.pairs):
            at = slice(j * 128, (j + 1) * 128)
            mixed = y[m, :, at] + zg[m, :, at] * outer[:, at]
            squares = squares + mixed * mixed
            gated[m, :, at] = (mixed * gain[:, at]).astype(BF16)
        first_round(m)
        square_hi, square_lo = split_two(squares)
        ones = jnp.ones((8, 128), BF16)
        square_rows = dot(ones, square_hi, LANES) + dot(ones, square_lo, LANES)
        ssend[m] = square_rows[0:1]
        pass_squares(m, 0)

    carry(0)
    carry(1)
    for hop in range(1, plan.far):
        for m in range(BATCH):
            next_round(m, hop)
    for m in range(BATCH):
        project(m, 0, True)

    for m in range(BATCH):
        square = ssend[m]
        for side, upward in enumerate((True, False)):
            last = (plan.far if upward else plan.far - 1) - 1
            if last >= 0:
                square_copies[m, last, upward].wait_recv()
            for hop in range(last + 1):
                square = square + srecv[m, side, hop]
        scale = lax.rsqrt(square / INNER + EPSILON)
        for q in (*late, *early):
            rows = slice(q * quarter, (q + 1) * quarter)
            total = part[m, me, rows].astype(F32)
            for upward in (True, False):
                last = hops(q, upward) - 1
                if last >= 0:
                    arrows[m, q, last, upward].wait_recv()
                    buffer = up_recv if upward else dn_recv
                    total = total + buffer[m, last, rows].astype(F32)
            out_ref[m, rows, :] = (total * scale).astype(BF16)

    def sent():
        for copy in halos:
            copy.wait_send()

    pl.when(has_next)(sent)
    for group in (*a_copies, *c_copies):
        for copy in group:
            copy.wait_send()
    sent_halves = BATCH * (2 * plan.far - 1)
    assert QUARTERS == 2 and sent_halves % 2 == 0
    for side, to in enumerate((up, down)):
        pltpu.make_async_remote_copy(
            src_ref=part.at[0, pl.ds(0, sent_halves // 2)],
            dst_ref=part.at[0, pl.ds(0, sent_halves // 2)],
            send_sem=ring_send.at[side],
            recv_sem=up_got.at[0, 0, 0],
            device_id=to,
            device_id_type=pl.DeviceIdType.MESH,
        ).wait_send()
        for m in range(BATCH):
            rows = pl.ds(0, plan.far - side)
            if plan.far > side:
                pltpu.make_async_remote_copy(
                    src_ref=srecv.at[m, side, rows],
                    dst_ref=srecv.at[m, side, rows],
                    send_sem=s_send.at[m, side],
                    recv_sem=s_recv.at[m, side, 0],
                    device_id=to,
                    device_id_type=pl.DeviceIdType.MESH,
                ).wait_send()
    for m in range(BATCH):
        for slot, k in jumps:
            pl.when(goes(k))(b_copies[m][slot].wait_send)


def shards(
    plan,
    x_inner,
    z_gate,
    b_input,
    c_input,
    dt_raw,
    doc_ids,
    conv_x,
    conv_b,
    conv_c,
    dt_bias,
    decay_rate,
    norm_gain,
    w_out,
):
    hbm = pl.BlockSpec(memory_space=pltpu.HBM)
    vmem = pl.BlockSpec(memory_space=pltpu.VMEM)
    ch, ring, members = plan.channels, plan.ring, plan.members
    dma = pltpu.SemaphoreType.DMA
    scratch = [
        pltpu.SMEM((plan.heads,), F32),
        pltpu.SMEM((plan.heads,), F32),
        pltpu.VMEM((ch,), F32),
        pltpu.VMEM((BATCH, LENGTH, plan.conv), BF16),
        pltpu.VMEM((BATCH, HALO, plan.conv), BF16),
        pltpu.VMEM((BATCH, LENGTH), jnp.int32),
        pltpu.VMEM((BATCH, 128), jnp.int32),
        pltpu.VMEM((plan.heads, BATCH, LENGTH), F32),
        pltpu.VMEM((TAPS, plan.conv), BF16),
        pltpu.VMEM((BATCH, LENGTH, ch), BF16),
        pltpu.VMEM((ch, plan.width), BF16),
        pltpu.VMEM((plan.width, ch), BF16),
        pltpu.VMEM((BATCH, LENGTH, plan.conv), BF16),
        pltpu.VMEM((BATCH, TAPS - 1, LENGTH, 128), F32),
        pltpu.VMEM((BATCH, ch, DSTATE), F32),
        pltpu.VMEM((BATCH, LENGTH, ch), BF16),
        pltpu.VMEM((BATCH, LENGTH, ch), F32),
        pltpu.VMEM((BATCH, LENGTH, LENGTH), F32),
        pltpu.VMEM((BATCH, LENGTH, ch), F32),
        pltpu.VMEM((BATCH, LENGTH, ch), BF16),
        pltpu.VMEM((BATCH, ring, plan.packet, DSTATE), BF16),
        pltpu.VMEM((BATCH, ring, plan.packet, DSTATE), BF16),
        pltpu.VMEM((BATCH, ring, plan.shard, DSTATE), F32),
        pltpu.VMEM((BATCH, ring, plan.gate_rows, DSTATE), F32),
        pltpu.VMEM((BATCH, plan.packet, DSTATE), BF16),
        pltpu.VMEM((BATCH, plan.packet, DSTATE), BF16),
        pltpu.VMEM((BATCH, plan.shard, DSTATE), F32),
        pltpu.VMEM((BATCH, plan.gate_rows, DSTATE), F32),
        pltpu.VMEM((BATCH, 3, plan.packet, DSTATE), BF16),
        pltpu.VMEM((BATCH, ring, plan.shard, DSTATE), BF16),
        pltpu.VMEM((BATCH, ch, DSTATE), BF16),
        pltpu.VMEM((BATCH, members, plan.out, LENGTH), BF16),
        pltpu.VMEM((BATCH, plan.far, plan.out, LENGTH), BF16),
        pltpu.VMEM((BATCH, plan.far, plan.out, LENGTH), BF16),
        pltpu.VMEM((BATCH, 1, LENGTH), F32),
        pltpu.VMEM((BATCH, 2, plan.far, 1, LENGTH), F32),
        dma((9,)),
        dma((BATCH + 1,)),
        dma((BATCH + 1,)),
        dma((BATCH,)),
        dma((BATCH,)),
        dma((BATCH, 3)),
        dma((BATCH, 3)),
        dma((BATCH,)),
        dma((BATCH,)),
        dma((BATCH, 2)),
        dma((BATCH, 2, plan.far)),
        dma((2,)),
        dma((BATCH, QUARTERS, plan.far)),
        dma((BATCH, QUARTERS, plan.far)),
        pltpu.SemaphoreType.REGULAR((2,)),
    ]
    out = pl.pallas_call(
        functools.partial(layer_kernel, plan),
        name="mixer_layer",
        out_shape=pltpu.VMEM((BATCH, plan.out, LENGTH), BF16),
        in_specs=[hbm] * 13,
        out_specs=vmem,
        scratch_shapes=scratch,
        compiler_params=pltpu.CompilerParams(
            collective_id=0, has_side_effects=True, vmem_limit_bytes=60 * 1024 * 1024
        ),
    )(
        x_inner,
        z_gate,
        b_input,
        c_input,
        jnp.transpose(dt_raw, (2, 0, 1)),
        doc_ids,
        conv_x,
        conv_b,
        conv_c,
        dt_bias,
        decay_rate,
        norm_gain,
        w_out,
    )
    return jnp.transpose(out, (0, 2, 1))


def solution(mesh):
    members = mesh.shape["mp"]
    line = Mesh(mesh.devices.reshape(*SPLIT, members), (*SEQ, "mp"))

    def layer(*arrays):
        channels = arrays[0].shape[2] // members
        plan = Plan(SPLIT, members, channels, arrays[12].shape[1])
        placed = (
            P(None, SEQ, "mp"),
            P(None, SEQ, "mp"),
            P(None, SEQ, None),
            P(None, SEQ, None),
            P(None, SEQ, "mp"),
            P(None, SEQ),
            P(None, "mp"),
            P(),
            P(),
            P("mp"),
            P("mp"),
            P("mp"),
            P("mp", None),
        )
        return jax.shard_map(
            functools.partial(shards, plan),
            mesh=line,
            in_specs=placed,
            out_specs=P(None, SEQ, "mp"),
            check_vma=False,
        )(*arrays)

    return layer
```

```python
import functools

import jax
import jax.numpy as jnp
from jax import lax
from jax.experimental import pallas as pl
from jax.experimental.pallas import tpu as pltpu
from jax.sharding import Mesh
from jax.sharding import PartitionSpec as P

SPLIT = (8, 4, 2)
SEQ = ("sz", "sx", "sc")
INNER = 5120
EPSILON = 1e-05
BATCH = 2
LENGTH = 256
HALF = 128
QUARTERS = 2
HALO = 8
TAPS = 4
HEADDIM = 64
DSTATE = 128
REACH = 8192 // LENGTH
F32 = jnp.float32
BF16 = jnp.bfloat16
LANES = (((1,), (1,)), ((), ()))
ROWS = (((0,), (0,)), ((), ()))


def dot(a, b, dims):
    return lax.dot_general(a, b, dims, preferred_element_type=F32)


def split_two(value):
    high = value.astype(BF16)
    return high, (value - high.astype(F32)).astype(BF16)


def silu(value):
    return value / (1.0 + jnp.exp(-value))


class Plan:
    def __init__(self, split, members, channels, width):
        self.planes, self.xs, self.cores = split
        self.ring = self.xs * self.cores
        self.members = members
        self.channels = channels
        self.heads = channels // HEADDIM
        self.pairs = self.heads // 2
        self.conv = channels + 2 * DSTATE
        self.shard = channels // self.ring
        self.groups = self.shard // 16
        self.gate_rows = max(8, 1 << (self.groups - 1).bit_length())
        self.packet = self.shard + 2 * self.gate_rows
        assert REACH <= 4 * self.ring or self.planes <= 5
        self.width = width
        self.out = width // members
        self.far = members // 2


def spread(rows, plan):
    return jnp.concatenate(
        [jnp.broadcast_to(rows[q : q + 1], (16, DSTATE)) for q in range(plan.groups)], axis=0
    )


def pair_columns(cols, first, lane):
    a = jnp.broadcast_to(cols[:, first : first + 1], (cols.shape[0], 128))
    b = jnp.broadcast_to(cols[:, first + 1 : first + 2], (cols.shape[0], 128))
    return jnp.where(lane < HEADDIM, a, b)


def layer_kernel(
    plan,
    x_hbm,
    z_hbm,
    b_hbm,
    c_hbm,
    dt_hbm,
    doc_hbm,
    cx_hbm,
    cb_hbm,
    cc_hbm,
    bias_hbm,
    rate_hbm,
    gain_hbm,
    w_hbm,
    out_ref,
    bias_ref,
    rate_ref,
    gain_ref,
    xbc,
    halo,
    docs_ref,
    doc_halo,
    dt_ref,
    taps,
    z_ref,
    w_ref,
    wt,
    conv,
    masks,
    main_state,
    xw,
    y,
    scores,
    zg,
    gated,
    fsend,
    arecv,
    pref,
    qpref,
    tsend,
    usend,
    ptot,
    qtot,
    brecv,
    hsend,
    hstate,
    part,
    up_recv,
    dn_recv,
    ssend,
    srecv,
    load_sem,
    halo_send,
    halo_recv,
    a_send,
    a_recv,
    b_send,
    b_recv,
    c_send,
    c_recv,
    s_send,
    s_recv,
    ring_send,
    up_got,
    dn_got,
    word,
):
    ch, nh, ring, members = plan.channels, plan.heads, plan.ring, plan.members
    iz, ix, ic = lax.axis_index("sz"), lax.axis_index("sx"), lax.axis_index("sc")
    me = lax.axis_index("mp")
    rank = ix * plan.cores + ic
    place = iz * ring + rank
    blocks = plan.planes * ring

    def in_plane(r):
        return {"sx": r // plan.cores, "sc": r % plan.cores}

    def in_line(j):
        return {"sz": j // ring, "sx": (j % ring) // plan.cores, "sc": j % plan.cores}

    after, prior = in_line(place + 1), in_line(place - 1)
    up = {"mp": lax.rem(me + 1, members)}
    down = {"mp": lax.rem(me + members - 1, members)}

    has_next, has_prior = place + 1 < blocks, place > 0

    def one(flag):
        return jnp.where(flag, 1, 0)

    barrier = pltpu.get_barrier_semaphore()

    def greet(peer):
        pl.semaphore_signal(barrier, inc=1, device_id=peer, device_id_type=pl.DeviceIdType.MESH)

    for k in range(1, ring):
        greet(in_plane(lax.rem(rank + k, ring)))
    greet(up)
    greet(down)
    pl.when(has_prior)(lambda: greet(prior))
    count = ring - 1 + 2 + one(has_next)
    above, below = {"sz": iz + 1}, {"sz": iz - 1}
    has_above, has_below = iz + 1 < plan.planes, iz > 0
    pl.when(has_below)(lambda: greet(below))
    pl.when(has_above)(lambda: greet(above))
    count = count + one(has_above) + one(has_below)

    def tell_below(at):
        pl.semaphore_signal(
            word.at[at], inc=1, device_id=below, device_id_type=pl.DeviceIdType.MESH
        )

    loads = []

    def load(src, dst, sem=None):
        copy = pltpu.make_async_copy(src, dst, load_sem.at[len(loads) if sem is None else sem])
        copy.start()
        if sem is None:
            loads.append(copy)
        return copy

    def load_group(copies, whole):
        sem = len(loads)
        for src, dst in copies:
            load(src, dst, sem)
        loads.append(pltpu.make_async_copy(whole, whole, load_sem.at[sem]))
        return loads[-1]

    done = []

    def need(copy):
        if not any(copy is other for other in done):
            copy.wait()
            done.append(copy)

    def got_waits():
        for copy in loads:
            need(copy)

    got_docs = load(doc_hbm, docs_ref)
    row_parts = []
    for m in range(BATCH):
        row_parts += [
            (x_hbm.at[m], xbc.at[m, :, pl.ds(0, ch)]),
            (b_hbm.at[m], xbc.at[m, :, pl.ds(ch, DSTATE)]),
            (c_hbm.at[m], xbc.at[m, :, pl.ds(ch + DSTATE, DSTATE)]),
        ]
    got_rows = load_group(row_parts, xbc)
    got_dt = [load(dt_hbm, dt_ref), load(bias_hbm, bias_ref), load(rate_hbm, rate_ref)]
    got_taps = load_group(
        [
            (cx_hbm, taps.at[:, pl.ds(0, ch)]),
            (cb_hbm, taps.at[:, pl.ds(ch, DSTATE)]),
            (cc_hbm, taps.at[:, pl.ds(ch + DSTATE, DSTATE)]),
        ],
        taps,
    )
    got_gain = load(gain_hbm, gain_ref)

    need(got_docs)
    need(got_rows)
    got_z = load(z_hbm, z_ref)
    got_w = load(w_hbm, w_ref)
    pl.semaphore_wait(barrier, count)
    pl.when(has_below & has_above)(lambda: tell_below(0))

    halos = [
        pltpu.make_async_remote_copy(
            src_ref=docs_ref.at[:, pl.ds(LENGTH - 128, 128)],
            dst_ref=doc_halo,
            send_sem=halo_send.at[0],
            recv_sem=halo_recv.at[0],
            device_id=after,
            device_id_type=pl.DeviceIdType.MESH,
        ),
        pltpu.make_async_remote_copy(
            src_ref=xbc.at[:, pl.ds(LENGTH - HALO, HALO)],
            dst_ref=halo,
            send_sem=halo_send.at[1],
            recv_sem=halo_recv.at[1],
            device_id=after,
            device_id_type=pl.DeviceIdType.MESH,
        ),
    ]

    def send_halo():
        for copy in halos:
            copy.start()

    pl.when(has_next)(send_halo)

    lane = lax.broadcasted_iota(jnp.int32, (LENGTH, 128), 1)

    docs = docs_ref[...].astype(F32)
    marks = []
    for m in range(BATCH):
        own = docs[m : m + 1]
        marks.append(own)
        for k in range(1, TAPS):
            marks.append(jnp.where(pltpu.roll(own, k, 1) == own, 1.0, 0.0))
    mark_cols = jnp.concatenate(marks, axis=0).T
    for m in range(BATCH):
        for k in range(1, TAPS):
            at = m * TAPS + k
            masks[m, k - 1] = jnp.broadcast_to(mark_cols[:, at : at + 1], (LENGTH, 128))
    for copy in got_dt:
        need(copy)
    head_row = lax.broadcasted_iota(jnp.int32, (16, LENGTH), 0)
    bias = jnp.zeros((16, LENGTH), F32)
    rate = jnp.zeros((16, LENGTH), F32)
    for h in range(nh):
        bias = jnp.where(head_row == h, bias_ref[h], bias)
        rate = jnp.where(head_row == h, rate_ref[h], rate)
    step_rows, log_parts = [], []
    for m in range(BATCH):
        raw = dt_ref[:, m, :]
        if nh < 16:
            raw = jnp.concatenate([raw, jnp.zeros((16 - nh, LENGTH), F32)], axis=0)
        shifted = raw + bias
        step = jnp.maximum(shifted, 0.0) + jnp.log1p(jnp.exp(-jnp.abs(shifted)))
        step_rows.append(step)
        log_parts.append(-(step * rate))
    log_step = jnp.concatenate(log_parts, axis=0)
    hi = log_step.astype(BF16)
    rest = log_step - hi.astype(F32)
    mid = rest.astype(BF16)
    low = (rest - mid.astype(F32)).astype(BF16)
    before = lax.broadcasted_iota(jnp.int32, (LENGTH, LENGTH), 0) <= lax.broadcasted_iota(
        jnp.int32, (LENGTH, LENGTH), 1
    )
    upper = jnp.where(before, 1.0, 0.0).astype(BF16)
    sums = dot(jnp.concatenate([low, mid, hi], axis=0), upper, (((1,), (0,)), ((), ())))
    span = BATCH * 16
    log_cum = sums[0:span] + sums[span : 2 * span] + sums[2 * span : 3 * span]
    log_rows = [log_cum[m * 16 : (m + 1) * 16] for m in range(BATCH)]
    row_mats = list(log_rows)
    ends = []
    for m in range(BATCH):
        end = log_rows[m][:, LENGTH - 1 : LENGTH]
        ends.append(end)
        keep = jnp.where(docs[m : m + 1] == docs[m : m + 1, LENGTH - 1 : LENGTH], 1.0, 0.0)
        row_mats.append(jnp.exp(jnp.minimum(end - log_rows[m], 0.0)) * step_rows[m] * keep)
    for m in range(BATCH):
        row_mats.append(jnp.exp(log_rows[m]))
    row_mats.append(jnp.zeros((128 - 3 * span, LENGTH), F32))
    cols = jnp.concatenate(row_mats, axis=0).T
    log_col, weight_col, entry_col = 0, span, 2 * span

    need(got_taps)
    tap = taps[...].astype(F32)
    tiles = plan.conv // 128
    def convolve(m):
        for j in range(tiles):
            at = slice(j * 128, (j + 1) * 128)
            rows = xbc[m, :, at].astype(F32)
            total = rows * tap[TAPS - 1 : TAPS, at]
            for k in range(1, TAPS):
                weight = tap[TAPS - 1 - k : TAPS - k, at]
                total = total + (pltpu.roll(rows, k, 0) * weight) * masks[m, k - 1]
            total = silu(total)
            conv[m, :, at] = total.astype(BF16)
            if j < plan.pairs:
                scale = pair_columns(cols, weight_col + m * 16 + 2 * j, lane)
                xw[m, :, at] = (total.astype(BF16).astype(F32) * scale).astype(BF16)
        xw[m, 0:HALO, :] = jnp.zeros((HALO, ch), BF16)
        main_state[m] = dot(xw[m], conv[m, :, ch : ch + DSTATE], ROWS)

    def turn_weights():
        need(got_w)
        for j in range(plan.width // 128):
            wt[j * 128 : (j + 1) * 128, :] = w_ref[:, j * 128 : (j + 1) * 128].T

    def gate_inputs(m):
        need(got_z)
        for j in range(plan.pairs):
            at = slice(j * 128, (j + 1) * 128)
            zg[m, :, at] = silu(z_ref[m, :, at].astype(F32))

    group_row = lax.broadcasted_iota(jnp.int32, (ring * plan.gate_rows, 16), 0)
    group_head = lax.broadcasted_iota(jnp.int32, (ring * plan.gate_rows, 16), 1)
    bits = plan.gate_rows.bit_length() - 1
    shard_of, group_of = group_row >> bits, group_row & (plan.gate_rows - 1)
    picks = (((shard_of * plan.groups + group_of) >> 2) == group_head) & (group_of < plan.groups)
    pick = jnp.where(picks, 1.0, 0.0).astype(BF16)
    plain = (((1,), (0,)), ((), ()))
    gate_parts = []
    for m in range(BATCH):
        gate_hi, gate_lo = split_two(jnp.broadcast_to(jnp.exp(ends[m]), (16, DSTATE)))
        gate_parts.append((dot(pick, gate_hi, plain), dot(pick, gate_lo, plain)))
    convolve(0)
    pl.when(has_prior)(halos[0].wait_recv)
    doc_before = jnp.where(has_prior, doc_halo[...].astype(F32), -1.0)
    row8 = lax.broadcasted_iota(jnp.int32, (HALO, 128), 0)

    def edge_mask(m, k):
        mask = masks[m, k - 1, 0:HALO]
        for t in range(k):
            at = 128 - k + t
            same = docs[m : m + 1, t : t + 1] == doc_before[m : m + 1, at : at + 1]
            mask = jnp.where(row8 == t, jnp.where(same, 1.0, 0.0), mask)
        return mask

    def exchange(m, source, target, peers_send, peers_recv):
        copies = []
        for k in range(1, ring):
            to = lax.rem(rank + k, ring)
            copies.append(
                pltpu.make_async_remote_copy(
                    src_ref=source.at[m, to],
                    dst_ref=target(to),
                    send_sem=peers_send.at[m],
                    recv_sem=peers_recv.at[m],
                    device_id=in_plane(to),
                    device_id_type=pl.DeviceIdType.MESH,
                )
            )
        return copies

    def all_of(m, ref, send_sem, recv_sem):
        return pltpu.make_async_remote_copy(
            src_ref=ref.at[m, pl.ds(0, ring - 1)],
            dst_ref=ref.at[m, pl.ds(0, ring - 1)],
            send_sem=send_sem.at[m],
            recv_sem=recv_sem.at[m],
            device_id=in_plane(lax.rem(rank + 1, ring)),
            device_id_type=pl.DeviceIdType.MESH,
        )

    a_copies = []
    for m in range(BATCH):
        if m > 0:
            convolve(m)
        else:
            pl.when(has_prior)(halos[1].wait_recv)
        same = [None, *(edge_mask(m, k) for k in range(1, TAPS))]
        scaled = []
        for j in range(tiles):
            at = slice(j * 128, (j + 1) * 128)
            lead = jnp.where(has_prior, halo[m, :, at].astype(F32), 0.0)
            own = xbc[m, 0:HALO, at].astype(F32)
            both = jnp.concatenate([lead, own], axis=0)
            total = own * tap[TAPS - 1 : TAPS, at]
            for k in range(1, TAPS):
                weight = tap[TAPS - 1 - k : TAPS - k, at]
                total = total + (pltpu.roll(both, k, 0)[HALO : 2 * HALO] * weight) * same[k]
            total = silu(total).astype(BF16)
            conv[m, 0:HALO, at] = total
            if j < plan.pairs:
                scale = pair_columns(cols[0:HALO], weight_col + m * 16 + 2 * j, lane[0:HALO])
                scaled.append((total.astype(F32) * scale).astype(BF16))
            if j == plan.pairs:
                first_b = total
        edge_state = dot(jnp.concatenate(scaled, axis=1), first_b, ROWS)
        state = (main_state[m] + edge_state).astype(BF16)
        carried_end = docs[m : m + 1, LENGTH - 1 : LENGTH] == doc_before[m : m + 1, 127:128]
        carried_end = jnp.where(carried_end, 1.0, 0.0)
        hi_rows = (gate_parts[m][0] * carried_end).astype(BF16)
        lo_rows = (gate_parts[m][1] * carried_end).astype(BF16)
        for r in range(ring):
            fsend[m, r, 0 : plan.shard] = state[r * plan.shard : (r + 1) * plan.shard]
            at = slice(r * plan.gate_rows, (r + 1) * plan.gate_rows)
            fsend[m, r, plan.shard : plan.packet] = jnp.concatenate(
                [hi_rows[at], lo_rows[at]], axis=0
            )
        copies = exchange(m, fsend, lambda to, m=m: arecv.at[m, rank], a_send, a_recv)
        for copy in copies:
            copy.start()
        a_copies.append([all_of(m, arecv, a_send, a_recv)])
        arecv[m, pl.ds(rank, 1)] = fsend[m, pl.ds(rank, 1)]

    def scores_of(m):
        t_pos = lax.broadcasted_iota(jnp.int32, (LENGTH, LENGTH), 0)
        s_pos = lax.broadcasted_iota(jnp.int32, (LENGTH, LENGTH), 1)
        doc_t = mark_cols[:, m * TAPS : m * TAPS + 1]
        keep = (s_pos <= t_pos) & (doc_t == docs[m : m + 1])
        full = dot(conv[m, :, ch + DSTATE : ch + 2 * DSTATE], conv[m, :, ch : ch + DSTATE], LANES)
        scores[m] = jnp.where(keep, full, 0.0)

    def inner_of(m):
        low_lane = lane < HEADDIM
        for j in range(plan.pairs):
            at = slice(j * 128, (j + 1) * 128)
            xs = conv[m, :, at]
            xs_a = jnp.where(low_lane, xs, jnp.zeros_like(xs))
            xs_b = jnp.where(low_lane, jnp.zeros_like(xs), xs)
            for half in range(2):
                t0, s1 = half * HALF, (half + 1) * HALF
                base = scores[m, t0 : t0 + HALF, 0:s1]
                mixes = []
                for h in (2 * j, 2 * j + 1):
                    t_log = cols[t0 : t0 + HALF, log_col + m * 16 + h : log_col + m * 16 + h + 1]
                    s_log = log_rows[m][h : h + 1, 0:s1]
                    decay = jnp.exp(jnp.minimum(t_log - s_log, 0.0))
                    mixes.append((base * step_rows[m][h : h + 1, 0:s1] * decay).astype(BF16))
                y[m, t0 : t0 + HALF, at] = dot(
                    jnp.concatenate(mixes, axis=1),
                    jnp.concatenate([xs_a[0:s1], xs_b[0:s1]], axis=0),
                    (((1,), (0,)), ((), ())),
                )

    def gate_both(m):
        carried = mark_cols[:, m * TAPS : m * TAPS + 1] == doc_before[m : m + 1, 127:128]
        for j in range(plan.pairs):
            at = slice(j * 128, (j + 1) * 128)
            opened = zg[m, :, at]
            y[m, :, at] = y[m, :, at] * opened
            entry = pair_columns(cols, entry_col + m * 16 + 2 * j, lane)
            zg[m, :, at] = jnp.where(carried, entry, 0.0) * opened

    def unpack(packet):
        packet = packet.astype(F32)
        split = plan.shard + plan.gate_rows
        return packet[0 : plan.shard], packet[plan.shard : split] + packet[split:]

    def pack(ref, m, total, product):
        ref[m, 0 : plan.shard] = total.astype(BF16)
        hi_rows, lo_rows = split_two(product)
        ref[m, plan.shard : plan.packet] = jnp.concatenate([hi_rows, lo_rows], axis=0)

    def ahead(source, m, slot, k):
        return pltpu.make_async_remote_copy(
            src_ref=source.at[m],
            dst_ref=brecv.at[m, slot],
            send_sem=b_send.at[m, slot],
            recv_sem=b_recv.at[m, slot],
            device_id={"sz": iz + k},
            device_id_type=pl.DeviceIdType.MESH,
        )

    jumps = [(0, 1), (1, 1), (2, 3)]
    b_copies = [
        [ahead(tsend if slot == 0 else usend, m, slot, k) for slot, k in jumps] for m in range(BATCH)
    ]

    def goes(k):
        return iz + k < plan.planes

    def plane_total(m):
        for copy in a_copies[m]:
            copy.wait_recv()
        total = jnp.zeros((plan.shard, DSTATE), F32)
        product = jnp.ones((plan.gate_rows, DSTATE), F32)
        for d in range(ring):
            pref[m, d] = total
            qpref[m, d] = product
            fresh, gates = unpack(arecv[m, d])
            total = spread(gates, plan) * total + fresh
            product = product * gates
        pack(tsend, m, total, product)
        ptot[m] = total
        qtot[m] = product
        pl.when(has_above)(b_copies[m][0].start)

    def two_planes(m):
        pl.when(has_below)(b_copies[m][0].wait_recv)
        lower, gates = unpack(brecv[m, 0])
        lower = jnp.where(has_below, lower, 0.0)
        gates = jnp.where(has_below, gates, 0.0)
        product = qtot[m]
        pack(usend, m, spread(product, plan) * lower + ptot[m], product * gates)
        pl.when(has_above)(b_copies[m][1].start)
        pl.when(goes(3))(b_copies[m][2].start)

    gate_inputs(0)
    scores_of(0)
    pl.when(goes(2))(lambda: pl.semaphore_wait(word.at[0], 1))
    pl.when(has_below & goes(2))(lambda: tell_below(1))
    inner_of(0)
    gate_both(0)
    plane_total(0)
    plane_total(1)
    scores_of(1)
    pl.when(goes(3))(lambda: pl.semaphore_wait(word.at[1], 1))
    two_planes(0)
    two_planes(1)
    inner_of(1)
    c_copies = []
    for m in range(BATCH):
        pl.when(has_below)(b_copies[m][1].wait_recv)
        pl.when(iz >= 3)(b_copies[m][2].wait_recv)
        near, gates = unpack(brecv[m, 1])
        remote, _ = unpack(brecv[m, 2])
        incoming = spread(gates, plan) * jnp.where(iz >= 3, remote, 0.0) + near
        incoming = jnp.where(has_below, incoming, 0.0)
        for d in range(ring):
            entering = pref[m, d] + spread(qpref[m, d], plan) * incoming
            hsend[m, d] = entering.astype(BF16)
        home = pl.ds(pl.multiple_of(rank * plan.shard, 16), plan.shard)
        copies = exchange(m, hsend, lambda to, m=m: hstate.at[m, home], c_send, c_recv)
        for copy in copies:
            copy.start()
        c_copies.append([all_of(m, hsend, c_send, c_recv)])
        hstate[m, home] = hsend[m, rank]
        if m == 0:
            gate_inputs(1)
            gate_both(1)
            turn_weights()

    quarter = plan.out // QUARTERS

    def hops(q, upward):
        return plan.far if (q < QUARTERS // 2) == upward else plan.far - 1

    def owner_at(distance, upward):
        return lax.rem(me + distance if upward else me + members - distance, members)

    def arrow(m, q, hop, upward):
        buffer, send, got, to = (
            (up_recv, ring_send.at[0], up_got, up)
            if upward
            else (dn_recv, ring_send.at[1], dn_got, down)
        )
        rows = pl.ds(q * quarter, quarter)
        return pltpu.make_async_remote_copy(
            src_ref=part.at[m, owner_at(hops(q, upward) - hop, upward), rows],
            dst_ref=buffer.at[m, hop, rows],
            send_sem=send,
            recv_sem=got.at[m, q, hop],
            device_id=to,
            device_id_type=pl.DeviceIdType.MESH,
        )

    arrows = {}
    square_copies = {}
    need(got_gain)
    gain = gain_ref[...].reshape(1, ch)

    def project(m, distance, upward):
        owner = owner_at(distance, upward)
        rows = pl.ds(pl.multiple_of(owner * plan.out, 16), plan.out)
        part[m, owner] = dot(wt[rows, :], gated[m], LANES).astype(BF16)

    def shoot(m, hop, upward, pieces):
        for q in pieces:
            if hop < hops(q, upward):
                if hop > 0:
                    arrows[m, q, hop - 1, upward].wait_recv()
                    buffer = up_recv if upward else dn_recv
                    owner = owner_at(hops(q, upward) - hop, upward)
                    rows = slice(q * quarter, (q + 1) * quarter)
                    total = part[m, owner, rows].astype(F32) + buffer[m, hop - 1, rows].astype(F32)
                    part[m, owner, rows] = total.astype(BF16)
                arrows[m, q, hop, upward] = arrow(m, q, hop, upward)
                arrows[m, q, hop, upward].start()

    early, late = range(QUARTERS // 2), range(QUARTERS // 2, QUARTERS)

    def first_round(m):
        project(m, plan.far, True)
        shoot(m, 0, True, early)
        shoot(m, 0, False, late)
        if plan.far > 1:
            project(m, plan.far - 1, True)
            shoot(m, 0, True, late)
            project(m, plan.far - 1, False)
            shoot(m, 0, False, early)

    def pass_squares(m, hop):
        for side, upward in enumerate((True, False)):
            if hop < (plan.far if upward else plan.far - 1):
                if hop > 0:
                    square_copies[m, hop - 1, upward].wait_recv()
                copy = pltpu.make_async_remote_copy(
                    src_ref=ssend.at[m] if hop == 0 else srecv.at[m, side, hop - 1],
                    dst_ref=srecv.at[m, side, hop],
                    send_sem=s_send.at[m, side],
                    recv_sem=s_recv.at[m, side, hop],
                    device_id=up if upward else down,
                    device_id_type=pl.DeviceIdType.MESH,
                )
                copy.start()
                square_copies[m, hop, upward] = copy

    def next_round(m, hop):
        if hop + 1 < plan.far:
            project(m, plan.far - 1 - hop, True)
            project(m, plan.far - 1 - hop, False)
        shoot(m, hop, True, early)
        shoot(m, hop, False, late)
        shoot(m, hop, True, late)
        shoot(m, hop, False, early)
        pass_squares(m, hop)

    def carry(m):
        for copy in c_copies[m]:
            copy.wait_recv()
        squares = jnp.zeros((LENGTH, 128), F32)
        outer = dot(conv[m, :, ch + DSTATE : ch + 2 * DSTATE], hstate[m], LANES)
        for j in range(plan.pairs):
            at = slice(j * 128, (j + 1) * 128)
            mixed = y[m, :, at] + zg[m, :, at] * outer[:, at]
            squares = squares + mixed * mixed
            gated[m, :, at] = (mixed * gain[:, at]).astype(BF16)
        first_round(m)
        square_hi, square_lo = split_two(squares)
        ones = jnp.ones((8, 128), BF16)
        square_rows = dot(ones, square_hi, LANES) + dot(ones, square_lo, LANES)
        ssend[m] = square_rows[0:1]
        pass_squares(m, 0)

    carry(0)
    carry(1)
    for hop in range(1, plan.far):
        for m in range(BATCH):
            next_round(m, hop)
    for m in range(BATCH):
        project(m, 0, True)

    for m in range(BATCH):
        square = ssend[m]
        for side, upward in enumerate((True, False)):
            last = (plan.far if upward else plan.far - 1) - 1
            if last >= 0:
                square_copies[m, last, upward].wait_recv()
            for hop in range(last + 1):
                square = square + srecv[m, side, hop]
        scale = lax.rsqrt(square / INNER + EPSILON)
        for q in (*late, *early):
            rows = slice(q * quarter, (q + 1) * quarter)
            total = part[m, me, rows].astype(F32)
            for upward in (True, False):
                last = hops(q, upward) - 1
                if last >= 0:
                    arrows[m, q, last, upward].wait_recv()
                    buffer = up_recv if upward else dn_recv
                    total = total + buffer[m, last, rows].astype(F32)
            out_ref[m, rows, :] = (total * scale).astype(BF16)

    def sent():
        for copy in halos:
            copy.wait_send()

    pl.when(has_next)(sent)
    for group in (*a_copies, *c_copies):
        for copy in group:
            copy.wait_send()
    sent_halves = BATCH * (2 * plan.far - 1)
    assert QUARTERS == 2 and sent_halves % 2 == 0
    for side, to in enumerate((up, down)):
        pltpu.make_async_remote_copy(
            src_ref=part.at[0, pl.ds(0, sent_halves // 2)],
            dst_ref=part.at[0, pl.ds(0, sent_halves // 2)],
            send_sem=ring_send.at[side],
            recv_sem=up_got.at[0, 0, 0],
            device_id=to,
            device_id_type=pl.DeviceIdType.MESH,
        ).wait_send()
        for m in range(BATCH):
            rows = pl.ds(0, plan.far - side)
            if plan.far > side:
                pltpu.make_async_remote_copy(
                    src_ref=srecv.at[m, side, rows],
                    dst_ref=srecv.at[m, side, rows],
                    send_sem=s_send.at[m, side],
                    recv_sem=s_recv.at[m, side, 0],
                    device_id=to,
                    device_id_type=pl.DeviceIdType.MESH,
                ).wait_send()
    for m in range(BATCH):
        for slot, k in jumps:
            pl.when(goes(k))(b_copies[m][slot].wait_send)


def shards(
    plan,
    x_inner,
    z_gate,
    b_input,
    c_input,
    dt_raw,
    doc_ids,
    conv_x,
    conv_b,
    conv_c,
    dt_bias,
    decay_rate,
    norm_gain,
    w_out,
):
    hbm = pl.BlockSpec(memory_space=pltpu.HBM)
    vmem = pl.BlockSpec(memory_space=pltpu.VMEM)
    ch, ring, members = plan.channels, plan.ring, plan.members
    dma = pltpu.SemaphoreType.DMA
    scratch = [
        pltpu.SMEM((plan.heads,), F32),
        pltpu.SMEM((plan.heads,), F32),
        pltpu.VMEM((ch,), F32),
        pltpu.VMEM((BATCH, LENGTH, plan.conv), BF16),
        pltpu.VMEM((BATCH, HALO, plan.conv), BF16),
        pltpu.VMEM((BATCH, LENGTH), jnp.int32),
        pltpu.VMEM((BATCH, 128), jnp.int32),
        pltpu.VMEM((plan.heads, BATCH, LENGTH), F32),
        pltpu.VMEM((TAPS, plan.conv), BF16),
        pltpu.VMEM((BATCH, LENGTH, ch), BF16),
        pltpu.VMEM((ch, plan.width), BF16),
        pltpu.VMEM((plan.width, ch), BF16),
        pltpu.VMEM((BATCH, LENGTH, plan.conv), BF16),
        pltpu.VMEM((BATCH, TAPS - 1, LENGTH, 128), F32),
        pltpu.VMEM((BATCH, ch, DSTATE), F32),
        pltpu.VMEM((BATCH, LENGTH, ch), BF16),
        pltpu.VMEM((BATCH, LENGTH, ch), F32),
        pltpu.VMEM((BATCH, LENGTH, LENGTH), F32),
        pltpu.VMEM((BATCH, LENGTH, ch), F32),
        pltpu.VMEM((BATCH, LENGTH, ch), BF16),
        pltpu.VMEM((BATCH, ring, plan.packet, DSTATE), BF16),
        pltpu.VMEM((BATCH, ring, plan.packet, DSTATE), BF16),
        pltpu.VMEM((BATCH, ring, plan.shard, DSTATE), F32),
        pltpu.VMEM((BATCH, ring, plan.gate_rows, DSTATE), F32),
        pltpu.VMEM((BATCH, plan.packet, DSTATE), BF16),
        pltpu.VMEM((BATCH, plan.packet, DSTATE), BF16),
        pltpu.VMEM((BATCH, plan.shard, DSTATE), F32),
        pltpu.VMEM((BATCH, plan.gate_rows, DSTATE), F32),
        pltpu.VMEM((BATCH, 3, plan.packet, DSTATE), BF16),
        pltpu.VMEM((BATCH, ring, plan.shard, DSTATE), BF16),
        pltpu.VMEM((BATCH, ch, DSTATE), BF16),
        pltpu.VMEM((BATCH, members, plan.out, LENGTH), BF16),
        pltpu.VMEM((BATCH, plan.far, plan.out, LENGTH), BF16),
        pltpu.VMEM((BATCH, plan.far, plan.out, LENGTH), BF16),
        pltpu.VMEM((BATCH, 1, LENGTH), F32),
        pltpu.VMEM((BATCH, 2, plan.far, 1, LENGTH), F32),
        dma((9,)),
        dma((2,)),
        dma((2,)),
        dma((BATCH,)),
        dma((BATCH,)),
        dma((BATCH, 3)),
        dma((BATCH, 3)),
        dma((BATCH,)),
        dma((BATCH,)),
        dma((BATCH, 2)),
        dma((BATCH, 2, plan.far)),
        dma((2,)),
        dma((BATCH, QUARTERS, plan.far)),
        dma((BATCH, QUARTERS, plan.far)),
        pltpu.SemaphoreType.REGULAR((2,)),
    ]
    out = pl.pallas_call(
        functools.partial(layer_kernel, plan),
        name="mixer_layer",
        out_shape=pltpu.VMEM((BATCH, plan.out, LENGTH), BF16),
        in_specs=[hbm] * 13,
        out_specs=vmem,
        scratch_shapes=scratch,
        compiler_params=pltpu.CompilerParams(
            collective_id=0, has_side_effects=True, vmem_limit_bytes=60 * 1024 * 1024
        ),
    )(
        x_inner,
        z_gate,
        b_input,
        c_input,
        jnp.transpose(dt_raw, (2, 0, 1)),
        doc_ids,
        conv_x,
        conv_b,
        conv_c,
        dt_bias,
        decay_rate,
        norm_gain,
        w_out,
    )
    return jnp.transpose(out, (0, 2, 1))


def solution(mesh):
    members = mesh.shape["mp"]
    line = Mesh(mesh.devices.reshape(*SPLIT, members), (*SEQ, "mp"))

    def layer(*arrays):
        channels = arrays[0].shape[2] // members
        plan = Plan(SPLIT, members, channels, arrays[12].shape[1])
        placed = (
            P(None, SEQ, "mp"),
            P(None, SEQ, "mp"),
            P(None, SEQ, None),
            P(None, SEQ, None),
            P(None, SEQ, "mp"),
            P(None, SEQ),
            P(None, "mp"),
            P(),
            P(),
            P("mp"),
            P("mp"),
            P("mp"),
            P("mp", None),
        )
        return jax.shard_map(
            functools.partial(shards, plan),
            mesh=line,
            in_specs=placed,
            out_specs=P(None, SEQ, "mp"),
            check_vma=False,
        )(*arrays)

    return layer
```

```python
import functools

import jax
import jax.numpy as jnp
from jax import lax
from jax.experimental import pallas as pl
from jax.experimental.pallas import tpu as pltpu
from jax.sharding import Mesh
from jax.sharding import PartitionSpec as P

SPLIT = (8, 4, 2)
SEQ = ("sz", "sx", "sc")
INNER = 5120
EPSILON = 1e-05
BATCH = 2
LENGTH = 256
HALF = 128
QUARTERS = 2
HALO = 8
TAPS = 4
HEADDIM = 64
DSTATE = 128
REACH = 8192 // LENGTH
F32 = jnp.float32
BF16 = jnp.bfloat16
LANES = (((1,), (1,)), ((), ()))
ROWS = (((0,), (0,)), ((), ()))


def dot(a, b, dims):
    return lax.dot_general(a, b, dims, preferred_element_type=F32)


def split_two(value):
    high = value.astype(BF16)
    return high, (value - high.astype(F32)).astype(BF16)


def silu(value):
    return value / (1.0 + jnp.exp(-value))


class Plan:
    def __init__(self, split, members, channels, width):
        self.planes, self.xs, self.cores = split
        self.ring = self.xs * self.cores
        self.members = members
        self.channels = channels
        self.heads = channels // HEADDIM
        self.pairs = self.heads // 2
        self.conv = channels + 2 * DSTATE
        self.shard = channels // self.ring
        self.groups = self.shard // 16
        self.gate_rows = max(8, 1 << (self.groups - 1).bit_length())
        self.packet = self.shard + 2 * self.gate_rows
        assert REACH <= 4 * self.ring or self.planes <= 5
        self.width = width
        self.out = width // members
        self.far = members // 2


def spread(rows, plan):
    return jnp.concatenate(
        [jnp.broadcast_to(rows[q : q + 1], (16, DSTATE)) for q in range(plan.groups)], axis=0
    )


def pair_columns(cols, first, lane):
    a = jnp.broadcast_to(cols[:, first : first + 1], (cols.shape[0], 128))
    b = jnp.broadcast_to(cols[:, first + 1 : first + 2], (cols.shape[0], 128))
    return jnp.where(lane < HEADDIM, a, b)


def layer_kernel(
    plan,
    x_hbm,
    z_hbm,
    b_hbm,
    c_hbm,
    dt_hbm,
    doc_hbm,
    cx_hbm,
    cb_hbm,
    cc_hbm,
    bias_hbm,
    rate_hbm,
    gain_hbm,
    w_hbm,
    out_ref,
    bias_ref,
    rate_ref,
    gain_ref,
    xbc,
    halo,
    docs_ref,
    doc_halo,
    dt_ref,
    taps,
    z_ref,
    w_ref,
    wt,
    conv,
    masks,
    main_state,
    xw,
    y,
    scores,
    zg,
    gated,
    fsend,
    arecv,
    pref,
    qpref,
    tsend,
    usend,
    ptot,
    qtot,
    brecv,
    hsend,
    hstate,
    part,
    up_recv,
    dn_recv,
    ssend,
    srecv,
    load_sem,
    halo_send,
    halo_recv,
    a_send,
    a_recv,
    b_send,
    b_recv,
    c_send,
    c_recv,
    s_send,
    s_recv,
    ring_send,
    up_got,
    dn_got,
    word,
):
    ch, nh, ring, members = plan.channels, plan.heads, plan.ring, plan.members
    iz, ix, ic = lax.axis_index("sz"), lax.axis_index("sx"), lax.axis_index("sc")
    me = lax.axis_index("mp")
    rank = ix * plan.cores + ic
    place = iz * ring + rank
    blocks = plan.planes * ring

    def in_plane(r):
        return {"sx": r // plan.cores, "sc": r % plan.cores}

    def in_line(j):
        return {"sz": j // ring, "sx": (j % ring) // plan.cores, "sc": j % plan.cores}

    after, prior = in_line(place + 1), in_line(place - 1)
    up = {"mp": lax.rem(me + 1, members)}
    down = {"mp": lax.rem(me + members - 1, members)}

    loads = []

    def load(src, dst, sem=None):
        copy = pltpu.make_async_copy(src, dst, load_sem.at[len(loads) if sem is None else sem])
        copy.start()
        if sem is None:
            loads.append(copy)
        return copy

    def load_group(copies, whole):
        sem = len(loads)
        for src, dst in copies:
            load(src, dst, sem)
        loads.append(pltpu.make_async_copy(whole, whole, load_sem.at[sem]))
        return loads[-1]

    done = []

    def need(copy):
        if not any(copy is other for other in done):
            copy.wait()
            done.append(copy)

    def got_waits():
        for copy in loads:
            need(copy)

    got_docs = load(doc_hbm, docs_ref)
    row_parts = []
    for m in range(BATCH):
        row_parts += [
            (x_hbm.at[m], xbc.at[m, :, pl.ds(0, ch)]),
            (b_hbm.at[m], xbc.at[m, :, pl.ds(ch, DSTATE)]),
            (c_hbm.at[m], xbc.at[m, :, pl.ds(ch + DSTATE, DSTATE)]),
        ]
    got_rows = load_group(row_parts, xbc)
    got_dt = [load(dt_hbm, dt_ref), load(bias_hbm, bias_ref), load(rate_hbm, rate_ref)]
    got_taps = load_group(
        [
            (cx_hbm, taps.at[:, pl.ds(0, ch)]),
            (cb_hbm, taps.at[:, pl.ds(ch, DSTATE)]),
            (cc_hbm, taps.at[:, pl.ds(ch + DSTATE, DSTATE)]),
        ],
        taps,
    )
    got_gain = load(gain_hbm, gain_ref)

    has_next, has_prior = place + 1 < blocks, place > 0

    def one(flag):
        return jnp.where(flag, 1, 0)

    barrier = pltpu.get_barrier_semaphore()

    def greet(peer):
        pl.semaphore_signal(barrier, inc=1, device_id=peer, device_id_type=pl.DeviceIdType.MESH)

    for k in range(1, ring):
        greet(in_plane(lax.rem(rank + k, ring)))
    greet(up)
    greet(down)
    pl.when(has_prior)(lambda: greet(prior))
    count = ring - 1 + 2 + one(has_next)
    above, below = {"sz": iz + 1}, {"sz": iz - 1}
    has_above, has_below = iz + 1 < plan.planes, iz > 0
    pl.when(has_below)(lambda: greet(below))
    pl.when(has_above)(lambda: greet(above))
    count = count + one(has_above) + one(has_below)

    def tell_below(at):
        pl.semaphore_signal(
            word.at[at], inc=1, device_id=below, device_id_type=pl.DeviceIdType.MESH
        )

    need(got_docs)
    need(got_rows)
    got_z = load(z_hbm, z_ref)
    got_w = load(w_hbm, w_ref)
    pl.semaphore_wait(barrier, count)
    pl.when(has_below & has_above)(lambda: tell_below(0))

    halos = [
        pltpu.make_async_remote_copy(
            src_ref=docs_ref.at[:, pl.ds(LENGTH - 128, 128)],
            dst_ref=doc_halo,
            send_sem=halo_send.at[0],
            recv_sem=halo_recv.at[0],
            device_id=after,
            device_id_type=pl.DeviceIdType.MESH,
        ),
        pltpu.make_async_remote_copy(
            src_ref=xbc.at[:, pl.ds(LENGTH - HALO, HALO)],
            dst_ref=halo,
            send_sem=halo_send.at[1],
            recv_sem=halo_recv.at[1],
            device_id=after,
            device_id_type=pl.DeviceIdType.MESH,
        ),
    ]

    def send_halo():
        for copy in halos:
            copy.start()

    pl.when(has_next)(send_halo)

    lane = lax.broadcasted_iota(jnp.int32, (LENGTH, 128), 1)

    docs = docs_ref[...].astype(F32)
    marks = []
    for m in range(BATCH):
        own = docs[m : m + 1]
        marks.append(own)
        for k in range(1, TAPS):
            marks.append(jnp.where(pltpu.roll(own, k, 1) == own, 1.0, 0.0))
    mark_cols = jnp.concatenate(marks, axis=0).T
    for m in range(BATCH):
        for k in range(1, TAPS):
            at = m * TAPS + k
            masks[m, k - 1] = jnp.broadcast_to(mark_cols[:, at : at + 1], (LENGTH, 128))
    for copy in got_dt:
        need(copy)
    head_row = lax.broadcasted_iota(jnp.int32, (16, LENGTH), 0)
    bias = jnp.zeros((16, LENGTH), F32)
    rate = jnp.zeros((16, LENGTH), F32)
    for h in range(nh):
        bias = jnp.where(head_row == h, bias_ref[h], bias)
        rate = jnp.where(head_row == h, rate_ref[h], rate)
    step_rows, log_parts = [], []
    for m in range(BATCH):
        raw = dt_ref[:, m, :]
        if nh < 16:
            raw = jnp.concatenate([raw, jnp.zeros((16 - nh, LENGTH), F32)], axis=0)
        shifted = raw + bias
        step = jnp.maximum(shifted, 0.0) + jnp.log1p(jnp.exp(-jnp.abs(shifted)))
        step_rows.append(step)
        log_parts.append(-(step * rate))
    log_step = jnp.concatenate(log_parts, axis=0)
    hi = log_step.astype(BF16)
    rest = log_step - hi.astype(F32)
    mid = rest.astype(BF16)
    low = (rest - mid.astype(F32)).astype(BF16)
    before = lax.broadcasted_iota(jnp.int32, (LENGTH, LENGTH), 0) <= lax.broadcasted_iota(
        jnp.int32, (LENGTH, LENGTH), 1
    )
    upper = jnp.where(before, 1.0, 0.0).astype(BF16)
    sums = dot(jnp.concatenate([low, mid, hi], axis=0), upper, (((1,), (0,)), ((), ())))
    span = BATCH * 16
    log_cum = sums[0:span] + sums[span : 2 * span] + sums[2 * span : 3 * span]
    log_rows = [log_cum[m * 16 : (m + 1) * 16] for m in range(BATCH)]
    row_mats = list(log_rows)
    ends = []
    for m in range(BATCH):
        end = log_rows[m][:, LENGTH - 1 : LENGTH]
        ends.append(end)
        keep = jnp.where(docs[m : m + 1] == docs[m : m + 1, LENGTH - 1 : LENGTH], 1.0, 0.0)
        row_mats.append(jnp.exp(jnp.minimum(end - log_rows[m], 0.0)) * step_rows[m] * keep)
    for m in range(BATCH):
        row_mats.append(jnp.exp(log_rows[m]))
    row_mats.append(jnp.zeros((128 - 3 * span, LENGTH), F32))
    cols = jnp.concatenate(row_mats, axis=0).T
    log_col, weight_col, entry_col = 0, span, 2 * span

    need(got_taps)
    tap = taps[...].astype(F32)
    tiles = plan.conv // 128
    def convolve(m):
        for j in range(tiles):
            at = slice(j * 128, (j + 1) * 128)
            rows = xbc[m, :, at].astype(F32)
            total = rows * tap[TAPS - 1 : TAPS, at]
            for k in range(1, TAPS):
                weight = tap[TAPS - 1 - k : TAPS - k, at]
                total = total + (pltpu.roll(rows, k, 0) * weight) * masks[m, k - 1]
            total = silu(total)
            conv[m, :, at] = total.astype(BF16)
            if j < plan.pairs:
                scale = pair_columns(cols, weight_col + m * 16 + 2 * j, lane)
                xw[m, :, at] = (total.astype(BF16).astype(F32) * scale).astype(BF16)
        xw[m, 0:HALO, :] = jnp.zeros((HALO, ch), BF16)
        main_state[m] = dot(xw[m], conv[m, :, ch : ch + DSTATE], ROWS)

    def turn_weights():
        need(got_w)
        for j in range(plan.width // 128):
            wt[j * 128 : (j + 1) * 128, :] = w_ref[:, j * 128 : (j + 1) * 128].T

    def gate_inputs(m):
        need(got_z)
        for j in range(plan.pairs):
            at = slice(j * 128, (j + 1) * 128)
            zg[m, :, at] = silu(z_ref[m, :, at].astype(F32))

    group_row = lax.broadcasted_iota(jnp.int32, (ring * plan.gate_rows, 16), 0)
    group_head = lax.broadcasted_iota(jnp.int32, (ring * plan.gate_rows, 16), 1)
    bits = plan.gate_rows.bit_length() - 1
    shard_of, group_of = group_row >> bits, group_row & (plan.gate_rows - 1)
    picks = (((shard_of * plan.groups + group_of) >> 2) == group_head) & (group_of < plan.groups)
    pick = jnp.where(picks, 1.0, 0.0).astype(BF16)
    plain = (((1,), (0,)), ((), ()))
    gate_parts = []
    for m in range(BATCH):
        gate_hi, gate_lo = split_two(jnp.broadcast_to(jnp.exp(ends[m]), (16, DSTATE)))
        gate_parts.append((dot(pick, gate_hi, plain), dot(pick, gate_lo, plain)))
    convolve(0)
    pl.when(has_prior)(halos[0].wait_recv)
    doc_before = jnp.where(has_prior, doc_halo[...].astype(F32), -1.0)
    row8 = lax.broadcasted_iota(jnp.int32, (HALO, 128), 0)

    def edge_mask(m, k):
        mask = masks[m, k - 1, 0:HALO]
        for t in range(k):
            at = 128 - k + t
            same = docs[m : m + 1, t : t + 1] == doc_before[m : m + 1, at : at + 1]
            mask = jnp.where(row8 == t, jnp.where(same, 1.0, 0.0), mask)
        return mask

    def exchange(m, source, target, peers_send, peers_recv):
        copies = []
        for k in range(1, ring):
            to = lax.rem(rank + k, ring)
            copies.append(
                pltpu.make_async_remote_copy(
                    src_ref=source.at[m, to],
                    dst_ref=target(to),
                    send_sem=peers_send.at[m],
                    recv_sem=peers_recv.at[m],
                    device_id=in_plane(to),
                    device_id_type=pl.DeviceIdType.MESH,
                )
            )
        return copies

    def all_of(m, ref, send_sem, recv_sem):
        return pltpu.make_async_remote_copy(
            src_ref=ref.at[m, pl.ds(0, ring - 1)],
            dst_ref=ref.at[m, pl.ds(0, ring - 1)],
            send_sem=send_sem.at[m],
            recv_sem=recv_sem.at[m],
            device_id=in_plane(lax.rem(rank + 1, ring)),
            device_id_type=pl.DeviceIdType.MESH,
        )

    a_copies = []
    for m in range(BATCH):
        if m > 0:
            convolve(m)
        else:
            pl.when(has_prior)(halos[1].wait_recv)
        same = [None, *(edge_mask(m, k) for k in range(1, TAPS))]
        scaled = []
        for j in range(tiles):
            at = slice(j * 128, (j + 1) * 128)
            lead = jnp.where(has_prior, halo[m, :, at].astype(F32), 0.0)
            own = xbc[m, 0:HALO, at].astype(F32)
            both = jnp.concatenate([lead, own], axis=0)
            total = own * tap[TAPS - 1 : TAPS, at]
            for k in range(1, TAPS):
                weight = tap[TAPS - 1 - k : TAPS - k, at]
                total = total + (pltpu.roll(both, k, 0)[HALO : 2 * HALO] * weight) * same[k]
            total = silu(total).astype(BF16)
            conv[m, 0:HALO, at] = total
            if j < plan.pairs:
                scale = pair_columns(cols[0:HALO], weight_col + m * 16 + 2 * j, lane[0:HALO])
                scaled.append((total.astype(F32) * scale).astype(BF16))
            if j == plan.pairs:
                first_b = total
        edge_state = dot(jnp.concatenate(scaled, axis=1), first_b, ROWS)
        state = (main_state[m] + edge_state).astype(BF16)
        carried_end = docs[m : m + 1, LENGTH - 1 : LENGTH] == doc_before[m : m + 1, 127:128]
        carried_end = jnp.where(carried_end, 1.0, 0.0)
        hi_rows = (gate_parts[m][0] * carried_end).astype(BF16)
        lo_rows = (gate_parts[m][1] * carried_end).astype(BF16)
        for r in range(ring):
            fsend[m, r, 0 : plan.shard] = state[r * plan.shard : (r + 1) * plan.shard]
            at = slice(r * plan.gate_rows, (r + 1) * plan.gate_rows)
            fsend[m, r, plan.shard : plan.packet] = jnp.concatenate(
                [hi_rows[at], lo_rows[at]], axis=0
            )
        copies = exchange(m, fsend, lambda to, m=m: arecv.at[m, rank], a_send, a_recv)
        for copy in copies:
            copy.start()
        a_copies.append([all_of(m, arecv, a_send, a_recv)])
        arecv[m, pl.ds(rank, 1)] = fsend[m, pl.ds(rank, 1)]

    def scores_of(m):
        t_pos = lax.broadcasted_iota(jnp.int32, (LENGTH, LENGTH), 0)
        s_pos = lax.broadcasted_iota(jnp.int32, (LENGTH, LENGTH), 1)
        doc_t = mark_cols[:, m * TAPS : m * TAPS + 1]
        keep = (s_pos <= t_pos) & (doc_t == docs[m : m + 1])
        full = dot(conv[m, :, ch + DSTATE : ch + 2 * DSTATE], conv[m, :, ch : ch + DSTATE], LANES)
        scores[m] = jnp.where(keep, full, 0.0)

    def inner_of(m):
        low_lane = lane < HEADDIM
        for j in range(plan.pairs):
            at = slice(j * 128, (j + 1) * 128)
            xs = conv[m, :, at]
            xs_a = jnp.where(low_lane, xs, jnp.zeros_like(xs))
            xs_b = jnp.where(low_lane, jnp.zeros_like(xs), xs)
            for half in range(2):
                t0, s1 = half * HALF, (half + 1) * HALF
                base = scores[m, t0 : t0 + HALF, 0:s1]
                mixes = []
                for h in (2 * j, 2 * j + 1):
                    t_log = cols[t0 : t0 + HALF, log_col + m * 16 + h : log_col + m * 16 + h + 1]
                    s_log = log_rows[m][h : h + 1, 0:s1]
                    decay = jnp.exp(jnp.minimum(t_log - s_log, 0.0))
                    mixes.append((base * step_rows[m][h : h + 1, 0:s1] * decay).astype(BF16))
                y[m, t0 : t0 + HALF, at] = dot(
                    jnp.concatenate(mixes, axis=1),
                    jnp.concatenate([xs_a[0:s1], xs_b[0:s1]], axis=0),
                    (((1,), (0,)), ((), ())),
                )

    def gate_both(m):
        carried = mark_cols[:, m * TAPS : m * TAPS + 1] == doc_before[m : m + 1, 127:128]
        for j in range(plan.pairs):
            at = slice(j * 128, (j + 1) * 128)
            opened = zg[m, :, at]
            y[m, :, at] = y[m, :, at] * opened
            entry = pair_columns(cols, entry_col + m * 16 + 2 * j, lane)
            zg[m, :, at] = jnp.where(carried, entry, 0.0) * opened

    def unpack(packet):
        packet = packet.astype(F32)
        split = plan.shard + plan.gate_rows
        return packet[0 : plan.shard], packet[plan.shard : split] + packet[split:]

    def pack(ref, m, total, product):
        ref[m, 0 : plan.shard] = total.astype(BF16)
        hi_rows, lo_rows = split_two(product)
        ref[m, plan.shard : plan.packet] = jnp.concatenate([hi_rows, lo_rows], axis=0)

    def ahead(source, m, slot, k):
        return pltpu.make_async_remote_copy(
            src_ref=source.at[m],
            dst_ref=brecv.at[m, slot],
            send_sem=b_send.at[slot],
            recv_sem=b_recv.at[m, slot],
            device_id={"sz": iz + k},
            device_id_type=pl.DeviceIdType.MESH,
        )

    jumps = [(0, 1), (1, 1), (2, 3)]
    b_copies = [
        [ahead(tsend if slot == 0 else usend, m, slot, k) for slot, k in jumps] for m in range(BATCH)
    ]

    def goes(k):
        return iz + k < plan.planes

    def plane_total(m):
        for copy in a_copies[m]:
            copy.wait_recv()
        total = jnp.zeros((plan.shard, DSTATE), F32)
        product = jnp.ones((plan.gate_rows, DSTATE), F32)
        for d in range(ring):
            pref[m, d] = total
            qpref[m, d] = product
            fresh, gates = unpack(arecv[m, d])
            total = spread(gates, plan) * total + fresh
            product = product * gates
        pack(tsend, m, total, product)
        ptot[m] = total
        qtot[m] = product
        pl.when(has_above)(b_copies[m][0].start)

    def two_planes(m):
        pl.when(has_below)(b_copies[m][0].wait_recv)
        lower, gates = unpack(brecv[m, 0])
        lower = jnp.where(has_below, lower, 0.0)
        gates = jnp.where(has_below, gates, 0.0)
        product = qtot[m]
        pack(usend, m, spread(product, plan) * lower + ptot[m], product * gates)
        pl.when(has_above)(b_copies[m][1].start)
        pl.when(goes(3))(b_copies[m][2].start)

    gate_inputs(0)
    scores_of(0)
    pl.when(goes(2))(lambda: pl.semaphore_wait(word.at[0], 1))
    pl.when(has_below & goes(2))(lambda: tell_below(1))
    inner_of(0)
    gate_both(0)
    plane_total(0)
    plane_total(1)
    scores_of(1)
    pl.when(goes(3))(lambda: pl.semaphore_wait(word.at[1], 1))
    two_planes(0)
    two_planes(1)
    inner_of(1)
    c_copies = []
    for m in range(BATCH):
        pl.when(has_below)(b_copies[m][1].wait_recv)
        pl.when(iz >= 3)(b_copies[m][2].wait_recv)
        near, gates = unpack(brecv[m, 1])
        remote, _ = unpack(brecv[m, 2])
        incoming = spread(gates, plan) * jnp.where(iz >= 3, remote, 0.0) + near
        incoming = jnp.where(has_below, incoming, 0.0)
        for d in range(ring):
            entering = pref[m, d] + spread(qpref[m, d], plan) * incoming
            hsend[m, d] = entering.astype(BF16)
        home = pl.ds(pl.multiple_of(rank * plan.shard, 16), plan.shard)
        copies = exchange(m, hsend, lambda to, m=m: hstate.at[m, home], c_send, c_recv)
        for copy in copies:
            copy.start()
        c_copies.append([all_of(m, hsend, c_send, c_recv)])
        hstate[m, home] = hsend[m, rank]
        if m == 0:
            gate_inputs(1)
            gate_both(1)
            turn_weights()

    quarter = plan.out // QUARTERS

    def hops(q, upward):
        return plan.far if (q < QUARTERS // 2) == upward else plan.far - 1

    def owner_at(distance, upward):
        return lax.rem(me + distance if upward else me + members - distance, members)

    def arrow(m, q, hop, upward):
        buffer, send, got, to = (
            (up_recv, ring_send.at[0], up_got, up)
            if upward
            else (dn_recv, ring_send.at[1], dn_got, down)
        )
        rows = pl.ds(q * quarter, quarter)
        return pltpu.make_async_remote_copy(
            src_ref=part.at[m, owner_at(hops(q, upward) - hop, upward), rows],
            dst_ref=buffer.at[m, hop, rows],
            send_sem=send,
            recv_sem=got.at[m, q, hop],
            device_id=to,
            device_id_type=pl.DeviceIdType.MESH,
        )

    arrows = {}
    square_copies = {}
    need(got_gain)
    gain = gain_ref[...].reshape(1, ch)

    def project(m, distance, upward):
        owner = owner_at(distance, upward)
        rows = pl.ds(pl.multiple_of(owner * plan.out, 16), plan.out)
        part[m, owner] = dot(wt[rows, :], gated[m], LANES).astype(BF16)

    def shoot(m, hop, upward, pieces):
        for q in pieces:
            if hop < hops(q, upward):
                if hop > 0:
                    arrows[m, q, hop - 1, upward].wait_recv()
                    buffer = up_recv if upward else dn_recv
                    owner = owner_at(hops(q, upward) - hop, upward)
                    rows = slice(q * quarter, (q + 1) * quarter)
                    total = part[m, owner, rows].astype(F32) + buffer[m, hop - 1, rows].astype(F32)
                    part[m, owner, rows] = total.astype(BF16)
                arrows[m, q, hop, upward] = arrow(m, q, hop, upward)
                arrows[m, q, hop, upward].start()

    early, late = range(QUARTERS // 2), range(QUARTERS // 2, QUARTERS)

    def first_round(m):
        project(m, plan.far, True)
        shoot(m, 0, True, early)
        shoot(m, 0, False, late)
        if plan.far > 1:
            project(m, plan.far - 1, True)
            shoot(m, 0, True, late)
            project(m, plan.far - 1, False)
            shoot(m, 0, False, early)

    def pass_squares(m, hop):
        for side, upward in enumerate((True, False)):
            if hop < (plan.far if upward else plan.far - 1):
                if hop > 0:
                    square_copies[m, hop - 1, upward].wait_recv()
                copy = pltpu.make_async_remote_copy(
                    src_ref=ssend.at[m] if hop == 0 else srecv.at[m, side, hop - 1],
                    dst_ref=srecv.at[m, side, hop],
                    send_sem=s_send.at[m, side],
                    recv_sem=s_recv.at[m, side, hop],
                    device_id=up if upward else down,
                    device_id_type=pl.DeviceIdType.MESH,
                )
                copy.start()
                square_copies[m, hop, upward] = copy

    def next_round(m, hop):
        if hop + 1 < plan.far:
            project(m, plan.far - 1 - hop, True)
            project(m, plan.far - 1 - hop, False)
        shoot(m, hop, True, early)
        shoot(m, hop, False, late)
        shoot(m, hop, True, late)
        shoot(m, hop, False, early)
        pass_squares(m, hop)

    def carry(m):
        for copy in c_copies[m]:
            copy.wait_recv()
        squares = jnp.zeros((LENGTH, 128), F32)
        outer = dot(conv[m, :, ch + DSTATE : ch + 2 * DSTATE], hstate[m], LANES)
        for j in range(plan.pairs):
            at = slice(j * 128, (j + 1) * 128)
            mixed = y[m, :, at] + zg[m, :, at] * outer[:, at]
            squares = squares + mixed * mixed
            gated[m, :, at] = (mixed * gain[:, at]).astype(BF16)
        first_round(m)
        square_hi, square_lo = split_two(squares)
        ones = jnp.ones((8, 128), BF16)
        square_rows = dot(ones, square_hi, LANES) + dot(ones, square_lo, LANES)
        ssend[m] = square_rows[0:1]
        pass_squares(m, 0)

    carry(0)
    carry(1)
    for hop in range(1, plan.far):
        for m in range(BATCH):
            next_round(m, hop)
    for m in range(BATCH):
        project(m, 0, True)

    for m in range(BATCH):
        square = ssend[m]
        for side, upward in enumerate((True, False)):
            last = (plan.far if upward else plan.far - 1) - 1
            if last >= 0:
                square_copies[m, last, upward].wait_recv()
            for hop in range(last + 1):
                square = square + srecv[m, side, hop]
        scale = lax.rsqrt(square / INNER + EPSILON)
        for q in (*late, *early):
            rows = slice(q * quarter, (q + 1) * quarter)
            total = part[m, me, rows].astype(F32)
            for upward in (True, False):
                last = hops(q, upward) - 1
                if last >= 0:
                    arrows[m, q, last, upward].wait_recv()
                    buffer = up_recv if upward else dn_recv
                    total = total + buffer[m, last, rows].astype(F32)
            out_ref[m, rows, :] = (total * scale).astype(BF16)

    def sent():
        for copy in halos:
            copy.wait_send()

    pl.when(has_next)(sent)
    for group in (*a_copies, *c_copies):
        for copy in group:
            copy.wait_send()
    sent_halves = BATCH * (2 * plan.far - 1)
    assert QUARTERS == 2 and sent_halves % 2 == 0
    for side, to in enumerate((up, down)):
        pltpu.make_async_remote_copy(
            src_ref=part.at[0, pl.ds(0, sent_halves // 2)],
            dst_ref=part.at[0, pl.ds(0, sent_halves // 2)],
            send_sem=ring_send.at[side],
            recv_sem=up_got.at[0, 0, 0],
            device_id=to,
            device_id_type=pl.DeviceIdType.MESH,
        ).wait_send()
        for m in range(BATCH):
            rows = pl.ds(0, plan.far - side)
            if plan.far > side:
                pltpu.make_async_remote_copy(
                    src_ref=srecv.at[m, side, rows],
                    dst_ref=srecv.at[m, side, rows],
                    send_sem=s_send.at[m, side],
                    recv_sem=s_recv.at[m, side, 0],
                    device_id=to,
                    device_id_type=pl.DeviceIdType.MESH,
                ).wait_send()
    for slot, k in jumps:
        source = tsend if slot == 0 else usend
        pl.when(goes(k))(
            pltpu.make_async_remote_copy(
                src_ref=source,
                dst_ref=source,
                send_sem=b_send.at[slot],
                recv_sem=b_recv.at[0, slot],
                device_id={"sz": iz + k},
                device_id_type=pl.DeviceIdType.MESH,
            ).wait_send
        )


def shards(
    plan,
    x_inner,
    z_gate,
    b_input,
    c_input,
    dt_raw,
    doc_ids,
    conv_x,
    conv_b,
    conv_c,
    dt_bias,
    decay_rate,
    norm_gain,
    w_out,
):
    hbm = pl.BlockSpec(memory_space=pltpu.HBM)
    vmem = pl.BlockSpec(memory_space=pltpu.VMEM)
    ch, ring, members = plan.channels, plan.ring, plan.members
    dma = pltpu.SemaphoreType.DMA
    scratch = [
        pltpu.SMEM((plan.heads,), F32),
        pltpu.SMEM((plan.heads,), F32),
        pltpu.VMEM((ch,), F32),
        pltpu.VMEM((BATCH, LENGTH, plan.conv), BF16),
        pltpu.VMEM((BATCH, HALO, plan.conv), BF16),
        pltpu.VMEM((BATCH, LENGTH), jnp.int32),
        pltpu.VMEM((BATCH, 128), jnp.int32),
        pltpu.VMEM((plan.heads, BATCH, LENGTH), F32),
        pltpu.VMEM((TAPS, plan.conv), BF16),
        pltpu.VMEM((BATCH, LENGTH, ch), BF16),
        pltpu.VMEM((ch, plan.width), BF16),
        pltpu.VMEM((plan.width, ch), BF16),
        pltpu.VMEM((BATCH, LENGTH, plan.conv), BF16),
        pltpu.VMEM((BATCH, TAPS - 1, LENGTH, 128), F32),
        pltpu.VMEM((BATCH, ch, DSTATE), F32),
        pltpu.VMEM((BATCH, LENGTH, ch), BF16),
        pltpu.VMEM((BATCH, LENGTH, ch), F32),
        pltpu.VMEM((BATCH, LENGTH, LENGTH), F32),
        pltpu.VMEM((BATCH, LENGTH, ch), F32),
        pltpu.VMEM((BATCH, LENGTH, ch), BF16),
        pltpu.VMEM((BATCH, ring, plan.packet, DSTATE), BF16),
        pltpu.VMEM((BATCH, ring, plan.packet, DSTATE), BF16),
        pltpu.VMEM((BATCH, ring, plan.shard, DSTATE), F32),
        pltpu.VMEM((BATCH, ring, plan.gate_rows, DSTATE), F32),
        pltpu.VMEM((BATCH, plan.packet, DSTATE), BF16),
        pltpu.VMEM((BATCH, plan.packet, DSTATE), BF16),
        pltpu.VMEM((BATCH, plan.shard, DSTATE), F32),
        pltpu.VMEM((BATCH, plan.gate_rows, DSTATE), F32),
        pltpu.VMEM((BATCH, 3, plan.packet, DSTATE), BF16),
        pltpu.VMEM((BATCH, ring, plan.shard, DSTATE), BF16),
        pltpu.VMEM((BATCH, ch, DSTATE), BF16),
        pltpu.VMEM((BATCH, members, plan.out, LENGTH), BF16),
        pltpu.VMEM((BATCH, plan.far, plan.out, LENGTH), BF16),
        pltpu.VMEM((BATCH, plan.far, plan.out, LENGTH), BF16),
        pltpu.VMEM((BATCH, 1, LENGTH), F32),
        pltpu.VMEM((BATCH, 2, plan.far, 1, LENGTH), F32),
        dma((9,)),
        dma((2,)),
        dma((2,)),
        dma((BATCH,)),
        dma((BATCH,)),
        dma((3,)),
        dma((BATCH, 3)),
        dma((BATCH,)),
        dma((BATCH,)),
        dma((BATCH, 2)),
        dma((BATCH, 2, plan.far)),
        dma((2,)),
        dma((BATCH, QUARTERS, plan.far)),
        dma((BATCH, QUARTERS, plan.far)),
        pltpu.SemaphoreType.REGULAR((2,)),
    ]
    out = pl.pallas_call(
        functools.partial(layer_kernel, plan),
        name="mixer_layer",
        out_shape=pltpu.VMEM((BATCH, plan.out, LENGTH), BF16),
        in_specs=[hbm] * 13,
        out_specs=vmem,
        scratch_shapes=scratch,
        compiler_params=pltpu.CompilerParams(
            collective_id=0, has_side_effects=True, vmem_limit_bytes=60 * 1024 * 1024
        ),
    )(
        x_inner,
        z_gate,
        b_input,
        c_input,
        jnp.transpose(dt_raw, (2, 0, 1)),
        doc_ids,
        conv_x,
        conv_b,
        conv_c,
        dt_bias,
        decay_rate,
        norm_gain,
        w_out,
    )
    return jnp.transpose(out, (0, 2, 1))


def solution(mesh):
    members = mesh.shape["mp"]
    line = Mesh(mesh.devices.reshape(*SPLIT, members), (*SEQ, "mp"))

    def layer(*arrays):
        channels = arrays[0].shape[2] // members
        plan = Plan(SPLIT, members, channels, arrays[12].shape[1])
        placed = (
            P(None, SEQ, "mp"),
            P(None, SEQ, "mp"),
            P(None, SEQ, None),
            P(None, SEQ, None),
            P(None, SEQ, "mp"),
            P(None, SEQ),
            P(None, "mp"),
            P(),
            P(),
            P("mp"),
            P("mp"),
            P("mp"),
            P("mp", None),
        )
        return jax.shard_map(
            functools.partial(shards, plan),
            mesh=line,
            in_specs=placed,
            out_specs=P(None, SEQ, "mp"),
            check_vma=False,
        )(*arrays)

    return layer
```
